16 devices in a mesh: depth: 2 (over z), col: 2 (over y), row: 4 (over x, core).
Axes of the slice: x: 2, y: 2, z: 2, core: 2. Of those that a mesh axis runs over, the one named last changes fastest.
Arguments:
- a_mat: bfloat16 [8192, 8192], P('row', 'col')
- b_mat: bfloat16 [8192, 8192], P('row', 'col')
Outputs:
- output: bfloat16 [8192, 8192], P(('row', 'depth'), 'col')
All inputs are finite; a program needn't handle non-finite values.
Results may differ from the reference program's by a relative error of at most 0.001.
Values are sent between devices in bfloat16 or wider.
A program may use at most 1 GiB of HBM per device.

```python
import jax
import jax.numpy as jnp

D = 8192


def setup_inputs(seed: int = 0) -> dict:
    key_a, key_b = jax.random.split(jax.random.key(seed))
    a_mat = jax.random.normal(key_a, (D, D), jnp.float32) + 0.5
    b_mat = (jax.random.normal(key_b, (D, D), jnp.float32) + 2.0 * D ** -0.5) * D ** -0.5
    return {"a_mat": a_mat.astype(jnp.bfloat16), "b_mat": b_mat.astype(jnp.bfloat16)}


def reference(a_mat, b_mat):
    return jnp.dot(a_mat, b_mat, preferred_element_type=jnp.float32).astype(jnp.bfloat16)
```

```python
import functools

import jax
import jax.numpy as jnp
from jax import lax
from jax.experimental import pallas as pl
from jax.experimental.pallas import tpu as pltpu
from jax.sharding import PartitionSpec as P

MESH = pl.DeviceIdType.MESH
GROUP = 128
SUBS = 4
AHEAD = 8
LAG = 3
TILE = 512


def kernel(a_ref, b_ref, c_ref, ball, a_v, acc, b_far, b_near, o_v,
           load_a, send_a, recv_a, send_x, recv_x, send_z, recv_z, send_own, recv_own,
           send_px, recv_px, send_pz, recv_pz, load_far, load_near, store_c):
    depth = lax.axis_index("depth")
    col = lax.axis_index("col")
    row = lax.axis_index("row")
    core = lax.rem(row, 2)
    chip_x = row // 2
    rows_c = a_ref.shape[0] // 2
    band = b_ref.shape[0]
    cols = b_ref.shape[1]
    steps = band // GROUP
    half = cols // 2
    width = half // SUBS
    count = steps * SUBS
    quarter = cols // SUBS

    row_far = lax.rem(row + 2, 4)
    row_peer = chip_x * 2 + (1 - core)
    row_far_peer = lax.rem(row_peer + 2, 4)
    dev_x = (depth, col, row_far)
    dev_y = (depth, 1 - col, row)
    dev_z = (1 - depth, col, row)
    dev_p = (depth, col, row_peer)
    at_near = chip_x * steps
    at_far = (1 - chip_x) * steps
    at_mine = col * steps
    at_other = (1 - col) * steps

    def a_load(step, part):
        return pltpu.make_async_copy(
            a_ref.at[pl.ds(depth * rows_c, rows_c), pl.ds(part * band + step * GROUP, GROUP)],
            a_v.at[at_mine + step, :, pl.ds(part * GROUP, GROUP)],
            load_a.at[step])

    def a_load_wait(step):
        pltpu.make_async_copy(a_v.at[at_mine + step], a_v.at[at_mine + step], load_a.at[step]).wait()

    def a_send(step):
        return pltpu.make_async_remote_copy(
            a_v.at[at_mine + step], a_v.at[at_mine + step], send_a.at[step], recv_a.at[step],
            device_id=dev_y, device_id_type=MESH)

    def a_recv(step):
        return pltpu.make_async_remote_copy(
            a_v.at[at_other + step], a_v.at[at_other + step], send_a.at[step], recv_a.at[step],
            device_id=dev_y, device_id_type=MESH)

    def piece(band_row, num, which):
        step = num // SUBS
        sub = lax.rem(num, SUBS)
        return ball.at[pl.ds(band_row * band + step * GROUP, GROUP), pl.ds(which * half + sub * width, width)]

    def x_send(num):
        step = num // SUBS
        sub = lax.rem(num, SUBS)
        return pltpu.make_async_remote_copy(
            b_ref.at[pl.ds(step * GROUP, GROUP), pl.ds(depth * half + sub * width, width)],
            piece(row, num, depth), send_x.at[num], recv_x.at[num], device_id=dev_x, device_id_type=MESH)

    def x_recv(num):
        return pltpu.make_async_remote_copy(
            piece(row_far, num, depth), piece(row_far, num, depth), send_x.at[num], recv_x.at[num],
            device_id=dev_x, device_id_type=MESH)

    def z_send(num):
        return pltpu.make_async_remote_copy(
            piece(row_far, num, depth), piece(row_far, num, depth), send_z.at[num], recv_z.at[num],
            device_id=dev_z, device_id_type=MESH)

    def z_recv(num):
        return pltpu.make_async_remote_copy(
            piece(row_far, num, 1 - depth), piece(row_far, num, 1 - depth), send_z.at[num], recv_z.at[num],
            device_id=dev_z, device_id_type=MESH)

    def own_send(step):
        return pltpu.make_async_remote_copy(
            b_ref.at[pl.ds(step * GROUP, GROUP), :], ball.at[pl.ds(row * band + step * GROUP, GROUP), :],
            send_own.at[step], recv_own.at[step], device_id=dev_p, device_id_type=MESH)

    def own_recv(step):
        here = ball.at[pl.ds(row_peer * band + step * GROUP, GROUP), :]
        return pltpu.make_async_remote_copy(
            here, here, send_own.at[step], recv_own.at[step], device_id=dev_p, device_id_type=MESH)

    def half_group(band_row, step, which):
        return ball.at[pl.ds(band_row * band + step * GROUP, GROUP), pl.ds(which * half, half)]

    def px_send(step):
        here = half_group(row_far, step, depth)
        return pltpu.make_async_remote_copy(
            here, here, send_px.at[step], recv_px.at[step], device_id=dev_p, device_id_type=MESH)

    def px_recv(step):
        here = half_group(row_far_peer, step, depth)
        return pltpu.make_async_remote_copy(
            here, here, send_px.at[step], recv_px.at[step], device_id=dev_p, device_id_type=MESH)

    def pz_send(num):
        here = piece(row_far, num, 1 - depth)
        return pltpu.make_async_remote_copy(
            here, here, send_pz.at[num], recv_pz.at[num], device_id=dev_p, device_id_type=MESH)

    def pz_recv(num):
        here = piece(row_far_peer, num, 1 - depth)
        return pltpu.make_async_remote_copy(
            here, here, send_pz.at[num], recv_pz.at[num], device_id=dev_p, device_id_type=MESH)

    def near_loads(step):
        slot = lax.rem(step, 2)
        pltpu.make_async_copy(
            b_ref.at[pl.ds(step * GROUP, GROUP), :],
            b_near.at[slot, pl.ds(core * GROUP, GROUP), :], load_near.at[slot]).start()
        pltpu.make_async_copy(
            ball.at[pl.ds(row_peer * band + step * GROUP, GROUP), :],
            b_near.at[slot, pl.ds((1 - core) * GROUP, GROUP), :], load_near.at[slot]).start()

    def near_wait(step):
        slot = lax.rem(step, 2)
        pltpu.make_async_copy(b_near.at[slot], b_near.at[slot], load_near.at[slot]).wait()

    def far_loads(step):
        slot = lax.rem(step, 2)
        pltpu.make_async_copy(
            ball.at[pl.ds(row_far * band + step * GROUP, GROUP), :],
            b_far.at[slot, pl.ds(core * GROUP, GROUP), :], load_far.at[slot]).start()
        pltpu.make_async_copy(
            ball.at[pl.ds(row_far_peer * band + step * GROUP, GROUP), :],
            b_far.at[slot, pl.ds((1 - core) * GROUP, GROUP), :], load_far.at[slot]).start()

    def far_wait(step):
        slot = lax.rem(step, 2)
        pltpu.make_async_copy(b_far.at[slot], b_far.at[slot], load_far.at[slot]).wait()

    def add(a_at, buf, slot, sub):
        @pl.loop(0, quarter // TILE)
        def _(tile):
            at = pl.ds(pl.multiple_of(sub * quarter + tile * TILE, TILE), TILE)
            acc[:, at] += jnp.dot(a_v[a_at], buf[slot, :, at], preferred_element_type=jnp.float32)

    @pl.loop(0, steps)
    def _(step):
        a_load(step, 0).start()
        a_load(step, 1).start()

    barrier = pltpu.get_barrier_semaphore()
    for dev in (dev_x, dev_y, dev_z, dev_p):
        pl.semaphore_signal(barrier, inc=1, device_id=dev, device_id_type=MESH)
    pl.semaphore_wait(barrier, 4)

    @pl.loop(0, AHEAD)
    def _(num):
        x_send(num).start()

    own_send(0).start()
    own_send(1).start()

    @pl.loop(0, steps)
    def _(step):
        a_load_wait(step)
        a_send(step).start()

    @pl.loop(0, cols // TILE)
    def _(tile):
        at = pl.ds(pl.multiple_of(tile * TILE, TILE), TILE)
        acc[:, at] = jnp.zeros((rows_c, TILE), jnp.float32)

    @pl.loop(0, count)
    def _(num):
        step = num // SUBS
        sub = lax.rem(num, SUBS)
        x_recv(num).wait_recv()
        z_send(num).start()

        @pl.when(num + AHEAD < count)
        def _():
            x_send(num + AHEAD).start()

        @pl.when(sub == SUBS - 1)
        def _():
            px_send(step).start()

        @pl.when(num >= LAG)
        def _():
            z_recv(num - LAG).wait_recv()
            pz_send(num - LAG).start()

        @pl.when(sub == 0)
        def _():
            own_recv(step).wait_recv()
            near_loads(step)

            @pl.when(step + 2 < steps)
            def _():
                own_send(step + 2).start()

            @pl.when(step >= 1)
            def _():
                a_recv(step - 1).wait_recv()
                near_wait(step - 1)

            @pl.when(step >= 2)
            def _():
                far_wait(step - 2)

        @pl.when(step >= 1)
        def _():
            add(at_near + step - 1, b_near, lax.rem(step - 1, 2), sub)

        @pl.when(step >= 2)
        def _():
            add(at_far + step - 2, b_far, lax.rem(step - 2, 2), sub)

        @pl.when((sub == SUBS - 1) & (step >= 1))
        def _():
            px_recv(step - 1).wait_recv()
            for k in range(SUBS):
                pz_recv((step - 1) * SUBS + k).wait_recv()
            far_loads(step - 1)

    last = steps - 1
    a_recv(last).wait_recv()
    near_wait(last)
    far_wait(last - 1)

    for k in range(SUBS):
        if k < LAG:
            z_recv(count - LAG + k).wait_recv()
            pz_send(count - LAG + k).start()
        add(at_near + last, b_near, last % 2, k)
        add(at_far + last - 1, b_far, (last - 1) % 2, k)

    px_recv(last).wait_recv()
    for k in range(SUBS):
        pz_recv(last * SUBS + k).wait_recv()
    far_loads(last)
    far_wait(last)

    def c_store(sub):
        at = pl.ds(pl.multiple_of(sub * quarter, quarter), quarter)
        return pltpu.make_async_copy(o_v.at[:, at], c_ref.at[:, at], store_c.at[sub])

    @pl.loop(0, SUBS)
    def _(sub):
        @pl.loop(0, quarter // TILE)
        def _(tile):
            at = pl.ds(pl.multiple_of(sub * quarter + tile * TILE, TILE), TILE)
            total = acc[:, at] + jnp.dot(
                a_v[at_far + last], b_far[last % 2, :, at], preferred_element_type=jnp.float32)
            o_v[:, at] = total.astype(o_v.dtype)
        c_store(sub).start()

    @pl.loop(0, count)
    def _(num):
        x_send(num).wait_send()
        z_send(num).wait_send()
        pz_send(num).wait_send()

    @pl.loop(0, steps)
    def _(step):
        a_send(step).wait_send()
        own_send(step).wait_send()
        px_send(step).wait_send()

    @pl.loop(0, SUBS)
    def _(sub):
        c_store(sub).wait()


def solution(mesh):
    def local_mm(a_blk, b_blk):
        band, cols = b_blk.shape
        rows_c = a_blk.shape[0] // 2
        steps = band // GROUP
        count = steps * SUBS
        any_spec = pl.BlockSpec(memory_space=pl.ANY)
        dma = pltpu.SemaphoreType.DMA
        c_blk, _ = pl.pallas_call(
            kernel,
            out_shape=(jax.ShapeDtypeStruct((rows_c, cols), jnp.bfloat16),
                       jax.ShapeDtypeStruct((4 * band, cols), jnp.bfloat16)),
            in_specs=[any_spec] * 2,
            out_specs=(any_spec, any_spec),
            scratch_shapes=[
                pltpu.VMEM((2 * steps, rows_c, 2 * GROUP), jnp.bfloat16),
                pltpu.VMEM((rows_c, cols), jnp.float32),
                pltpu.VMEM((2, 2 * GROUP, cols), jnp.bfloat16),
                pltpu.VMEM((2, 2 * GROUP, cols), jnp.bfloat16),
                pltpu.VMEM((rows_c, cols), jnp.bfloat16),
                dma((steps,)), dma((steps,)), dma((steps,)),
                dma((count,)), dma((count,)), dma((count,)), dma((count,)),
                dma((steps,)), dma((steps,)), dma((steps,)), dma((steps,)),
                dma((count,)), dma((count,)),
                dma((2,)), dma((2,)), dma((SUBS,)),
            ],
            compiler_params=pltpu.CompilerParams(
                collective_id=0, has_side_effects=True, vmem_limit_bytes=60 * 1024 * 1024),
            cost_estimate=pl.CostEstimate(
                flops=2 * rows_c * cols * 2 * cols, bytes_accessed=200 * 2 ** 20, transcendentals=0),
        )(a_blk, b_blk)
        return c_blk

    return jax.shard_map(
        local_mm, mesh=mesh, in_specs=(P("row", "col"), P("row", "col")),
        out_specs=P(("row", "depth"), "col"), check_vma=False)
```

```python
import functools

import jax
import jax.numpy as jnp
from jax import lax
from jax.experimental import pallas as pl
from jax.experimental.pallas import tpu as pltpu
from jax.sharding import PartitionSpec as P

MESH = pl.DeviceIdType.MESH
GROUP = 128
SUBS = 8
AHEAD = 12
LAG = 4
SHIFT = 2
FAR = SUBS + LAG + 2
TILE = 512


def kernel(a_ref, b_ref, o_v, ball, a_v, acc, b_far, b_near, b_last,
           load_a, send_a, recv_a, send_x, recv_x, send_z, recv_z, send_own, recv_own,
           send_px, recv_px, send_pz, recv_pz, load_far, load_near, send_pl, recv_pl):
    depth = lax.axis_index("depth")
    col = lax.axis_index("col")
    row = lax.axis_index("row")
    core = lax.rem(row, 2)
    chip_x = row // 2
    rows_c = a_ref.shape[0] // 2
    band = b_ref.shape[0]
    cols = b_ref.shape[1]
    steps = band // GROUP
    half = cols // 2
    width = half // SUBS
    count = steps * SUBS

    row_far = lax.rem(row + 2, 4)
    row_peer = chip_x * 2 + (1 - core)
    row_far_peer = lax.rem(row_peer + 2, 4)
    dev_x = (depth, col, row_far)
    dev_y = (depth, 1 - col, row)
    dev_z = (1 - depth, col, row)
    dev_p = (depth, col, row_peer)
    at_near = chip_x * steps
    at_far = (1 - chip_x) * steps
    at_mine = col * steps
    at_other = (1 - col) * steps

    def a_load(step, part):
        return pltpu.make_async_copy(
            a_ref.at[pl.ds(depth * rows_c, rows_c), pl.ds(part * band + step * GROUP, GROUP)],
            a_v.at[at_mine + step, :, pl.ds(part * GROUP, GROUP)],
            load_a.at[step])

    def a_load_wait(step):
        pltpu.make_async_copy(a_v.at[at_mine + step], a_v.at[at_mine + step], load_a.at[step]).wait()

    def a_send(step):
        return pltpu.make_async_remote_copy(
            a_v.at[at_mine + step], a_v.at[at_mine + step], send_a.at[step], recv_a.at[step],
            device_id=dev_y, device_id_type=MESH)

    def a_recv(step):
        return pltpu.make_async_remote_copy(
            a_v.at[at_other + step], a_v.at[at_other + step], send_a.at[step], recv_a.at[step],
            device_id=dev_y, device_id_type=MESH)

    def piece(band_row, num, which):
        step = num // SUBS
        sub = lax.rem(num, SUBS)
        return ball.at[pl.ds(band_row * band + step * GROUP, GROUP), pl.ds(which * half + sub * width, width)]

    def last_piece(core_of, num, which):
        return b_last.at[pl.ds(core_of * GROUP, GROUP), pl.ds(which * half + lax.rem(num, SUBS) * width, width)]

    def source(num, which):
        return b_ref.at[pl.ds((num // SUBS) * GROUP, GROUP),
                        pl.ds(which * half + lax.rem(num, SUBS) * width, width)]

    def remote(src, dst, send, recv, num, dev):
        return pltpu.make_async_remote_copy(
            src, dst, send.at[num], recv.at[num], device_id=dev, device_id_type=MESH)

    def x_send(num):
        return remote(source(num, depth), piece(row, num, depth), send_x, recv_x, num, dev_x)

    def x_send_last(num):
        return remote(source(num, depth), last_piece(core, num, depth), send_x, recv_x, num, dev_x)

    def x_send_extra(num):
        return remote(source(num, 1 - depth), last_piece(core, num, 1 - depth), send_z, recv_z, num, dev_x)

    def x_recv(num):
        here = piece(row_far, num, depth)
        return remote(here, here, send_x, recv_x, num, dev_x)

    def x_recv_last(num):
        here = last_piece(core, num, depth)
        return remote(here, here, send_x, recv_x, num, dev_x)

    def z_send(num):
        here = piece(row_far, num, depth)
        return remote(here, here, send_z, recv_z, num, dev_z)

    def z_send_last(num):
        here = last_piece(core, num, depth)
        return remote(here, here, send_z, recv_z, num, dev_z)

    def z_recv(num):
        here = piece(row_far, num, 1 - depth)
        return remote(here, here, send_z, recv_z, num, dev_z)

    def z_recv_last(num):
        here = last_piece(core, num, 1 - depth)
        return remote(here, here, send_z, recv_z, num, dev_z)

    def own_send(step):
        return pltpu.make_async_remote_copy(
            b_ref.at[pl.ds(step * GROUP, GROUP), :], ball.at[pl.ds(row * band + step * GROUP, GROUP), :],
            send_own.at[step], recv_own.at[step], device_id=dev_p, device_id_type=MESH)

    def own_recv(step):
        here = ball.at[pl.ds(row_peer * band + step * GROUP, GROUP), :]
        return pltpu.make_async_remote_copy(
            here, here, send_own.at[step], recv_own.at[step], device_id=dev_p, device_id_type=MESH)

    def half_group(band_row, step, which):
        return ball.at[pl.ds(band_row * band + step * GROUP, GROUP), pl.ds(which * half, half)]

    def px_send(step):
        here = half_group(row_far, step, depth)
        return pltpu.make_async_remote_copy(
            here, here, send_px.at[step], recv_px.at[step], device_id=dev_p, device_id_type=MESH)

    def px_recv(step):
        here = half_group(row_far_peer, step, depth)
        return pltpu.make_async_remote_copy(
            here, here, send_px.at[step], recv_px.at[step], device_id=dev_p, device_id_type=MESH)

    def px_send_last(sub):
        here = last_piece(core, sub, depth)
        return remote(here, here, send_pl, recv_pl, sub, dev_p)

    def px_recv_last(sub):
        here = last_piece(1 - core, sub, depth)
        return remote(here, here, send_pl, recv_pl, sub, dev_p)

    def pz_send(num):
        here = piece(row_far, num, 1 - depth)
        return remote(here, here, send_pz, recv_pz, num, dev_p)

    def pz_recv(num):
        here = piece(row_far_peer, num, 1 - depth)
        return remote(here, here, send_pz, recv_pz, num, dev_p)

    def pz_send_last(num):
        here = last_piece(core, num, 1 - depth)
        return remote(here, here, send_pz, recv_pz, num, dev_p)

    def pz_recv_last(num):
        here = last_piece(1 - core, num, 1 - depth)
        return remote(here, here, send_pz, recv_pz, num, dev_p)

    def near_loads(step):
        slot = lax.rem(step, 2)
        pltpu.make_async_copy(
            b_ref.at[pl.ds(step * GROUP, GROUP), :],
            b_near.at[slot, pl.ds(core * GROUP, GROUP), :], load_near.at[slot]).start()
        pltpu.make_async_copy(
            ball.at[pl.ds(row_peer * band + step * GROUP, GROUP), :],
            b_near.at[slot, pl.ds((1 - core) * GROUP, GROUP), :], load_near.at[slot]).start()

    def near_wait(step):
        slot = lax.rem(step, 2)
        pltpu.make_async_copy(b_near.at[slot], b_near.at[slot], load_near.at[slot]).wait()

    def far_loads(step):
        slot = lax.rem(step, 2)
        pltpu.make_async_copy(
            ball.at[pl.ds(row_far * band + step * GROUP, GROUP), :],
            b_far.at[slot, pl.ds(core * GROUP, GROUP), :], load_far.at[slot]).start()
        pltpu.make_async_copy(
            ball.at[pl.ds(row_far_peer * band + step * GROUP, GROUP), :],
            b_far.at[slot, pl.ds((1 - core) * GROUP, GROUP), :], load_far.at[slot]).start()

    def far_wait(step):
        slot = lax.rem(step, 2)
        pltpu.make_async_copy(b_far.at[slot], b_far.at[slot], load_far.at[slot]).wait()

    def add(a_at, buf, slot, sub):
        at = pl.ds(pl.multiple_of(sub * TILE, TILE), TILE)
        acc[:, at] += jnp.dot(a_v[a_at], buf[slot, :, at], preferred_element_type=jnp.float32)

    def work(num):
        step = num // SUBS
        sub = lax.rem(num, SUBS)
        late = num - (FAR - 1)
        mul = num - FAR

        @pl.when(sub == 0)
        def _():
            own_recv(step).wait_recv()
            near_loads(step)

            @pl.when(step + 2 < steps)
            def _():
                own_send(step + 2).start()

            @pl.when(step >= 1)
            def _():
                a_recv(step - 1).wait_recv()
                near_wait(step - 1)

        @pl.when(step >= 1)
        def _():
            add(at_near + step - 1, b_near, lax.rem(step - 1, 2), sub)

        @pl.when((mul >= 0) & (lax.rem(mul + SUBS * 2, SUBS) == 0))
        def _():
            far_wait(mul // SUBS)

        @pl.when(mul >= 0)
        def _():
            add(at_far + mul // SUBS, b_far, lax.rem(mul // SUBS, 2), lax.rem(mul, SUBS))

        @pl.when((late >= 0) & (lax.rem(late + SUBS * 2, SUBS) == 0))
        def _():
            px_recv(late // SUBS).wait_recv()

            @pl.loop(0, SUBS)
            def _(k):
                pz_recv((late // SUBS) * SUBS + k).wait_recv()
            far_loads(late // SUBS)

    @pl.loop(0, steps)
    def _(step):
        a_load(step, 0).start()
        a_load(step, 1).start()

    barrier = pltpu.get_barrier_semaphore()
    for dev in (dev_x, dev_y, dev_z, dev_p):
        pl.semaphore_signal(barrier, inc=1, device_id=dev, device_id_type=MESH)
    pl.semaphore_wait(barrier, 4)

    @pl.loop(0, AHEAD)
    def _(num):
        x_send(num).start()

    own_send(0).start()
    own_send(1).start()

    @pl.loop(0, steps)
    def _(step):
        a_load_wait(step)
        a_send(step).start()

    @pl.loop(0, cols // TILE)
    def _(tile):
        at = pl.ds(pl.multiple_of(tile * TILE, TILE), TILE)
        acc[:, at] = jnp.zeros((rows_c, TILE), jnp.float32)

    body = count - SUBS

    @pl.loop(0, body)
    def _(num):
        x_recv(num).wait_recv()
        z_send(num).start()

        @pl.when(num + AHEAD < body)
        def _():
            x_send(num + AHEAD).start()

        @pl.when(num + AHEAD >= body)
        def _():
            @pl.when(num + AHEAD < count)
            def _():
                x_send_last(num + AHEAD).start()

            @pl.when((num + AHEAD >= count) & (num + AHEAD < count + SHIFT))
            def _():
                x_send_extra(num + AHEAD - SHIFT).start()

        @pl.when(lax.rem(num, SUBS) == SUBS - 1)
        def _():
            px_send(num // SUBS).start()

        @pl.when(num >= LAG)
        def _():
            z_recv(num - LAG).wait_recv()
            pz_send(num - LAG).start()

        work(num)

    @pl.loop(body, count)
    def _(num):
        x_recv_last(num).wait_recv()

        @pl.when(num < count - SHIFT)
        def _():
            z_send_last(num).start()
        px_send_last(num - body).start()

        @pl.when(num < body + LAG)
        def _():
            z_recv(num - LAG).wait_recv()
            pz_send(num - LAG).start()

        @pl.when(num >= body + LAG)
        def _():
            z_recv_last(num - LAG).wait_recv()
            pz_send_last(num - LAG).start()

        work(num)

    last = steps - 1

    def relay_out(num):
        z_recv_last(num).wait_recv()
        pz_send_last(num).start()

    def far_add(mul):
        add(at_far + last - 1, b_far, (last - 1) % 2, mul - (last - 1) * SUBS)

    for num in range(count - FAR, body):
        far_add(num)
        if num - (count - FAR) < LAG - 2:
            relay_out(count - LAG + num - (count - FAR))
    a_recv(last).wait_recv()
    near_wait(last)
    for sub in range(SUBS):
        add(at_near + last, b_near, last % 2, sub)
        if sub == SUBS // 2:
            relay_out(count - 2)
    relay_out(count - 1)

    def finish(at):
        total = acc[:, at] + jnp.dot(a_v[at_far + last], b_last[:, at], preferred_element_type=jnp.float32)
        o_v[:, at] = total.astype(o_v.dtype)

    per = TILE // width

    @pl.loop(0, half // TILE)
    def _(tile):
        for k in range(per):
            px_recv_last(tile * per + k).wait_recv()
        finish(pl.ds(pl.multiple_of(depth * half + tile * TILE, TILE), TILE))

    @pl.loop(0, half // TILE)
    def _(tile):
        for k in range(per):
            pz_recv_last(body + tile * per + k).wait_recv()
        finish(pl.ds(pl.multiple_of((1 - depth) * half + tile * TILE, TILE), TILE))

    @pl.loop(0, body)
    def _(num):
        x_send(num).wait_send()
        z_send(num).wait_send()
        pz_send(num).wait_send()

    @pl.loop(body, count)
    def _(num):
        x_send_last(num).wait_send()
        z_send_last(num).wait_send()
        pz_send_last(num).wait_send()
        px_send_last(num - body).wait_send()

    @pl.loop(0, steps)
    def _(step):
        a_send(step).wait_send()
        own_send(step).wait_send()

    @pl.loop(0, steps - 1)
    def _(step):
        px_send(step).wait_send()


def solution(mesh):
    def local_mm(a_blk, b_blk):
        band, cols = b_blk.shape
        rows_c = a_blk.shape[0] // 2
        steps = band // GROUP
        count = steps * SUBS
        any_spec = pl.BlockSpec(memory_space=pl.ANY)
        dma = pltpu.SemaphoreType.DMA
        c_blk, _ = pl.pallas_call(
            kernel,
            out_shape=(pltpu.VMEM((rows_c, cols), jnp.bfloat16),
                       jax.ShapeDtypeStruct((4 * band, cols), jnp.bfloat16)),
            in_specs=[any_spec] * 2,
            out_specs=(pl.BlockSpec(memory_space=pltpu.VMEM), any_spec),
            scratch_shapes=[
                pltpu.VMEM((2 * steps, rows_c, 2 * GROUP), jnp.bfloat16),
                pltpu.VMEM((rows_c, cols), jnp.float32),
                pltpu.VMEM((2, 2 * GROUP, cols), jnp.bfloat16),
                pltpu.VMEM((2, 2 * GROUP, cols), jnp.bfloat16),
                pltpu.VMEM((2 * GROUP, cols), jnp.bfloat16),
                dma((steps,)), dma((steps,)), dma((steps,)),
                dma((count,)), dma((count,)), dma((count,)), dma((count,)),
                dma((steps,)), dma((steps,)), dma((steps,)), dma((steps,)),
                dma((count,)), dma((count,)),
                dma((2,)), dma((2,)), dma((SUBS,)), dma((SUBS,)),
            ],
            compiler_params=pltpu.CompilerParams(
                collective_id=0, has_side_effects=True, vmem_limit_bytes=48 * 1024 * 1024),
            cost_estimate=pl.CostEstimate(
                flops=2 * rows_c * cols * 2 * cols, bytes_accessed=200 * 2 ** 20, transcendentals=0),
        )(a_blk, b_blk)
        return c_blk

    return jax.shard_map(
        local_mm, mesh=mesh, in_specs=(P("row", "col"), P("row", "col")),
        out_specs=P(("row", "depth"), "col"), check_vma=False)
```

```python
import jax
import jax.numpy as jnp
from jax import lax
from jax.experimental import pallas as pl
from jax.experimental.pallas import tpu as pltpu
from jax.sharding import PartitionSpec as P

MESH = pl.DeviceIdType.MESH
GROUP = 128
SUBS = 8
AHEAD = 12
LAG = 4
SHIFT = 2
LOAD = 6
TILE = 512
WIDE = 1024


def kernel(a_ref, b_ref, o_v, ball, a_v, acc, b_v,
           load_a, send_a, recv_a, send_x, recv_x, send_z, recv_z, send_own, recv_own,
           send_px, recv_px, send_pz, recv_pz, load_far, load_near):
    depth = lax.axis_index("depth")
    col = lax.axis_index("col")
    row = lax.axis_index("row")
    core = lax.rem(row, 2)
    chip_x = row // 2
    rows_c = a_ref.shape[0] // 2
    band = b_ref.shape[0]
    cols = b_ref.shape[1]
    steps = band // GROUP
    last = steps - 1
    half = cols // 2
    width = half // SUBS
    count = steps * SUBS
    body = count - SUBS
    per = TILE // width
    tiles = half // TILE

    row_far = lax.rem(row + 2, 4)
    row_peer = chip_x * 2 + (1 - core)
    row_far_peer = lax.rem(row_peer + 2, 4)
    dev_x = (depth, col, row_far)
    dev_y = (depth, 1 - col, row)
    dev_z = (1 - depth, col, row)
    dev_p = (depth, col, row_peer)
    near = chip_x * 2 * GROUP
    far = (1 - chip_x) * 2 * GROUP

    def slot_of(step):
        return lax.rem(step, 2)

    def remote(src, dst, send, recv, num, dev):
        return pltpu.make_async_remote_copy(
            src, dst, send.at[num], recv.at[num], device_id=dev, device_id_type=MESH)

    def a_cols(step, side):
        return a_v.at[step, :, pl.ds(side * 2 * GROUP, 2 * GROUP)]

    def a_load(step, part):
        return pltpu.make_async_copy(
            a_ref.at[pl.ds(depth * rows_c, rows_c), pl.ds(part * band + step * GROUP, GROUP)],
            a_v.at[step, :, pl.ds(col * 2 * GROUP + part * GROUP, GROUP)], load_a.at[step])

    def a_load_wait(step):
        pltpu.make_async_copy(a_cols(step, col), a_cols(step, col), load_a.at[step]).wait()

    def a_send(step):
        return remote(a_cols(step, col), a_cols(step, col), send_a, recv_a, step, dev_y)

    def a_recv(step):
        return remote(a_cols(step, 1 - col), a_cols(step, 1 - col), send_a, recv_a, step, dev_y)

    def piece(band_row, num, which):
        return ball.at[pl.ds(band_row * band + (num // SUBS) * GROUP, GROUP),
                       pl.ds(which * half + lax.rem(num, SUBS) * width, width)]

    def last_piece(core_of, num, which, first=far):
        return b_v.at[2, pl.ds(first + core_of * GROUP, GROUP),
                      pl.ds(which * half + lax.rem(num, SUBS) * width, width)]

    def source(num, which):
        return b_ref.at[pl.ds((num // SUBS) * GROUP, GROUP),
                        pl.ds(which * half + lax.rem(num, SUBS) * width, width)]

    def mine(num, which, is_last):
        return last_piece(core, num, which) if is_last else piece(row_far, num, which)

    def peers(num, which, is_last):
        return last_piece(1 - core, num, which) if is_last else piece(row_far_peer, num, which)

    def x_send(num, is_last):
        dst = last_piece(core, num, depth, near) if is_last else piece(row, num, depth)
        return remote(source(num, depth), dst, send_x, recv_x, num, dev_x)

    def x_send_extra(num):
        return remote(source(num, 1 - depth), last_piece(core, num, 1 - depth, near), send_z, recv_z, num, dev_x)

    def x_recv(num, is_last):
        here = mine(num, depth, is_last)
        return remote(here, here, send_x, recv_x, num, dev_x)

    def z_send(num, is_last):
        here = mine(num, depth, is_last)
        return remote(here, here, send_z, recv_z, num, dev_z)

    def z_recv(num, is_last):
        here = mine(num, 1 - depth, is_last)
        return remote(here, here, send_z, recv_z, num, dev_z)

    def px_send(num, is_last):
        here = mine(num, depth, is_last)
        return remote(here, here, send_px, recv_px, num, dev_p)

    def px_recv(num, is_last):
        here = peers(num, depth, is_last)
        return remote(here, here, send_px, recv_px, num, dev_p)

    def pz_send(num, is_last):
        here = mine(num, 1 - depth, is_last)
        return remote(here, here, send_pz, recv_pz, num, dev_p)

    def pz_recv(num, is_last):
        here = peers(num, 1 - depth, is_last)
        return remote(here, here, send_pz, recv_pz, num, dev_p)

    def own_send(step):
        return remote(
            b_ref.at[pl.ds(step * GROUP, GROUP), :], ball.at[pl.ds(row * band + step * GROUP, GROUP), :],
            send_own, recv_own, step, dev_p)

    def own_recv(step):
        here = ball.at[pl.ds(row_peer * band + step * GROUP, GROUP), :]
        return remote(here, here, send_own, recv_own, step, dev_p)

    def near_loads(step, slot):
        pltpu.make_async_copy(
            b_ref.at[pl.ds(step * GROUP, GROUP), :],
            b_v.at[slot, pl.ds(near + core * GROUP, GROUP), :], load_near.at[lax.rem(step, 2)]).start()
        pltpu.make_async_copy(
            ball.at[pl.ds(row_peer * band + step * GROUP, GROUP), :],
            b_v.at[slot, pl.ds(near + (1 - core) * GROUP, GROUP), :], load_near.at[lax.rem(step, 2)]).start()

    def near_wait(step, slot):
        here = b_v.at[slot, pl.ds(near, 2 * GROUP), :]
        pltpu.make_async_copy(here, here, load_near.at[lax.rem(step, 2)]).wait()

    def tile_cols(num):
        at = lax.rem(num, 2 * tiles)
        which = jnp.where(at < tiles, depth, 1 - depth)
        return pl.ds(pl.multiple_of(which * half + lax.rem(at, tiles) * TILE, TILE), TILE)

    def far_loads(num):
        step = num // SUBS
        slot = slot_of(step)
        at = tile_cols(num)
        for band_row, part in ((row_far, core), (row_far_peer, 1 - core)):
            pltpu.make_async_copy(
                ball.at[pl.ds(band_row * band + step * GROUP, GROUP), at],
                b_v.at[slot, pl.ds(far + part * GROUP, GROUP), at], load_far.at[lax.rem(num, SUBS)]).start()

    def far_wait(num):
        here = b_v.at[slot_of(num // SUBS), pl.ds(far, 2 * GROUP), tile_cols(num)]
        pltpu.make_async_copy(here, here, load_far.at[lax.rem(num, SUBS)]).wait()

    def work(num, to_load):
        step = num // SUBS
        sub = lax.rem(num, SUBS)

        @pl.when(sub == 0)
        def _():
            own_recv(step).wait_recv()
            if to_load:
                near_loads(step, slot_of(step))

                @pl.when(step + 2 < steps)
                def _():
                    own_send(step + 2).start()
            else:
                near_loads(step, 2)

            @pl.when(step >= 1)
            def _():
                a_recv(step - 1).wait_recv()
                near_wait(step - 1, slot_of(step - 1))

        @pl.when((num >= LOAD) & (num < body + LOAD))
        def _():
            new = num - LOAD
            at = lax.rem(new, 2 * tiles)
            first = (new // SUBS) * SUBS + lax.rem(at, tiles) * per

            @pl.when(at < tiles)
            def _():
                for k in range(per):
                    px_recv(first + k, False).wait_recv()

            @pl.when(at >= tiles)
            def _():
                for k in range(per):
                    pz_recv(first + k, False).wait_recv()
            far_loads(new)

        @pl.when(step >= 1)
        def _():
            far_wait(num - SUBS)
            at = tile_cols(num)
            acc[:, at] += jnp.dot(a_v[step - 1], b_v[slot_of(step - 1), :, at], preferred_element_type=jnp.float32)

    @pl.loop(0, steps)
    def _(step):
        a_load(step, 0).start()
        a_load(step, 1).start()

    barrier = pltpu.get_barrier_semaphore()
    for dev in (dev_x, dev_y, dev_z, dev_p):
        pl.semaphore_signal(barrier, inc=1, device_id=dev, device_id_type=MESH)
    pl.semaphore_wait(barrier, 4)

    @pl.loop(0, AHEAD)
    def _(num):
        x_send(num, False).start()

    own_send(0).start()
    own_send(1).start()

    @pl.loop(0, steps)
    def _(step):
        a_load_wait(step)
        a_send(step).start()

    @pl.loop(0, cols // TILE)
    def _(tile):
        at = pl.ds(pl.multiple_of(tile * TILE, TILE), TILE)
        acc[:, at] = jnp.zeros((rows_c, TILE), jnp.float32)

    @pl.loop(0, body)
    def _(num):
        x_recv(num, False).wait_recv()
        z_send(num, False).start()
        px_send(num, False).start()

        @pl.when(num + AHEAD < body)
        def _():
            x_send(num + AHEAD, False).start()

        @pl.when((num + AHEAD >= body) & (num + AHEAD < count))
        def _():
            x_send(num + AHEAD, True).start()

        @pl.when((num + AHEAD >= count) & (num + AHEAD < count + SHIFT))
        def _():
            x_send_extra(num + AHEAD - SHIFT).start()

        @pl.when(num >= LAG)
        def _():
            z_recv(num - LAG, False).wait_recv()
            pz_send(num - LAG, False).start()

        work(num, True)

    @pl.loop(body, count)
    def _(num):
        x_recv(num, True).wait_recv()

        @pl.when(num < count - SHIFT)
        def _():
            z_send(num, True).start()
        px_send(num, True).start()

        @pl.when(num < body + LAG)
        def _():
            z_recv(num - LAG, False).wait_recv()
            pz_send(num - LAG, False).start()

        @pl.when(num >= body + LAG)
        def _():
            z_recv(num - LAG, True).wait_recv()
            pz_send(num - LAG, True).start()

        work(num, False)

    def relay_out(num):
        z_recv(num, True).wait_recv()
        pz_send(num, True).start()

    relay_out(count - 4)
    a_recv(last).wait_recv()
    near_wait(last, 2)
    wide = half // WIDE
    for part in range(2 * wide):
        which = depth if part < wide else 1 - depth
        first = (part % wide) * (WIDE // width)
        for k in range(WIDE // width):
            if part < wide:
                px_recv(body + first + k, True).wait_recv()
            else:
                pz_recv(body + first + k, True).wait_recv()
        at = pl.ds(pl.multiple_of(which * half + (part % wide) * WIDE, WIDE), WIDE)
        total = acc[:, at] + jnp.dot(a_v[last], b_v[2, :, at], preferred_element_type=jnp.float32)
        o_v[:, at] = total.astype(o_v.dtype)
        if part < 3:
            relay_out(count - 3 + part)

    @pl.loop(0, body)
    def _(num):
        x_send(num, False).wait_send()
        z_send(num, False).wait_send()
        px_send(num, False).wait_send()
        pz_send(num, False).wait_send()

    @pl.loop(body, count)
    def _(num):
        x_send(num, True).wait_send()
        z_send(num, True).wait_send()
        px_send(num, True).wait_send()
        pz_send(num, True).wait_send()

    @pl.loop(0, steps)
    def _(step):
        a_send(step).wait_send()
        own_send(step).wait_send()


def solution(mesh):
    def local_mm(a_blk, b_blk):
        band, cols = b_blk.shape
        rows_c = a_blk.shape[0] // 2
        steps = band // GROUP
        count = steps * SUBS
        any_spec = pl.BlockSpec(memory_space=pl.ANY)
        dma = pltpu.SemaphoreType.DMA
        c_blk, _ = pl.pallas_call(
            kernel,
            out_shape=(pltpu.VMEM((rows_c, cols), jnp.bfloat16),
                       jax.ShapeDtypeStruct((4 * band, cols), jnp.bfloat16)),
            in_specs=[any_spec] * 2,
            out_specs=(pl.BlockSpec(memory_space=pltpu.VMEM), any_spec),
            scratch_shapes=[
                pltpu.VMEM((steps, rows_c, 4 * GROUP), jnp.bfloat16),
                pltpu.VMEM((rows_c, cols), jnp.float32),
                pltpu.VMEM((3, 4 * GROUP, cols), jnp.bfloat16),
                dma((steps,)), dma((steps,)), dma((steps,)),
                dma((count,)), dma((count,)), dma((count,)), dma((count,)),
                dma((steps,)), dma((steps,)),
                dma((count,)), dma((count,)), dma((count,)), dma((count,)),
                dma((SUBS,)), dma((2,)),
            ],
            compiler_params=pltpu.CompilerParams(
                collective_id=0, has_side_effects=True, vmem_limit_bytes=52 * 1024 * 1024),
            cost_estimate=pl.CostEstimate(
                flops=2 * rows_c * cols * 2 * cols, bytes_accessed=200 * 2 ** 20, transcendentals=0),
        )(a_blk, b_blk)
        return c_blk

    return jax.shard_map(
        local_mm, mesh=mesh, in_specs=(P("row", "col"), P("row", "col")),
        out_specs=P(("row", "depth"), "col"), check_vma=False)
```

```python
import jax
import jax.numpy as jnp
from jax import lax
from jax.experimental import pallas as pl
from jax.experimental.pallas import tpu as pltpu
from jax.sharding import PartitionSpec as P

MESH = pl.DeviceIdType.MESH
GROUP = 128
SUBS = 8
AHEAD = 16
LAG = 4
SHIFT = 6
LOAD = 6
TILE = 512
WIDE = 1024


def kernel(a_ref, b_ref, o_v, ball, a_v, acc, b_v,
           load_a, send_a, recv_a, send_x, recv_x, send_z, recv_z, send_own, recv_own,
           send_px, recv_px, send_pz, recv_pz, load_far, load_near):
    depth = lax.axis_index("depth")
    col = lax.axis_index("col")
    row = lax.axis_index("row")
    core = lax.rem(row, 2)
    chip_x = row // 2
    rows_c = a_ref.shape[0] // 2
    band = b_ref.shape[0]
    cols = b_ref.shape[1]
    steps = band // GROUP
    last = steps - 1
    half = cols // 2
    width = half // SUBS
    count = steps * SUBS
    body = count - SUBS
    per = TILE // width
    tiles = half // TILE

    row_far = lax.rem(row + 2, 4)
    row_peer = chip_x * 2 + (1 - core)
    row_far_peer = lax.rem(row_peer + 2, 4)
    dev_x = (depth, col, row_far)
    dev_y = (depth, 1 - col, row)
    dev_z = (1 - depth, col, row)
    dev_p = (depth, col, row_peer)
    near = chip_x * 2 * GROUP
    far = (1 - chip_x) * 2 * GROUP

    def slot_of(step):
        return lax.rem(step, 2)

    def remote(src, dst, send, recv, num, dev):
        return pltpu.make_async_remote_copy(
            src, dst, send.at[num], recv.at[num], device_id=dev, device_id_type=MESH)

    def a_cols(step, side):
        return a_v.at[step, :, pl.ds(side * 2 * GROUP, 2 * GROUP)]

    def a_load(step, part):
        return pltpu.make_async_copy(
            a_ref.at[pl.ds(depth * rows_c, rows_c), pl.ds(part * band + step * GROUP, GROUP)],
            a_v.at[step, :, pl.ds(col * 2 * GROUP + part * GROUP, GROUP)], load_a.at[step])

    def a_load_wait(step):
        pltpu.make_async_copy(a_cols(step, col), a_cols(step, col), load_a.at[step]).wait()

    def a_send(step):
        return remote(a_cols(step, col), a_cols(step, col), send_a, recv_a, step, dev_y)

    def a_recv(step):
        return remote(a_cols(step, 1 - col), a_cols(step, 1 - col), send_a, recv_a, step, dev_y)

    def piece(band_row, num, which):
        return ball.at[pl.ds(band_row * band + (num // SUBS) * GROUP, GROUP),
                       pl.ds(which * half + lax.rem(num, SUBS) * width, width)]

    def last_piece(core_of, num, which, first=far):
        return b_v.at[2, pl.ds(first + core_of * GROUP, GROUP),
                      pl.ds(which * half + lax.rem(num, SUBS) * width, width)]

    def source(num, which):
        return b_ref.at[pl.ds((num // SUBS) * GROUP, GROUP),
                        pl.ds(which * half + lax.rem(num, SUBS) * width, width)]

    def mine(num, which, is_last):
        return last_piece(core, num, which) if is_last else piece(row_far, num, which)

    def peers(num, which, is_last):
        return last_piece(1 - core, num, which) if is_last else piece(row_far_peer, num, which)

    def x_send(num, is_last):
        dst = last_piece(core, num, depth, near) if is_last else piece(row, num, depth)
        return remote(source(num, depth), dst, send_x, recv_x, num, dev_x)

    def x_send_extra(num):
        return remote(source(num, 1 - depth), last_piece(core, num, 1 - depth, near), send_z, recv_z, num, dev_x)

    def x_recv(num, is_last):
        here = mine(num, depth, is_last)
        return remote(here, here, send_x, recv_x, num, dev_x)

    def z_send(num, is_last):
        here = mine(num, depth, is_last)
        return remote(here, here, send_z, recv_z, num, dev_z)

    def z_recv(num, is_last):
        here = mine(num, 1 - depth, is_last)
        return remote(here, here, send_z, recv_z, num, dev_z)

    def px_send(num, is_last):
        here = mine(num, depth, is_last)
        return remote(here, here, send_px, recv_px, num, dev_p)

    def px_recv(num, is_last):
        here = peers(num, depth, is_last)
        return remote(here, here, send_px, recv_px, num, dev_p)

    def pz_send(num, is_last):
        here = mine(num, 1 - depth, is_last)
        return remote(here, here, send_pz, recv_pz, num, dev_p)

    def pz_recv(num, is_last):
        here = peers(num, 1 - depth, is_last)
        return remote(here, here, send_pz, recv_pz, num, dev_p)

    def own_send(step):
        return remote(
            b_ref.at[pl.ds(step * GROUP, GROUP), :], ball.at[pl.ds(row * band + step * GROUP, GROUP), :],
            send_own, recv_own, step, dev_p)

    def own_recv(step):
        here = ball.at[pl.ds(row_peer * band + step * GROUP, GROUP), :]
        return remote(here, here, send_own, recv_own, step, dev_p)

    def near_loads(step, slot):
        pltpu.make_async_copy(
            b_ref.at[pl.ds(step * GROUP, GROUP), :],
            b_v.at[slot, pl.ds(near + core * GROUP, GROUP), :], load_near.at[lax.rem(step, 2)]).start()
        pltpu.make_async_copy(
            ball.at[pl.ds(row_peer * band + step * GROUP, GROUP), :],
            b_v.at[slot, pl.ds(near + (1 - core) * GROUP, GROUP), :], load_near.at[lax.rem(step, 2)]).start()

    def near_wait(step, slot):
        here = b_v.at[slot, pl.ds(near, 2 * GROUP), :]
        pltpu.make_async_copy(here, here, load_near.at[lax.rem(step, 2)]).wait()

    def tile_cols(num):
        at = lax.rem(num, 2 * tiles)
        which = jnp.where(at < tiles, depth, 1 - depth)
        return pl.ds(pl.multiple_of(which * half + lax.rem(at, tiles) * TILE, TILE), TILE)

    def far_loads(num):
        step = num // SUBS
        slot = slot_of(step)
        at = tile_cols(num)
        for band_row, part in ((row_far, core), (row_far_peer, 1 - core)):
            pltpu.make_async_copy(
                ball.at[pl.ds(band_row * band + step * GROUP, GROUP), at],
                b_v.at[slot, pl.ds(far + part * GROUP, GROUP), at], load_far.at[lax.rem(num, SUBS)]).start()

    def far_wait(num):
        here = b_v.at[slot_of(num // SUBS), pl.ds(far, 2 * GROUP), tile_cols(num)]
        pltpu.make_async_copy(here, here, load_far.at[lax.rem(num, SUBS)]).wait()

    def work(num, to_load):
        step = num // SUBS
        sub = lax.rem(num, SUBS)

        @pl.when(sub == 0)
        def _():
            own_recv(step).wait_recv()
            if to_load:
                near_loads(step, slot_of(step))

                @pl.when(step + 2 < steps)
                def _():
                    own_send(step + 2).start()
            else:
                near_loads(step, 2)

            @pl.when(step >= 1)
            def _():
                a_recv(step - 1).wait_recv()
                near_wait(step - 1, slot_of(step - 1))

        @pl.when((num >= LOAD) & (num < body + LOAD))
        def _():
            new = num - LOAD
            at = lax.rem(new, 2 * tiles)
            first = (new // SUBS) * SUBS + lax.rem(at, tiles) * per

            @pl.when(at < tiles)
            def _():
                for k in range(per):
                    px_recv(first + k, False).wait_recv()

            @pl.when(at >= tiles)
            def _():
                for k in range(per):
                    pz_recv(first + k, False).wait_recv()
            far_loads(new)

        @pl.when(step >= 1)
        def _():
            far_wait(num - SUBS)
            at = tile_cols(num)
            acc[:, at] += jnp.dot(a_v[step - 1], b_v[slot_of(step - 1), :, at], preferred_element_type=jnp.float32)

    @pl.loop(0, steps)
    def _(step):
        a_load(step, 0).start()
        a_load(step, 1).start()

    barrier = pltpu.get_barrier_semaphore()
    for dev in (dev_x, dev_y, dev_z, dev_p):
        pl.semaphore_signal(barrier, inc=1, device_id=dev, device_id_type=MESH)
    pl.semaphore_wait(barrier, 4)

    @pl.loop(0, AHEAD)
    def _(num):
        x_send(num, False).start()

    own_send(0).start()
    own_send(1).start()

    @pl.loop(0, steps)
    def _(step):
        a_load_wait(step)
        a_send(step).start()

    @pl.loop(0, cols // TILE)
    def _(tile):
        at = pl.ds(pl.multiple_of(tile * TILE, TILE), TILE)
        acc[:, at] = jnp.zeros((rows_c, TILE), jnp.float32)

    @pl.loop(0, body)
    def _(num):
        x_recv(num, False).wait_recv()
        z_send(num, False).start()
        px_send(num, False).start()

        @pl.when(num + AHEAD < body)
        def _():
            x_send(num + AHEAD, False).start()

        @pl.when((num + AHEAD >= body) & (num + AHEAD < count))
        def _():
            x_send(num + AHEAD, True).start()

        @pl.when((num + AHEAD >= count) & (num + AHEAD < count + SHIFT))
        def _():
            x_send_extra(num + AHEAD - SHIFT).start()

        @pl.when(num >= LAG)
        def _():
            z_recv(num - LAG, False).wait_recv()
            pz_send(num - LAG, False).start()

        work(num, True)

    @pl.loop(body, count)
    def _(num):
        x_recv(num, True).wait_recv()

        @pl.when(num < count - SHIFT)
        def _():
            z_send(num, True).start()
        px_send(num, True).start()

        @pl.when(num < body + LAG)
        def _():
            z_recv(num - LAG, False).wait_recv()
            pz_send(num - LAG, False).start()

        @pl.when(num >= body + LAG)
        def _():
            z_recv(num - LAG, True).wait_recv()
            pz_send(num - LAG, True).start()

        work(num, False)

    def relay_out(num):
        z_recv(num, True).wait_recv()
        pz_send(num, True).start()

    relay_out(count - 4)
    a_recv(last).wait_recv()
    near_wait(last, 2)
    wide = half // WIDE
    for part in range(2 * wide):
        which = depth if part < wide else 1 - depth
        first = (part % wide) * (WIDE // width)
        for k in range(WIDE // width):
            if part < wide:
                px_recv(body + first + k, True).wait_recv()
            else:
                pz_recv(body + first + k, True).wait_recv()
        at = pl.ds(pl.multiple_of(which * half + (part % wide) * WIDE, WIDE), WIDE)
        total = acc[:, at] + jnp.dot(a_v[last], b_v[2, :, at], preferred_element_type=jnp.float32)
        o_v[:, at] = total.astype(o_v.dtype)
        if part < 3:
            relay_out(count - 3 + part)

    @pl.loop(0, body)
    def _(num):
        x_send(num, False).wait_send()
        z_send(num, False).wait_send()
        px_send(num, False).wait_send()
        pz_send(num, False).wait_send()

    @pl.loop(body, count)
    def _(num):
        x_send(num, True).wait_send()
        z_send(num, True).wait_send()
        px_send(num, True).wait_send()
        pz_send(num, True).wait_send()

    @pl.loop(0, steps)
    def _(step):
        a_send(step).wait_send()
        own_send(step).wait_send()


def solution(mesh):
    def local_mm(a_blk, b_blk):
        band, cols = b_blk.shape
        rows_c = a_blk.shape[0] // 2
        steps = band // GROUP
        count = steps * SUBS
        any_spec = pl.BlockSpec(memory_space=pl.ANY)
        dma = pltpu.SemaphoreType.DMA
        c_blk, _ = pl.pallas_call(
            kernel,
            out_shape=(pltpu.VMEM((rows_c, cols), jnp.bfloat16),
                       jax.ShapeDtypeStruct((4 * band, cols), jnp.bfloat16)),
            in_specs=[any_spec] * 2,
            out_specs=(pl.BlockSpec(memory_space=pltpu.VMEM), any_spec),
            scratch_shapes=[
                pltpu.VMEM((steps, rows_c, 4 * GROUP), jnp.bfloat16),
                pltpu.VMEM((rows_c, cols), jnp.float32),
                pltpu.VMEM((3, 4 * GROUP, cols), jnp.bfloat16),
                dma((steps,)), dma((steps,)), dma((steps,)),
                dma((count,)), dma((count,)), dma((count,)), dma((count,)),
                dma((steps,)), dma((steps,)),
                dma((count,)), dma((count,)), dma((count,)), dma((count,)),
                dma((SUBS,)), dma((2,)),
            ],
            compiler_params=pltpu.CompilerParams(
                collective_id=0, has_side_effects=True, vmem_limit_bytes=52 * 1024 * 1024),
            cost_estimate=pl.CostEstimate(
                flops=2 * rows_c * cols * 2 * cols, bytes_accessed=200 * 2 ** 20, transcendentals=0),
        )(a_blk, b_blk)
        return c_blk

    return jax.shard_map(
        local_mm, mesh=mesh, in_specs=(P("row", "col"), P("row", "col")),
        out_specs=P(("row", "depth"), "col"), check_vma=False)
```

```python
import jax
import jax.numpy as jnp
from jax import lax
from jax.experimental import pallas as pl
from jax.experimental.pallas import tpu as pltpu
from jax.sharding import PartitionSpec as P

MESH = pl.DeviceIdType.MESH
GROUP = 128
SUBS = 8
AHEAD = 12
LAG = 4
SHIFT = 2
LOAD = 6
TILE = 512
WIDE = 1024


def kernel(a_ref, b_ref, o_v, ball, a_v, acc, b_v,
           load_a, send_a, recv_a, send_x, recv_x, send_z, recv_z, send_own, recv_own,
           send_px, recv_px, send_pz, recv_pz, load_far, load_near):
    depth = lax.axis_index("depth")
    col = lax.axis_index("col")
    row = lax.axis_index("row")
    core = lax.rem(row, 2)
    chip_x = row // 2
    rows_c = a_ref.shape[0] // 2
    band = b_ref.shape[0]
    cols = b_ref.shape[1]
    steps = band // GROUP
    last = steps - 1
    half = cols // 2
    width = half // SUBS
    count = steps * SUBS
    body = count - SUBS
    per = TILE // width
    tiles = half // TILE

    row_far = lax.rem(row + 2, 4)
    row_peer = chip_x * 2 + (1 - core)
    row_far_peer = lax.rem(row_peer + 2, 4)
    dev_x = (depth, col, row_far)
    dev_y = (depth, 1 - col, row)
    dev_z = (1 - depth, col, row)
    dev_p = (depth, col, row_peer)
    near = chip_x * 2 * GROUP
    far = (1 - chip_x) * 2 * GROUP

    def slot_of(step):
        return lax.rem(step, 2)

    def remote(src, dst, send, recv, num, dev):
        return pltpu.make_async_remote_copy(
            src, dst, send.at[num], recv.at[num], device_id=dev, device_id_type=MESH)

    def a_cols(step, side):
        return a_v.at[step, :, pl.ds(side * 2 * GROUP, 2 * GROUP)]

    def a_load(step, part):
        return pltpu.make_async_copy(
            a_ref.at[pl.ds(depth * rows_c, rows_c), pl.ds(part * band + step * GROUP, GROUP)],
            a_v.at[step, :, pl.ds(col * 2 * GROUP + part * GROUP, GROUP)], load_a.at[step])

    def a_load_wait(step):
        pltpu.make_async_copy(a_cols(step, col), a_cols(step, col), load_a.at[step]).wait()

    def a_send(step):
        return remote(a_cols(step, col), a_cols(step, col), send_a, recv_a, step, dev_y)

    def a_recv(step):
        return remote(a_cols(step, 1 - col), a_cols(step, 1 - col), send_a, recv_a, step, dev_y)

    def piece(band_row, num, which):
        return ball.at[pl.ds(band_row * band + (num // SUBS) * GROUP, GROUP),
                       pl.ds(which * half + lax.rem(num, SUBS) * width, width)]

    def last_piece(core_of, num, which, first=far):
        return b_v.at[2, pl.ds(first + core_of * GROUP, GROUP),
                      pl.ds(which * half + lax.rem(num, SUBS) * width, width)]

    def source(num, which):
        return b_ref.at[pl.ds((num // SUBS) * GROUP, GROUP),
                        pl.ds(which * half + lax.rem(num, SUBS) * width, width)]

    def mine(num, which, is_last):
        return last_piece(core, num, which) if is_last else piece(row_far, num, which)

    def peers(num, which, is_last):
        return last_piece(1 - core, num, which) if is_last else piece(row_far_peer, num, which)

    def x_send(num, is_last):
        dst = last_piece(core, num, depth, near) if is_last else piece(row, num, depth)
        return remote(source(num, depth), dst, send_x, recv_x, num, dev_x)

    def x_send_extra(num):
        return remote(source(num, 1 - depth), last_piece(core, num, 1 - depth, near), send_z, recv_z, num, dev_x)

    def x_recv(num, is_last):
        here = mine(num, depth, is_last)
        return remote(here, here, send_x, recv_x, num, dev_x)

    def z_send(num, is_last):
        here = mine(num, depth, is_last)
        return remote(here, here, send_z, recv_z, num, dev_z)

    def z_recv(num, is_last):
        here = mine(num, 1 - depth, is_last)
        return remote(here, here, send_z, recv_z, num, dev_z)

    def px_send(num, is_last):
        here = mine(num, depth, is_last)
        return remote(here, here, send_px, recv_px, num, dev_p)

    def px_recv(num, is_last):
        here = peers(num, depth, is_last)
        return remote(here, here, send_px, recv_px, num, dev_p)

    def pz_send(num, is_last):
        here = mine(num, 1 - depth, is_last)
        return remote(here, here, send_pz, recv_pz, num, dev_p)

    def pz_recv(num, is_last):
        here = peers(num, 1 - depth, is_last)
        return remote(here, here, send_pz, recv_pz, num, dev_p)

    def own_send(step):
        return remote(
            b_ref.at[pl.ds(step * GROUP, GROUP), :], ball.at[pl.ds(row * band + step * GROUP, GROUP), :],
            send_own, recv_own, step, dev_p)

    def own_recv(step):
        here = ball.at[pl.ds(row_peer * band + step * GROUP, GROUP), :]
        return remote(here, here, send_own, recv_own, step, dev_p)

    def near_loads(step, slot):
        pltpu.make_async_copy(
            b_ref.at[pl.ds(step * GROUP, GROUP), :],
            b_v.at[slot, pl.ds(near + core * GROUP, GROUP), :], load_near.at[lax.rem(step, 2)]).start()
        pltpu.make_async_copy(
            ball.at[pl.ds(row_peer * band + step * GROUP, GROUP), :],
            b_v.at[slot, pl.ds(near + (1 - core) * GROUP, GROUP), :], load_near.at[lax.rem(step, 2)]).start()

    def near_wait(step, slot):
        here = b_v.at[slot, pl.ds(near, 2 * GROUP), :]
        pltpu.make_async_copy(here, here, load_near.at[lax.rem(step, 2)]).wait()

    def tile_cols(num):
        at = lax.rem(num, 2 * tiles)
        which = jnp.where(at < tiles, depth, 1 - depth)
        return pl.ds(pl.multiple_of(which * half + lax.rem(at, tiles) * TILE, TILE), TILE)

    def far_loads(num):
        step = num // SUBS
        slot = slot_of(step)
        at = tile_cols(num)
        for band_row, part in ((row_far, core), (row_far_peer, 1 - core)):
            pltpu.make_async_copy(
                ball.at[pl.ds(band_row * band + step * GROUP, GROUP), at],
                b_v.at[slot, pl.ds(far + part * GROUP, GROUP), at], load_far.at[lax.rem(num, SUBS)]).start()

    def far_wait(num):
        here = b_v.at[slot_of(num // SUBS), pl.ds(far, 2 * GROUP), tile_cols(num)]
        pltpu.make_async_copy(here, here, load_far.at[lax.rem(num, SUBS)]).wait()

    def work(num, to_load):
        step = num // SUBS
        sub = lax.rem(num, SUBS)

        @pl.when(sub == 0)
        def _():
            own_recv(step).wait_recv()
            if to_load:
                near_loads(step, slot_of(step))

                @pl.when(step + 2 < steps)
                def _():
                    own_send(step + 2).start()
            else:
                near_loads(step, 2)

            @pl.when(step >= 1)
            def _():
                a_recv(step - 1).wait_recv()
                near_wait(step - 1, slot_of(step - 1))

        @pl.when((num >= LOAD) & (num < body + LOAD))
        def _():
            new = num - LOAD
            at = lax.rem(new, 2 * tiles)
            first = (new // SUBS) * SUBS + lax.rem(at, tiles) * per

            @pl.when(at < tiles)
            def _():
                for k in range(per):
                    px_recv(first + k, False).wait_recv()

            @pl.when(at >= tiles)
            def _():
                for k in range(per):
                    pz_recv(first + k, False).wait_recv()
            far_loads(new)

        @pl.when(step >= 1)
        def _():
            far_wait(num - SUBS)
            at = tile_cols(num)
            acc[:, at] += jnp.dot(a_v[step - 1], b_v[slot_of(step - 1), :, at], preferred_element_type=jnp.float32)

    @pl.loop(0, steps)
    def _(step):
        a_load(step, 0).start()
        a_load(step, 1).start()

    barrier = pltpu.get_barrier_semaphore()
    for dev in (dev_x, dev_y, dev_z, dev_p):
        pl.semaphore_signal(barrier, inc=1, device_id=dev, device_id_type=MESH)
    pl.semaphore_wait(barrier, 4)

    @pl.when(core == 0)
    def _():
        x_send(0, False).start()

    @pl.when(core == 1)
    def _():
        for k in range(2):
            rows = pl.ds(k * GROUP // 2, GROUP // 2)
            remote(source(0, depth).at[rows], piece(row, 0, depth).at[rows], send_x, recv_x, 0, dev_x).start()

    @pl.loop(1, AHEAD)
    def _(num):
        x_send(num, False).start()

    own_send(0).start()
    own_send(1).start()

    @pl.loop(0, steps)
    def _(step):
        a_load_wait(step)
        a_send(step).start()

    @pl.loop(0, cols // TILE)
    def _(tile):
        at = pl.ds(pl.multiple_of(tile * TILE, TILE), TILE)
        acc[:, at] = jnp.zeros((rows_c, TILE), jnp.float32)

    @pl.loop(0, body)
    def _(num):
        x_recv(num, False).wait_recv()
        z_send(num, False).start()
        px_send(num, False).start()

        @pl.when(num + AHEAD < body)
        def _():
            x_send(num + AHEAD, False).start()

        @pl.when((num + AHEAD >= body) & (num + AHEAD < count))
        def _():
            x_send(num + AHEAD, True).start()

        @pl.when((num + AHEAD >= count) & (num + AHEAD < count + SHIFT))
        def _():
            x_send_extra(num + AHEAD - SHIFT).start()

        @pl.when(num >= LAG)
        def _():
            z_recv(num - LAG, False).wait_recv()
            pz_send(num - LAG, False).start()

        work(num, True)

    @pl.loop(body, count)
    def _(num):
        x_recv(num, True).wait_recv()

        @pl.when(num < count - SHIFT)
        def _():
            z_send(num, True).start()
        px_send(num, True).start()

        @pl.when(num < body + LAG)
        def _():
            z_recv(num - LAG, False).wait_recv()
            pz_send(num - LAG, False).start()

        @pl.when(num >= body + LAG)
        def _():
            z_recv(num - LAG, True).wait_recv()
            pz_send(num - LAG, True).start()

        work(num, False)

    def relay_out(num):
        z_recv(num, True).wait_recv()
        pz_send(num, True).start()

    relay_out(count - 4)
    a_recv(last).wait_recv()
    near_wait(last, 2)
    wide = half // WIDE
    for part in range(2 * wide):
        which = depth if part < wide else 1 - depth
        first = (part % wide) * (WIDE // width)
        for k in range(WIDE // width):
            if part < wide:
                px_recv(body + first + k, True).wait_recv()
            else:
                pz_recv(body + first + k, True).wait_recv()
        at = pl.ds(pl.multiple_of(which * half + (part % wide) * WIDE, WIDE), WIDE)
        total = acc[:, at] + jnp.dot(a_v[last], b_v[2, :, at], preferred_element_type=jnp.float32)
        o_v[:, at] = total.astype(o_v.dtype)
        if part < 3:
            relay_out(count - 3 + part)

    @pl.loop(0, body)
    def _(num):
        x_send(num, False).wait_send()
        z_send(num, False).wait_send()
        px_send(num, False).wait_send()
        pz_send(num, False).wait_send()

    @pl.loop(body, count)
    def _(num):
        x_send(num, True).wait_send()
        z_send(num, True).wait_send()
        px_send(num, True).wait_send()
        pz_send(num, True).wait_send()

    @pl.loop(0, steps)
    def _(step):
        a_send(step).wait_send()
        own_send(step).wait_send()


def solution(mesh):
    def local_mm(a_blk, b_blk):
        band, cols = b_blk.shape
        rows_c = a_blk.shape[0] // 2
        steps = band // GROUP
        count = steps * SUBS
        any_spec = pl.BlockSpec(memory_space=pl.ANY)
        dma = pltpu.SemaphoreType.DMA
        c_blk, _ = pl.pallas_call(
            kernel,
            out_shape=(pltpu.VMEM((rows_c, cols), jnp.bfloat16),
                       jax.ShapeDtypeStruct((4 * band, cols), jnp.bfloat16)),
            in_specs=[any_spec] * 2,
            out_specs=(pl.BlockSpec(memory_space=pltpu.VMEM), any_spec),
            scratch_shapes=[
                pltpu.VMEM((steps, rows_c, 4 * GROUP), jnp.bfloat16),
                pltpu.VMEM((rows_c, cols), jnp.float32),
                pltpu.VMEM((3, 4 * GROUP, cols), jnp.bfloat16),
                dma((steps,)), dma((steps,)), dma((steps,)),
                dma((count,)), dma((count,)), dma((count,)), dma((count,)),
                dma((steps,)), dma((steps,)),
                dma((count,)), dma((count,)), dma((count,)), dma((count,)),
                dma((SUBS,)), dma((2,)),
            ],
            compiler_params=pltpu.CompilerParams(
                collective_id=0, has_side_effects=True, vmem_limit_bytes=52 * 1024 * 1024),
            cost_estimate=pl.CostEstimate(
                flops=2 * rows_c * cols * 2 * cols, bytes_accessed=200 * 2 ** 20, transcendentals=0),
        )(a_blk, b_blk)
        return c_blk

    return jax.shard_map(
        local_mm, mesh=mesh, in_specs=(P("row", "col"), P("row", "col")),
        out_specs=P(("row", "depth"), "col"), check_vma=False)
```

```python
import jax
import jax.numpy as jnp
from jax import lax
from jax.experimental import pallas as pl
from jax.experimental.pallas import tpu as pltpu
from jax.sharding import PartitionSpec as P

MESH = pl.DeviceIdType.MESH
GROUP = 128
SUBS = 4
AHEAD = 6
LAG = 2
SHIFT = 1
LOAD = 3
TILE = 1024
WIDE = 1024


def kernel(a_ref, b_ref, o_v, ball, a_v, acc, b_v,
           load_a, send_a, recv_a, send_x, recv_x, send_z, recv_z, send_own, recv_own,
           send_px, recv_px, send_pz, recv_pz, load_far, load_near):
    depth = lax.axis_index("depth")
    col = lax.axis_index("col")
    row = lax.axis_index("row")
    core = lax.rem(row, 2)
    chip_x = row // 2
    rows_c = a_ref.shape[0] // 2
    band = b_ref.shape[0]
    cols = b_ref.shape[1]
    steps = band // GROUP
    last = steps - 1
    half = cols // 2
    width = half // SUBS
    count = steps * SUBS
    body = count - SUBS
    per = TILE // width
    tiles = half // TILE

    row_far = lax.rem(row + 2, 4)
    row_peer = chip_x * 2 + (1 - core)
    row_far_peer = lax.rem(row_peer + 2, 4)
    dev_x = (depth, col, row_far)
    dev_y = (depth, 1 - col, row)
    dev_z = (1 - depth, col, row)
    dev_p = (depth, col, row_peer)
    near = chip_x * 2 * GROUP
    far = (1 - chip_x) * 2 * GROUP

    def slot_of(step):
        return lax.rem(step, 2)

    def remote(src, dst, send, recv, num, dev):
        return pltpu.make_async_remote_copy(
            src, dst, send.at[num], recv.at[num], device_id=dev, device_id_type=MESH)

    def a_cols(step, side):
        return a_v.at[step, :, pl.ds(side * 2 * GROUP, 2 * GROUP)]

    def a_load(step, part):
        return pltpu.make_async_copy(
            a_ref.at[pl.ds(depth * rows_c, rows_c), pl.ds(part * band + step * GROUP, GROUP)],
            a_v.at[step, :, pl.ds(col * 2 * GROUP + part * GROUP, GROUP)], load_a.at[step])

    def a_load_wait(step):
        pltpu.make_async_copy(a_cols(step, col), a_cols(step, col), load_a.at[step]).wait()

    def a_send(step):
        return remote(a_cols(step, col), a_cols(step, col), send_a, recv_a, step, dev_y)

    def a_recv(step):
        return remote(a_cols(step, 1 - col), a_cols(step, 1 - col), send_a, recv_a, step, dev_y)

    def piece(band_row, num, which):
        return ball.at[pl.ds(band_row * band + (num // SUBS) * GROUP, GROUP),
                       pl.ds(which * half + lax.rem(num, SUBS) * width, width)]

    def last_piece(core_of, num, which, first=far):
        return b_v.at[2, pl.ds(first + core_of * GROUP, GROUP),
                      pl.ds(which * half + lax.rem(num, SUBS) * width, width)]

    def source(num, which):
        return b_ref.at[pl.ds((num // SUBS) * GROUP, GROUP),
                        pl.ds(which * half + lax.rem(num, SUBS) * width, width)]

    def mine(num, which, is_last):
        return last_piece(core, num, which) if is_last else piece(row_far, num, which)

    def peers(num, which, is_last):
        return last_piece(1 - core, num, which) if is_last else piece(row_far_peer, num, which)

    def x_send(num, is_last):
        dst = last_piece(core, num, depth, near) if is_last else piece(row, num, depth)
        return remote(source(num, depth), dst, send_x, recv_x, num, dev_x)

    def x_send_extra(num):
        return remote(source(num, 1 - depth), last_piece(core, num, 1 - depth, near), send_z, recv_z, num, dev_x)

    def x_recv(num, is_last):
        here = mine(num, depth, is_last)
        return remote(here, here, send_x, recv_x, num, dev_x)

    def z_send(num, is_last):
        here = mine(num, depth, is_last)
        return remote(here, here, send_z, recv_z, num, dev_z)

    def z_recv(num, is_last):
        here = mine(num, 1 - depth, is_last)
        return remote(here, here, send_z, recv_z, num, dev_z)

    def px_send(num, is_last):
        here = mine(num, depth, is_last)
        return remote(here, here, send_px, recv_px, num, dev_p)

    def px_recv(num, is_last):
        here = peers(num, depth, is_last)
        return remote(here, here, send_px, recv_px, num, dev_p)

    def pz_send(num, is_last):
        here = mine(num, 1 - depth, is_last)
        return remote(here, here, send_pz, recv_pz, num, dev_p)

    def pz_recv(num, is_last):
        here = peers(num, 1 - depth, is_last)
        return remote(here, here, send_pz, recv_pz, num, dev_p)

    def own_send(step):
        return remote(
            b_ref.at[pl.ds(step * GROUP, GROUP), :], ball.at[pl.ds(row * band + step * GROUP, GROUP), :],
            send_own, recv_own, step, dev_p)

    def own_recv(step):
        here = ball.at[pl.ds(row_peer * band + step * GROUP, GROUP), :]
        return remote(here, here, send_own, recv_own, step, dev_p)

    def near_loads(step, slot):
        pltpu.make_async_copy(
            b_ref.at[pl.ds(step * GROUP, GROUP), :],
            b_v.at[slot, pl.ds(near + core * GROUP, GROUP), :], load_near.at[lax.rem(step, 2)]).start()
        pltpu.make_async_copy(
            ball.at[pl.ds(row_peer * band + step * GROUP, GROUP), :],
            b_v.at[slot, pl.ds(near + (1 - core) * GROUP, GROUP), :], load_near.at[lax.rem(step, 2)]).start()

    def near_wait(step, slot):
        here = b_v.at[slot, pl.ds(near, 2 * GROUP), :]
        pltpu.make_async_copy(here, here, load_near.at[lax.rem(step, 2)]).wait()

    def tile_cols(num):
        at = lax.rem(num, 2 * tiles)
        which = jnp.where(at < tiles, depth, 1 - depth)
        return pl.ds(pl.multiple_of(which * half + lax.rem(at, tiles) * TILE, TILE), TILE)

    def far_loads(num):
        step = num // SUBS
        slot = slot_of(step)
        at = tile_cols(num)
        for band_row, part in ((row_far, core), (row_far_peer, 1 - core)):
            pltpu.make_async_copy(
                ball.at[pl.ds(band_row * band + step * GROUP, GROUP), at],
                b_v.at[slot, pl.ds(far + part * GROUP, GROUP), at], load_far.at[lax.rem(num, SUBS)]).start()

    def far_wait(num):
        here = b_v.at[slot_of(num // SUBS), pl.ds(far, 2 * GROUP), tile_cols(num)]
        pltpu.make_async_copy(here, here, load_far.at[lax.rem(num, SUBS)]).wait()

    def work(num, to_load):
        step = num // SUBS
        sub = lax.rem(num, SUBS)

        @pl.when(sub == 0)
        def _():
            own_recv(step).wait_recv()
            if to_load:
                near_loads(step, slot_of(step))

                @pl.when(step + 2 < steps)
                def _():
                    own_send(step + 2).start()
            else:
                near_loads(step, 2)

            @pl.when(step >= 1)
            def _():
                a_recv(step - 1).wait_recv()
                near_wait(step - 1, slot_of(step - 1))

        @pl.when((num >= LOAD) & (num < body + LOAD))
        def _():
            new = num - LOAD
            at = lax.rem(new, 2 * tiles)
            first = (new // SUBS) * SUBS + lax.rem(at, tiles) * per

            @pl.when(at < tiles)
            def _():
                for k in range(per):
                    px_recv(first + k, False).wait_recv()

            @pl.when(at >= tiles)
            def _():
                for k in range(per):
                    pz_recv(first + k, False).wait_recv()
            far_loads(new)

        @pl.when(step >= 1)
        def _():
            far_wait(num - SUBS)
            at = tile_cols(num)
            acc[:, at] += jnp.dot(a_v[step - 1], b_v[slot_of(step - 1), :, at], preferred_element_type=jnp.float32)

    @pl.loop(0, steps)
    def _(step):
        a_load(step, 0).start()
        a_load(step, 1).start()

    barrier = pltpu.get_barrier_semaphore()
    for dev in (dev_x, dev_y, dev_z, dev_p):
        pl.semaphore_signal(barrier, inc=1, device_id=dev, device_id_type=MESH)
    pl.semaphore_wait(barrier, 4)

    @pl.loop(0, AHEAD)
    def _(num):
        x_send(num, False).start()

    own_send(0).start()
    own_send(1).start()

    @pl.loop(0, steps)
    def _(step):
        a_load_wait(step)
        a_send(step).start()

    @pl.loop(0, cols // TILE)
    def _(tile):
        at = pl.ds(pl.multiple_of(tile * TILE, TILE), TILE)
        acc[:, at] = jnp.zeros((rows_c, TILE), jnp.float32)

    @pl.loop(0, body)
    def _(num):
        x_recv(num, False).wait_recv()
        z_send(num, False).start()
        px_send(num, False).start()

        @pl.when(num + AHEAD < body)
        def _():
            x_send(num + AHEAD, False).start()

        @pl.when((num + AHEAD >= body) & (num + AHEAD < count))
        def _():
            x_send(num + AHEAD, True).start()

        @pl.when((num + AHEAD >= count) & (num + AHEAD < count + SHIFT))
        def _():
            x_send_extra(num + AHEAD - SHIFT).start()

        @pl.when(num >= LAG)
        def _():
            z_recv(num - LAG, False).wait_recv()
            pz_send(num - LAG, False).start()

        work(num, True)

    @pl.loop(body, count)
    def _(num):
        x_recv(num, True).wait_recv()

        @pl.when(num < count - SHIFT)
        def _():
            z_send(num, True).start()
        px_send(num, True).start()

        @pl.when(num < body + LAG)
        def _():
            z_recv(num - LAG, False).wait_recv()
            pz_send(num - LAG, False).start()

        @pl.when(num >= body + LAG)
        def _():
            z_recv(num - LAG, True).wait_recv()
            pz_send(num - LAG, True).start()

        work(num, False)

    def relay_out(num):
        z_recv(num, True).wait_recv()
        pz_send(num, True).start()

    for num in range(count - LAG, count - 1):
        relay_out(num)
    a_recv(last).wait_recv()
    near_wait(last, 2)
    wide = half // WIDE
    for part in range(2 * wide):
        which = depth if part < wide else 1 - depth
        first = (part % wide) * (WIDE // width)
        for k in range(WIDE // width):
            if part < wide:
                px_recv(body + first + k, True).wait_recv()
            else:
                pz_recv(body + first + k, True).wait_recv()
        at = pl.ds(pl.multiple_of(which * half + (part % wide) * WIDE, WIDE), WIDE)
        total = acc[:, at] + jnp.dot(a_v[last], b_v[2, :, at], preferred_element_type=jnp.float32)
        o_v[:, at] = total.astype(o_v.dtype)
        if part == 1:
            relay_out(count - 1)

    @pl.loop(0, body)
    def _(num):
        x_send(num, False).wait_send()
        z_send(num, False).wait_send()
        px_send(num, False).wait_send()
        pz_send(num, False).wait_send()

    @pl.loop(body, count)
    def _(num):
        x_send(num, True).wait_send()
        z_send(num, True).wait_send()
        px_send(num, True).wait_send()
        pz_send(num, True).wait_send()

    @pl.loop(0, steps)
    def _(step):
        a_send(step).wait_send()
        own_send(step).wait_send()


def solution(mesh):
    def local_mm(a_blk, b_blk):
        band, cols = b_blk.shape
        rows_c = a_blk.shape[0] // 2
        steps = band // GROUP
        count = steps * SUBS
        any_spec = pl.BlockSpec(memory_space=pl.ANY)
        dma = pltpu.SemaphoreType.DMA
        c_blk, _ = pl.pallas_call(
            kernel,
            out_shape=(pltpu.VMEM((rows_c, cols), jnp.bfloat16),
                       jax.ShapeDtypeStruct((4 * band, cols), jnp.bfloat16)),
            in_specs=[any_spec] * 2,
            out_specs=(pl.BlockSpec(memory_space=pltpu.VMEM), any_spec),
            scratch_shapes=[
                pltpu.VMEM((steps, rows_c, 4 * GROUP), jnp.bfloat16),
                pltpu.VMEM((rows_c, cols), jnp.float32),
                pltpu.VMEM((3, 4 * GROUP, cols), jnp.bfloat16),
                dma((steps,)), dma((steps,)), dma((steps,)),
                dma((count,)), dma((count,)), dma((count,)), dma((count,)),
                dma((steps,)), dma((steps,)),
                dma((count,)), dma((count,)), dma((count,)), dma((count,)),
                dma((SUBS,)), dma((2,)),
            ],
            compiler_params=pltpu.CompilerParams(
                collective_id=0, has_side_effects=True, vmem_limit_bytes=52 * 1024 * 1024),
            cost_estimate=pl.CostEstimate(
                flops=2 * rows_c * cols * 2 * cols, bytes_accessed=200 * 2 ** 20, transcendentals=0),
        )(a_blk, b_blk)
        return c_blk

    return jax.shard_map(
        local_mm, mesh=mesh, in_specs=(P("row", "col"), P("row", "col")),
        out_specs=P(("row", "depth"), "col"), check_vma=False)
```

```python
import jax
import jax.numpy as jnp
from jax import lax
from jax.experimental import pallas as pl
from jax.experimental.pallas import tpu as pltpu
from jax.sharding import PartitionSpec as P

MESH = pl.DeviceIdType.MESH
GROUP = 128
SUBS = 4
AHEAD = 6
LAG = 2
SHIFT = 1
LOAD = 3
TILE = 1024
BACK = 8
WIDE = 1024


def kernel(a_ref, b_ref, o_v, ball, a_v, acc, b_v,
           load_a, send_a, recv_a, send_x, recv_x, send_z, recv_z, send_own, recv_own,
           send_px, recv_px, send_pz, recv_pz, load_far, load_near):
    depth = lax.axis_index("depth")
    col = lax.axis_index("col")
    row = lax.axis_index("row")
    core = lax.rem(row, 2)
    chip_x = row // 2
    rows_c = a_ref.shape[0] // 2
    band = b_ref.shape[0]
    cols = b_ref.shape[1]
    steps = band // GROUP
    last = steps - 1
    half = cols // 2
    width = half // SUBS
    count = steps * SUBS
    body = count - SUBS
    per = TILE // width
    tiles = half // TILE

    row_far = lax.rem(row + 2, 4)
    row_peer = chip_x * 2 + (1 - core)
    row_far_peer = lax.rem(row_peer + 2, 4)
    dev_x = (depth, col, row_far)
    dev_y = (depth, 1 - col, row)
    dev_z = (1 - depth, col, row)
    dev_p = (depth, col, row_peer)
    near = chip_x * 2 * GROUP
    far = (1 - chip_x) * 2 * GROUP

    def slot_of(step):
        return lax.rem(step, 2)

    def remote(src, dst, send, recv, num, dev):
        return pltpu.make_async_remote_copy(
            src, dst, send.at[num], recv.at[num], device_id=dev, device_id_type=MESH)

    def a_cols(step, side):
        return a_v.at[step, :, pl.ds(side * 2 * GROUP, 2 * GROUP)]

    def a_load(step, part):
        return pltpu.make_async_copy(
            a_ref.at[pl.ds(depth * rows_c, rows_c), pl.ds(part * band + step * GROUP, GROUP)],
            a_v.at[step, :, pl.ds(col * 2 * GROUP + part * GROUP, GROUP)], load_a.at[step])

    def a_load_wait(step):
        pltpu.make_async_copy(a_cols(step, col), a_cols(step, col), load_a.at[step]).wait()

    def a_send(step):
        return remote(a_cols(step, col), a_cols(step, col), send_a, recv_a, step, dev_y)

    def a_recv(step):
        return remote(a_cols(step, 1 - col), a_cols(step, 1 - col), send_a, recv_a, step, dev_y)

    def piece(band_row, num, which):
        return ball.at[pl.ds(band_row * band + (num // SUBS) * GROUP, GROUP),
                       pl.ds(which * half + lax.rem(num, SUBS) * width, width)]

    def last_piece(core_of, num, which, first=far):
        return b_v.at[2, pl.ds(first + core_of * GROUP, GROUP),
                      pl.ds(which * half + lax.rem(num, SUBS) * width, width)]

    def source(num, which):
        return b_ref.at[pl.ds((num // SUBS) * GROUP, GROUP),
                        pl.ds(which * half + lax.rem(num, SUBS) * width, width)]

    def mine(num, which, is_last):
        return last_piece(core, num, which) if is_last else piece(row_far, num, which)

    def peers(num, which, is_last):
        return last_piece(1 - core, num, which) if is_last else piece(row_far_peer, num, which)

    def x_send(num, is_last):
        dst = last_piece(core, num, depth, near) if is_last else piece(row, num, depth)
        return remote(source(num, depth), dst, send_x, recv_x, num, dev_x)

    def x_send_extra(num):
        return remote(source(num, 1 - depth), last_piece(core, num, 1 - depth, near), send_z, recv_z, num, dev_x)

    def x_recv(num, is_last):
        here = mine(num, depth, is_last)
        return remote(here, here, send_x, recv_x, num, dev_x)

    def z_send(num, is_last):
        here = mine(num, depth, is_last)
        return remote(here, here, send_z, recv_z, num, dev_z)

    def z_recv(num, is_last):
        here = mine(num, 1 - depth, is_last)
        return remote(here, here, send_z, recv_z, num, dev_z)

    def px_send(num, is_last):
        here = mine(num, depth, is_last)
        return remote(here, here, send_px, recv_px, num, dev_p)

    def px_recv(num, is_last):
        here = peers(num, depth, is_last)
        return remote(here, here, send_px, recv_px, num, dev_p)

    def pz_send(num, is_last):
        here = mine(num, 1 - depth, is_last)
        return remote(here, here, send_pz, recv_pz, num, dev_p)

    def pz_recv(num, is_last):
        here = peers(num, 1 - depth, is_last)
        return remote(here, here, send_pz, recv_pz, num, dev_p)

    def own_send(step):
        return remote(
            b_ref.at[pl.ds(step * GROUP, GROUP), :], ball.at[pl.ds(row * band + step * GROUP, GROUP), :],
            send_own, recv_own, step, dev_p)

    def own_recv(step):
        here = ball.at[pl.ds(row_peer * band + step * GROUP, GROUP), :]
        return remote(here, here, send_own, recv_own, step, dev_p)

    def near_loads(step, slot):
        pltpu.make_async_copy(
            b_ref.at[pl.ds(step * GROUP, GROUP), :],
            b_v.at[slot, pl.ds(near + core * GROUP, GROUP), :], load_near.at[lax.rem(step, 2)]).start()
        pltpu.make_async_copy(
            ball.at[pl.ds(row_peer * band + step * GROUP, GROUP), :],
            b_v.at[slot, pl.ds(near + (1 - core) * GROUP, GROUP), :], load_near.at[lax.rem(step, 2)]).start()

    def near_wait(step, slot):
        here = b_v.at[slot, pl.ds(near, 2 * GROUP), :]
        pltpu.make_async_copy(here, here, load_near.at[lax.rem(step, 2)]).wait()

    def tile_cols(num):
        at = lax.rem(num, 2 * tiles)
        which = jnp.where(at < tiles, depth, 1 - depth)
        return pl.ds(pl.multiple_of(which * half + lax.rem(at, tiles) * TILE, TILE), TILE)

    def far_loads(num):
        step = num // SUBS
        slot = slot_of(step)
        at = tile_cols(num)
        for band_row, part in ((row_far, core), (row_far_peer, 1 - core)):
            pltpu.make_async_copy(
                ball.at[pl.ds(band_row * band + step * GROUP, GROUP), at],
                b_v.at[slot, pl.ds(far + part * GROUP, GROUP), at], load_far.at[lax.rem(num, SUBS)]).start()

    def far_wait(num):
        here = b_v.at[slot_of(num // SUBS), pl.ds(far, 2 * GROUP), tile_cols(num)]
        pltpu.make_async_copy(here, here, load_far.at[lax.rem(num, SUBS)]).wait()

    def sent(num, is_last):
        x_send(num, is_last).wait_send()
        z_send(num, is_last).wait_send()
        px_send(num, is_last).wait_send()
        pz_send(num, is_last).wait_send()

    def work(num, to_load):
        step = num // SUBS
        sub = lax.rem(num, SUBS)

        @pl.when(sub == 0)
        def _():
            own_recv(step).wait_recv()
            if to_load:
                near_loads(step, slot_of(step))

                @pl.when(step + 2 < steps)
                def _():
                    own_send(step + 2).start()
            else:
                near_loads(step, 2)

            @pl.when(step >= 2)
            def _():
                a_send(step - 2).wait_send()
                own_send(step - 2).wait_send()

            @pl.when(step >= 1)
            def _():
                a_recv(step - 1).wait_recv()
                near_wait(step - 1, slot_of(step - 1))

        @pl.when((num >= LOAD) & (num < body + LOAD))
        def _():
            new = num - LOAD
            at = lax.rem(new, 2 * tiles)
            first = (new // SUBS) * SUBS + lax.rem(at, tiles) * per

            @pl.when(at < tiles)
            def _():
                for k in range(per):
                    px_recv(first + k, False).wait_recv()

            @pl.when(at >= tiles)
            def _():
                for k in range(per):
                    pz_recv(first + k, False).wait_recv()
            far_loads(new)

        @pl.when(step >= 1)
        def _():
            far_wait(num - SUBS)
            at = tile_cols(num)
            acc[:, at] += jnp.dot(a_v[step - 1], b_v[slot_of(step - 1), :, at], preferred_element_type=jnp.float32)

        @pl.when(num >= BACK)
        def _():
            sent(num - BACK, False)

    barrier = pltpu.get_barrier_semaphore()
    for dev in (dev_x, dev_y, dev_z, dev_p):
        pl.semaphore_signal(barrier, inc=1, device_id=dev, device_id_type=MESH)

    @pl.loop(0, steps)
    def _(step):
        a_load(step, 0).start()
        a_load(step, 1).start()

    pl.semaphore_wait(barrier, 4)

    @pl.loop(0, AHEAD)
    def _(num):
        x_send(num, False).start()

    own_send(0).start()
    own_send(1).start()

    @pl.loop(0, steps)
    def _(step):
        a_load_wait(step)
        a_send(step).start()

    @pl.loop(0, cols // TILE)
    def _(tile):
        at = pl.ds(pl.multiple_of(tile * TILE, TILE), TILE)
        acc[:, at] = jnp.zeros((rows_c, TILE), jnp.float32)

    @pl.loop(0, body)
    def _(num):
        x_recv(num, False).wait_recv()
        z_send(num, False).start()
        px_send(num, False).start()

        @pl.when(num + AHEAD < body)
        def _():
            x_send(num + AHEAD, False).start()

        @pl.when((num + AHEAD >= body) & (num + AHEAD < count))
        def _():
            x_send(num + AHEAD, True).start()

        @pl.when((num + AHEAD >= count) & (num + AHEAD < count + SHIFT))
        def _():
            x_send_extra(num + AHEAD - SHIFT).start()

        @pl.when(num >= LAG)
        def _():
            z_recv(num - LAG, False).wait_recv()
            pz_send(num - LAG, False).start()

        work(num, True)

    @pl.loop(body, count)
    def _(num):
        x_recv(num, True).wait_recv()

        @pl.when(num < count - SHIFT)
        def _():
            z_send(num, True).start()
        px_send(num, True).start()

        @pl.when(num < body + LAG)
        def _():
            z_recv(num - LAG, False).wait_recv()
            pz_send(num - LAG, False).start()

        @pl.when(num >= body + LAG)
        def _():
            z_recv(num - LAG, True).wait_recv()
            pz_send(num - LAG, True).start()

        work(num, False)

    def relay_out(num):
        z_recv(num, True).wait_recv()
        pz_send(num, True).start()

    for num in range(count - LAG, count - 1):
        relay_out(num)
    a_recv(last).wait_recv()
    near_wait(last, 2)
    wide = half // WIDE
    for part in range(2 * wide):
        which = depth if part < wide else 1 - depth
        first = (part % wide) * (WIDE // width)
        for k in range(WIDE // width):
            if part < wide:
                px_recv(body + first + k, True).wait_recv()
            else:
                pz_recv(body + first + k, True).wait_recv()
        at = pl.ds(pl.multiple_of(which * half + (part % wide) * WIDE, WIDE), WIDE)
        total = acc[:, at] + jnp.dot(a_v[last], b_v[2, :, at], preferred_element_type=jnp.float32)
        o_v[:, at] = total.astype(o_v.dtype)
        if part == 1:
            relay_out(count - 1)

    @pl.loop(count - BACK, body)
    def _(num):
        sent(num, False)

    @pl.loop(body, count)
    def _(num):
        sent(num, True)

    @pl.loop(steps - 2, steps)
    def _(step):
        a_send(step).wait_send()
        own_send(step).wait_send()


def solution(mesh):
    def local_mm(a_blk, b_blk):
        band, cols = b_blk.shape
        rows_c = a_blk.shape[0] // 2
        steps = band // GROUP
        count = steps * SUBS
        any_spec = pl.BlockSpec(memory_space=pl.ANY)
        dma = pltpu.SemaphoreType.DMA
        c_blk, _ = pl.pallas_call(
            kernel,
            out_shape=(pltpu.VMEM((rows_c, cols), jnp.bfloat16),
                       jax.ShapeDtypeStruct((4 * band, cols), jnp.bfloat16)),
            in_specs=[any_spec] * 2,
            out_specs=(pl.BlockSpec(memory_space=pltpu.VMEM), any_spec),
            scratch_shapes=[
                pltpu.VMEM((steps, rows_c, 4 * GROUP), jnp.bfloat16),
                pltpu.VMEM((rows_c, cols), jnp.float32),
                pltpu.VMEM((3, 4 * GROUP, cols), jnp.bfloat16),
                dma((steps,)), dma((steps,)), dma((steps,)),
                dma((count,)), dma((count,)), dma((count,)), dma((count,)),
                dma((steps,)), dma((steps,)),
                dma((count,)), dma((count,)), dma((count,)), dma((count,)),
                dma((SUBS,)), dma((2,)),
            ],
            compiler_params=pltpu.CompilerParams(
                collective_id=0, has_side_effects=True, vmem_limit_bytes=52 * 1024 * 1024),
            cost_estimate=pl.CostEstimate(
                flops=2 * rows_c * cols * 2 * cols, bytes_accessed=200 * 2 ** 20, transcendentals=0),
        )(a_blk, b_blk)
        return c_blk

    return jax.shard_map(
        local_mm, mesh=mesh, in_specs=(P("row", "col"), P("row", "col")),
        out_specs=P(("row", "depth"), "col"), check_vma=False)
```

```python
import jax
import jax.numpy as jnp
from jax import lax
from jax.experimental import pallas as pl
from jax.experimental.pallas import tpu as pltpu
from jax.sharding import PartitionSpec as P

MESH = pl.DeviceIdType.MESH
GROUP = 128
SUBS = 4
AHEAD = 6
LAG = 2
SHIFT = 1
LOAD = 3
TILE = 1024
BACK = 8
WIDE = 1024


def kernel(a_ref, b_ref, o_v, ball, a_v, acc, b_v,
           load_a, send_a, recv_a, send_x, recv_x, send_z, recv_z, send_own, recv_own,
           send_px, recv_px, send_pz, recv_pz, load_far, load_near):
    depth = lax.axis_index("depth")
    col = lax.axis_index("col")
    row = lax.axis_index("row")
    core = lax.rem(row, 2)
    chip_x = row // 2
    rows_c = a_ref.shape[0] // 2
    band = b_ref.shape[0]
    cols = b_ref.shape[1]
    steps = band // GROUP
    last = steps - 1
    half = cols // 2
    width = half // SUBS
    count = steps * SUBS
    body = count - SUBS
    per = TILE // width
    tiles = half // TILE

    row_far = lax.rem(row + 2, 4)
    row_peer = chip_x * 2 + (1 - core)
    row_far_peer = lax.rem(row_peer + 2, 4)
    dev_x = (depth, col, row_far)
    dev_y = (depth, 1 - col, row)
    dev_z = (1 - depth, col, row)
    dev_p = (depth, col, row_peer)
    near = chip_x * 2 * GROUP
    far = (1 - chip_x) * 2 * GROUP

    def slot_of(step):
        return lax.rem(step, 2)

    def remote(src, dst, send, recv, num, dev):
        return pltpu.make_async_remote_copy(
            src, dst, send.at[num], recv.at[num], device_id=dev, device_id_type=MESH)

    def a_cols(step, side):
        return a_v.at[step, :, pl.ds(side * 2 * GROUP, 2 * GROUP)]

    def a_load(step, part):
        return pltpu.make_async_copy(
            a_ref.at[pl.ds(depth * rows_c, rows_c), pl.ds(part * band + step * GROUP, GROUP)],
            a_v.at[step, :, pl.ds(col * 2 * GROUP + part * GROUP, GROUP)], load_a.at[step])

    def a_load_wait(step):
        pltpu.make_async_copy(a_cols(step, col), a_cols(step, col), load_a.at[step]).wait()

    def a_send(step):
        return remote(a_cols(step, col), a_cols(step, col), send_a, recv_a, step, dev_y)

    def a_recv(step):
        return remote(a_cols(step, 1 - col), a_cols(step, 1 - col), send_a, recv_a, step, dev_y)

    def piece(band_row, num, which):
        return ball.at[pl.ds(band_row * band + (num // SUBS) * GROUP, GROUP),
                       pl.ds(which * half + lax.rem(num, SUBS) * width, width)]

    def last_piece(core_of, num, which, first=far):
        return b_v.at[2, pl.ds(first + core_of * GROUP, GROUP),
                      pl.ds(which * half + lax.rem(num, SUBS) * width, width)]

    def source(num, which):
        return b_ref.at[pl.ds((num // SUBS) * GROUP, GROUP),
                        pl.ds(which * half + lax.rem(num, SUBS) * width, width)]

    def mine(num, which, is_last):
        return last_piece(core, num, which) if is_last else piece(row_far, num, which)

    def peers(num, which, is_last):
        return last_piece(1 - core, num, which) if is_last else piece(row_far_peer, num, which)

    def x_send(num, is_last):
        dst = last_piece(core, num, depth, near) if is_last else piece(row, num, depth)
        return remote(source(num, depth), dst, send_x, recv_x, num, dev_x)

    def x_send_extra(num):
        return remote(source(num, 1 - depth), last_piece(core, num, 1 - depth, near), send_z, recv_z, num, dev_x)

    def x_recv(num, is_last):
        here = mine(num, depth, is_last)
        return remote(here, here, send_x, recv_x, num, dev_x)

    def z_send(num, is_last):
        here = mine(num, depth, is_last)
        return remote(here, here, send_z, recv_z, num, dev_z)

    def z_recv(num, is_last):
        here = mine(num, 1 - depth, is_last)
        return remote(here, here, send_z, recv_z, num, dev_z)

    def px_send(num, is_last):
        here = mine(num, depth, is_last)
        return remote(here, here, send_px, recv_px, num, dev_p)

    def px_recv(num, is_last):
        here = peers(num, depth, is_last)
        return remote(here, here, send_px, recv_px, num, dev_p)

    def pz_send(num, is_last):
        here = mine(num, 1 - depth, is_last)
        return remote(here, here, send_pz, recv_pz, num, dev_p)

    def pz_recv(num, is_last):
        here = peers(num, 1 - depth, is_last)
        return remote(here, here, send_pz, recv_pz, num, dev_p)

    def own_send(step):
        return remote(
            b_ref.at[pl.ds(step * GROUP, GROUP), :], ball.at[pl.ds(row * band + step * GROUP, GROUP), :],
            send_own, recv_own, step, dev_p)

    def own_recv(step):
        here = ball.at[pl.ds(row_peer * band + step * GROUP, GROUP), :]
        return remote(here, here, send_own, recv_own, step, dev_p)

    def near_loads(step, slot):
        pltpu.make_async_copy(
            b_ref.at[pl.ds(step * GROUP, GROUP), :],
            b_v.at[slot, pl.ds(near + core * GROUP, GROUP), :], load_near.at[lax.rem(step, 2)]).start()
        pltpu.make_async_copy(
            ball.at[pl.ds(row_peer * band + step * GROUP, GROUP), :],
            b_v.at[slot, pl.ds(near + (1 - core) * GROUP, GROUP), :], load_near.at[lax.rem(step, 2)]).start()

    def near_wait(step, slot):
        here = b_v.at[slot, pl.ds(near, 2 * GROUP), :]
        pltpu.make_async_copy(here, here, load_near.at[lax.rem(step, 2)]).wait()

    def tile_cols(num):
        at = lax.rem(num, 2 * tiles)
        which = jnp.where(at < tiles, depth, 1 - depth)
        return pl.ds(pl.multiple_of(which * half + lax.rem(at, tiles) * TILE, TILE), TILE)

    def far_loads(num):
        step = num // SUBS
        slot = slot_of(step)
        at = tile_cols(num)
        for band_row, part in ((row_far, core), (row_far_peer, 1 - core)):
            pltpu.make_async_copy(
                ball.at[pl.ds(band_row * band + step * GROUP, GROUP), at],
                b_v.at[slot, pl.ds(far + part * GROUP, GROUP), at], load_far.at[lax.rem(num, SUBS)]).start()

    def far_wait(num):
        here = b_v.at[slot_of(num // SUBS), pl.ds(far, 2 * GROUP), tile_cols(num)]
        pltpu.make_async_copy(here, here, load_far.at[lax.rem(num, SUBS)]).wait()

    def sent(num, is_last):
        x_send(num, is_last).wait_send()
        z_send(num, is_last).wait_send()
        px_send(num, is_last).wait_send()
        pz_send(num, is_last).wait_send()

    def multiply(num, slot):
        step = num // SUBS

        @pl.when(lax.rem(num, SUBS) == 0)
        def _():
            own_recv(step).wait_recv()
            near_loads(step, slot)

            @pl.when(step + 2 < steps)
            def _():
                own_send(step + 2).start()

            @pl.when(step >= 1)
            def _():
                a_recv(step - 1).wait_recv()
                near_wait(step - 1, slot_of(step - 1))

        @pl.when(step >= 1)
        def _():
            far_wait(num - SUBS)
            at = tile_cols(num)
            acc[:, at] += jnp.dot(a_v[step - 1], b_v[slot_of(step - 1), :, at], preferred_element_type=jnp.float32)

    def load(num):
        step = num // SUBS

        @pl.when((num >= LOAD) & (num < body + LOAD))
        def _():
            new = num - LOAD
            at = lax.rem(new, 2 * tiles)
            first = (new // SUBS) * SUBS + lax.rem(at, tiles) * per

            @pl.when(at < tiles)
            def _():
                for k in range(per):
                    px_recv(first + k, False).wait_recv()

            @pl.when(at >= tiles)
            def _():
                for k in range(per):
                    pz_recv(first + k, False).wait_recv()
            far_loads(new)

        @pl.when(num >= BACK)
        def _():
            sent(num - BACK, False)

        @pl.when((lax.rem(num, SUBS) == 0) & (step >= 2))
        def _():
            a_send(step - 2).wait_send()
            own_send(step - 2).wait_send()

    barrier = pltpu.get_barrier_semaphore()
    for dev in (dev_x, dev_y, dev_z, dev_p):
        pl.semaphore_signal(barrier, inc=1, device_id=dev, device_id_type=MESH)

    @pl.loop(0, steps)
    def _(step):
        a_load(step, 0).start()
        a_load(step, 1).start()

    pl.semaphore_wait(barrier, 4)

    x_send(0, False).start()
    a_load_wait(0)
    a_send(0).start()

    @pl.loop(1, AHEAD)
    def _(num):
        x_send(num, False).start()

    own_send(0).start()
    own_send(1).start()

    @pl.loop(1, steps)
    def _(step):
        a_load_wait(step)
        a_send(step).start()

    @pl.loop(0, cols // TILE)
    def _(tile):
        at = pl.ds(pl.multiple_of(tile * TILE, TILE), TILE)
        acc[:, at] = jnp.zeros((rows_c, TILE), jnp.float32)

    @pl.loop(0, body)
    def _(num):
        x_recv(num, False).wait_recv()
        z_send(num, False).start()
        px_send(num, False).start()

        @pl.when(num + AHEAD < body)
        def _():
            x_send(num + AHEAD, False).start()

        @pl.when((num + AHEAD >= body) & (num + AHEAD < count))
        def _():
            x_send(num + AHEAD, True).start()

        @pl.when((num + AHEAD >= count) & (num + AHEAD < count + SHIFT))
        def _():
            x_send_extra(num + AHEAD - SHIFT).start()

        multiply(num, slot_of(num // SUBS))

        @pl.when(num >= LAG)
        def _():
            z_recv(num - LAG, False).wait_recv()
            pz_send(num - LAG, False).start()

        load(num)

    @pl.loop(body, count)
    def _(num):
        x_recv(num, True).wait_recv()

        @pl.when(num < count - SHIFT)
        def _():
            z_send(num, True).start()
        px_send(num, True).start()
        multiply(num, 2)

        @pl.when(num < body + LAG)
        def _():
            z_recv(num - LAG, False).wait_recv()
            pz_send(num - LAG, False).start()

        @pl.when(num >= body + LAG)
        def _():
            z_recv(num - LAG, True).wait_recv()
            pz_send(num - LAG, True).start()

        load(num)

    def relay_out(num):
        z_recv(num, True).wait_recv()
        pz_send(num, True).start()

    a_recv(last).wait_recv()
    near_wait(last, 2)
    wide = half // WIDE
    for part in range(2 * wide):
        which = depth if part < wide else 1 - depth
        first = (part % wide) * (WIDE // width)
        for k in range(WIDE // width):
            if part < wide:
                px_recv(body + first + k, True).wait_recv()
            else:
                pz_recv(body + first + k, True).wait_recv()
        at = pl.ds(pl.multiple_of(which * half + (part % wide) * WIDE, WIDE), WIDE)
        total = acc[:, at] + jnp.dot(a_v[last], b_v[2, :, at], preferred_element_type=jnp.float32)
        o_v[:, at] = total.astype(o_v.dtype)
        if part < LAG:
            relay_out(count - LAG + part)

    @pl.loop(count - BACK, body)
    def _(num):
        sent(num, False)

    @pl.loop(body, count)
    def _(num):
        sent(num, True)

    @pl.loop(steps - 2, steps)
    def _(step):
        a_send(step).wait_send()
        own_send(step).wait_send()


def solution(mesh):
    def local_mm(a_blk, b_blk):
        band, cols = b_blk.shape
        rows_c = a_blk.shape[0] // 2
        steps = band // GROUP
        count = steps * SUBS
        any_spec = pl.BlockSpec(memory_space=pl.ANY)
        dma = pltpu.SemaphoreType.DMA
        c_blk, _ = pl.pallas_call(
            kernel,
            out_shape=(pltpu.VMEM((rows_c, cols), jnp.bfloat16),
                       jax.ShapeDtypeStruct((4 * band, cols), jnp.bfloat16)),
            in_specs=[any_spec] * 2,
            out_specs=(pl.BlockSpec(memory_space=pltpu.VMEM), any_spec),
            scratch_shapes=[
                pltpu.VMEM((steps, rows_c, 4 * GROUP), jnp.bfloat16),
                pltpu.VMEM((rows_c, cols), jnp.float32),
                pltpu.VMEM((3, 4 * GROUP, cols), jnp.bfloat16),
                dma((steps,)), dma((steps,)), dma((steps,)),
                dma((count,)), dma((count,)), dma((count,)), dma((count,)),
                dma((steps,)), dma((steps,)),
                dma((count,)), dma((count,)), dma((count,)), dma((count,)),
                dma((SUBS,)), dma((2,)),
            ],
            compiler_params=pltpu.CompilerParams(
                collective_id=0, has_side_effects=True, vmem_limit_bytes=52 * 1024 * 1024),
            cost_estimate=pl.CostEstimate(
                flops=2 * rows_c * cols * 2 * cols, bytes_accessed=200 * 2 ** 20, transcendentals=0),
        )(a_blk, b_blk)
        return c_blk

    return jax.shard_map(
        local_mm, mesh=mesh, in_specs=(P("row", "col"), P("row", "col")),
        out_specs=P(("row", "depth"), "col"), check_vma=False)
```

```python
import jax
import jax.numpy as jnp
from jax import lax
from jax.experimental import pallas as pl
from jax.experimental.pallas import tpu as pltpu
from jax.sharding import PartitionSpec as P

MESH = pl.DeviceIdType.MESH
GROUP = 128
SUBS = 4
AHEAD = 6
LAG = 2
FINE = 8
FINE_LAG = 4
SHIFT = 2
LOAD = 3
TILE = 1024
BACK = 8
HALF_TILE = 512
LOADS = (0, 2, 5)


def kernel(a_ref, b_ref, o_v, ball, a_v, acc, b_v,
           load_a, send_a, recv_a, send_x, recv_x, send_z, recv_z, send_own, recv_own,
           send_px, recv_px, send_pz, recv_pz, load_far, load_near,
           send_xl, recv_xl, send_zl, recv_zl, send_pxl, recv_pxl, send_pzl, recv_pzl):
    depth = lax.axis_index("depth")
    col = lax.axis_index("col")
    row = lax.axis_index("row")
    core = lax.rem(row, 2)
    chip_x = row // 2
    rows_c = a_ref.shape[0] // 2
    band = b_ref.shape[0]
    cols = b_ref.shape[1]
    steps = band // GROUP
    last = steps - 1
    half = cols // 2
    width = half // SUBS
    fine = half // FINE
    body = last * SUBS
    per = TILE // width
    tiles = half // TILE

    row_far = lax.rem(row + 2, 4)
    row_peer = chip_x * 2 + (1 - core)
    row_far_peer = lax.rem(row_peer + 2, 4)
    dev_x = (depth, col, row_far)
    dev_y = (depth, 1 - col, row)
    dev_z = (1 - depth, col, row)
    dev_p = (depth, col, row_peer)
    near = chip_x * 2 * GROUP
    far = (1 - chip_x) * 2 * GROUP

    def slot_of(step):
        return lax.rem(step, 2)

    def remote(src, dst, send, recv, num, dev):
        return pltpu.make_async_remote_copy(
            src, dst, send.at[num], recv.at[num], device_id=dev, device_id_type=MESH)

    def a_cols(step, side):
        return a_v.at[step, :, pl.ds(side * 2 * GROUP, 2 * GROUP)]

    def a_load(step, part):
        return pltpu.make_async_copy(
            a_ref.at[pl.ds(depth * rows_c, rows_c), pl.ds(part * band + step * GROUP, GROUP)],
            a_v.at[step, :, pl.ds(col * 2 * GROUP + part * GROUP, GROUP)], load_a.at[step])

    def a_load_wait(step):
        pltpu.make_async_copy(a_cols(step, col), a_cols(step, col), load_a.at[step]).wait()

    def a_send(step):
        return remote(a_cols(step, col), a_cols(step, col), send_a, recv_a, step, dev_y)

    def a_recv(step):
        return remote(a_cols(step, 1 - col), a_cols(step, 1 - col), send_a, recv_a, step, dev_y)

    def piece(band_row, num, which):
        return ball.at[pl.ds(band_row * band + (num // SUBS) * GROUP, GROUP),
                       pl.ds(which * half + lax.rem(num, SUBS) * width, width)]

    def source(num, which):
        return b_ref.at[pl.ds((num // SUBS) * GROUP, GROUP),
                        pl.ds(which * half + lax.rem(num, SUBS) * width, width)]

    def x_send(num):
        return remote(source(num, depth), piece(row, num, depth), send_x, recv_x, num, dev_x)

    def x_recv(num):
        here = piece(row_far, num, depth)
        return remote(here, here, send_x, recv_x, num, dev_x)

    def z_send(num):
        here = piece(row_far, num, depth)
        return remote(here, here, send_z, recv_z, num, dev_z)

    def z_recv(num):
        here = piece(row_far, num, 1 - depth)
        return remote(here, here, send_z, recv_z, num, dev_z)

    def px_send(num):
        here = piece(row_far, num, depth)
        return remote(here, here, send_px, recv_px, num, dev_p)

    def px_recv(num):
        here = piece(row_far_peer, num, depth)
        return remote(here, here, send_px, recv_px, num, dev_p)

    def pz_send(num):
        here = piece(row_far, num, 1 - depth)
        return remote(here, here, send_pz, recv_pz, num, dev_p)

    def pz_recv(num):
        here = piece(row_far_peer, num, 1 - depth)
        return remote(here, here, send_pz, recv_pz, num, dev_p)

    def last_piece(core_of, num, which, first=far):
        return b_v.at[2, pl.ds(first + core_of * GROUP, GROUP), pl.ds(which * half + num * fine, fine)]

    def last_x_send(num):
        return remote(b_ref.at[pl.ds(last * GROUP, GROUP), pl.ds(depth * half + num * fine, fine)],
                      last_piece(core, num, depth, near), send_xl, recv_xl, num, dev_x)

    def last_x_extra(num):
        return remote(b_ref.at[pl.ds(last * GROUP, GROUP), pl.ds((1 - depth) * half + num * fine, fine)],
                      last_piece(core, num, 1 - depth, near), send_zl, recv_zl, num, dev_x)

    def last_x_recv(num):
        here = last_piece(core, num, depth)
        return remote(here, here, send_xl, recv_xl, num, dev_x)

    def last_z_send(num):
        here = last_piece(core, num, depth)
        return remote(here, here, send_zl, recv_zl, num, dev_z)

    def last_z_recv(num):
        here = last_piece(core, num, 1 - depth)
        return remote(here, here, send_zl, recv_zl, num, dev_z)

    def last_px_send(num):
        here = last_piece(core, num, depth)
        return remote(here, here, send_pxl, recv_pxl, num, dev_p)

    def last_px_recv(num):
        here = last_piece(1 - core, num, depth)
        return remote(here, here, send_pxl, recv_pxl, num, dev_p)

    def last_pz_send(num):
        here = last_piece(core, num, 1 - depth)
        return remote(here, here, send_pzl, recv_pzl, num, dev_p)

    def last_pz_recv(num):
        here = last_piece(1 - core, num, 1 - depth)
        return remote(here, here, send_pzl, recv_pzl, num, dev_p)

    def own_send(step):
        return remote(
            b_ref.at[pl.ds(step * GROUP, GROUP), :], ball.at[pl.ds(row * band + step * GROUP, GROUP), :],
            send_own, recv_own, step, dev_p)

    def own_recv(step):
        here = ball.at[pl.ds(row_peer * band + step * GROUP, GROUP), :]
        return remote(here, here, send_own, recv_own, step, dev_p)

    def near_loads(step, slot):
        pltpu.make_async_copy(
            b_ref.at[pl.ds(step * GROUP, GROUP), :],
            b_v.at[slot, pl.ds(near + core * GROUP, GROUP), :], load_near.at[lax.rem(step, 2)]).start()
        pltpu.make_async_copy(
            ball.at[pl.ds(row_peer * band + step * GROUP, GROUP), :],
            b_v.at[slot, pl.ds(near + (1 - core) * GROUP, GROUP), :], load_near.at[lax.rem(step, 2)]).start()

    def near_wait(step, slot):
        here = b_v.at[slot, pl.ds(near, 2 * GROUP), :]
        pltpu.make_async_copy(here, here, load_near.at[lax.rem(step, 2)]).wait()

    def tile_cols(num):
        at = lax.rem(num, 2 * tiles)
        which = jnp.where(at < tiles, depth, 1 - depth)
        return pl.ds(pl.multiple_of(which * half + lax.rem(at, tiles) * TILE, TILE), TILE)

    def far_loads(num):
        step = num // SUBS
        slot = slot_of(step)
        at = tile_cols(num)
        for band_row, part in ((row_far, core), (row_far_peer, 1 - core)):
            pltpu.make_async_copy(
                ball.at[pl.ds(band_row * band + step * GROUP, GROUP), at],
                b_v.at[slot, pl.ds(far + part * GROUP, GROUP), at], load_far.at[lax.rem(num, SUBS)]).start()

    def far_wait(num):
        here = b_v.at[slot_of(num // SUBS), pl.ds(far, 2 * GROUP), tile_cols(num)]
        pltpu.make_async_copy(here, here, load_far.at[lax.rem(num, SUBS)]).wait()

    def sent(num):
        x_send(num).wait_send()
        z_send(num).wait_send()
        px_send(num).wait_send()
        pz_send(num).wait_send()

    def start_group(step, slot):
        own_recv(step).wait_recv()
        near_loads(step, slot)

        @pl.when(step + 2 < steps)
        def _():
            own_send(step + 2).start()

        @pl.when(step >= 1)
        def _():
            a_recv(step - 1).wait_recv()
            near_wait(step - 1, slot_of(step - 1))

    def add(step, at):
        acc[:, at] += jnp.dot(a_v[step], b_v[slot_of(step), :, at], preferred_element_type=jnp.float32)

    def load(new):
        at = lax.rem(new, 2 * tiles)
        first = (new // SUBS) * SUBS + lax.rem(at, tiles) * per

        @pl.when(at < tiles)
        def _():
            for k in range(per):
                px_recv(first + k).wait_recv()

        @pl.when(at >= tiles)
        def _():
            for k in range(per):
                pz_recv(first + k).wait_recv()
        far_loads(new)

    barrier = pltpu.get_barrier_semaphore()
    for dev in (dev_x, dev_y, dev_z, dev_p):
        pl.semaphore_signal(barrier, inc=1, device_id=dev, device_id_type=MESH)

    @pl.loop(0, steps)
    def _(step):
        a_load(step, 0).start()
        a_load(step, 1).start()

    pl.semaphore_wait(barrier, 4)

    x_send(0).start()
    a_load_wait(0)
    a_send(0).start()

    @pl.loop(1, AHEAD)
    def _(num):
        x_send(num).start()

    own_send(0).start()
    own_send(1).start()

    @pl.loop(1, steps)
    def _(step):
        a_load_wait(step)
        a_send(step).start()

    @pl.loop(0, cols // TILE)
    def _(tile):
        at = pl.ds(pl.multiple_of(tile * TILE, TILE), TILE)
        acc[:, at] = jnp.zeros((rows_c, TILE), jnp.float32)

    @pl.loop(0, body)
    def _(num):
        step = num // SUBS
        x_recv(num).wait_recv()
        z_send(num).start()
        px_send(num).start()

        @pl.when(num + AHEAD < body)
        def _():
            x_send(num + AHEAD).start()

        @pl.when(num + AHEAD >= body)
        def _():
            for k in range(2):
                new = (num + AHEAD - body) * 2 + k

                @pl.when(new < FINE)
                def _():
                    last_x_send(new).start()

                @pl.when((new >= FINE) & (new < FINE + SHIFT))
                def _():
                    last_x_extra(new - SHIFT).start()

        @pl.when(lax.rem(num, SUBS) == 0)
        def _():
            start_group(step, slot_of(step))

        @pl.when(step >= 1)
        def _():
            far_wait(num - SUBS)
            add(step - 1, tile_cols(num))

        @pl.when(num >= LAG)
        def _():
            z_recv(num - LAG).wait_recv()
            pz_send(num - LAG).start()

        @pl.when(num >= LOAD)
        def _():
            load(num - LOAD)

        @pl.when(num >= BACK)
        def _():
            sent(num - BACK)

        @pl.when((lax.rem(num, SUBS) == 0) & (step >= 2))
        def _():
            a_send(step - 2).wait_send()
            own_send(step - 2).wait_send()

    def relay_out(num):
        last_z_recv(num).wait_recv()
        last_pz_send(num).start()

    for num in range(FINE):
        last_x_recv(num).wait_recv()
        if num < FINE - SHIFT:
            last_z_send(num).start()
        last_px_send(num).start()
        if num == 0:
            start_group(last, 2)
        part = num * SUBS // FINE
        if num % (FINE // SUBS) == 0:
            far_wait(body - SUBS + part)
        which = depth if part < tiles else 1 - depth
        add(last - 1, pl.ds(pl.multiple_of(
            which * half + (part % tiles) * TILE + (num % (FINE // SUBS)) * HALF_TILE, HALF_TILE), HALF_TILE))
        if num in (1, 3):
            z_recv(body - LAG + num // 2).wait_recv()
            pz_send(body - LAG + num // 2).start()
        if num >= FINE_LAG:
            relay_out(num - FINE_LAG)
        if num in LOADS:
            load(body - LOAD + LOADS.index(num))

    def finish(which, first, size):
        at = pl.ds(pl.multiple_of(which * half + first, HALF_TILE), size)
        total = acc[:, at] + jnp.dot(a_v[last], b_v[2, :, at], preferred_element_type=jnp.float32)
        o_v[:, at] = total.astype(o_v.dtype)

    a_recv(last).wait_recv()
    near_wait(last, 2)
    for part in range(2):
        for k in range(FINE // 2):
            last_px_recv(part * FINE // 2 + k).wait_recv()
        finish(depth, part * TILE, TILE)
        relay_out(FINE - FINE_LAG + part)
    for part in range(4):
        for k in range(FINE // 4):
            last_pz_recv(part * FINE // 4 + k).wait_recv()
        finish(1 - depth, part * HALF_TILE, HALF_TILE)
        if part < 2:
            relay_out(FINE - FINE_LAG + 2 + part)

    @pl.loop(body - BACK, body)
    def _(num):
        sent(num)

    @pl.loop(0, FINE)
    def _(num):
        last_x_send(num).wait_send()
        last_z_send(num).wait_send()
        last_px_send(num).wait_send()
        last_pz_send(num).wait_send()

    @pl.loop(steps - 3, steps)
    def _(step):
        a_send(step).wait_send()
        own_send(step).wait_send()


def solution(mesh):
    def local_mm(a_blk, b_blk):
        band, cols = b_blk.shape
        rows_c = a_blk.shape[0] // 2
        steps = band // GROUP
        count = (steps - 1) * SUBS
        any_spec = pl.BlockSpec(memory_space=pl.ANY)
        dma = pltpu.SemaphoreType.DMA
        c_blk, _ = pl.pallas_call(
            kernel,
            out_shape=(pltpu.VMEM((rows_c, cols), jnp.bfloat16),
                       jax.ShapeDtypeStruct((4 * band, cols), jnp.bfloat16)),
            in_specs=[any_spec] * 2,
            out_specs=(pl.BlockSpec(memory_space=pltpu.VMEM), any_spec),
            scratch_shapes=[
                pltpu.VMEM((steps, rows_c, 4 * GROUP), jnp.bfloat16),
                pltpu.VMEM((rows_c, cols), jnp.float32),
                pltpu.VMEM((3, 4 * GROUP, cols), jnp.bfloat16),
                dma((steps,)), dma((steps,)), dma((steps,)),
                dma((count,)), dma((count,)), dma((count,)), dma((count,)),
                dma((steps,)), dma((steps,)),
                dma((count,)), dma((count,)), dma((count,)), dma((count,)),
                dma((SUBS,)), dma((2,)),
                *[dma((FINE,))] * 8,
            ],
            compiler_params=pltpu.CompilerParams(
                collective_id=0, has_side_effects=True, vmem_limit_bytes=52 * 1024 * 1024),
            cost_estimate=pl.CostEstimate(
                flops=2 * rows_c * cols * 2 * cols, bytes_accessed=200 * 2 ** 20, transcendentals=0),
        )(a_blk, b_blk)
        return c_blk

    return jax.shard_map(
        local_mm, mesh=mesh, in_specs=(P("row", "col"), P("row", "col")),
        out_specs=P(("row", "depth"), "col"), check_vma=False)
```

```python
import jax
import jax.numpy as jnp
from jax import lax
from jax.experimental import pallas as pl
from jax.experimental.pallas import tpu as pltpu
from jax.sharding import PartitionSpec as P

MESH = pl.DeviceIdType.MESH
GROUP = 128
SUBS = 4
AHEAD = 6
LAG = 2
FINE = 8
FINE_LAG = 3
SHIFT = 2
LOAD = 3
TILE = 1024
BACK = 8
HALF_TILE = 512
LOADS = (0, 2, 5)


def kernel(a_ref, b_ref, o_v, ball, a_v, acc, b_v,
           load_a, send_a, recv_a, send_x, recv_x, send_z, recv_z, send_own, recv_own,
           send_px, recv_px, send_pz, recv_pz, load_far, load_near,
           send_xl, recv_xl, send_zl, recv_zl, send_pxl, recv_pxl, send_pzl, recv_pzl):
    depth = lax.axis_index("depth")
    col = lax.axis_index("col")
    row = lax.axis_index("row")
    core = lax.rem(row, 2)
    chip_x = row // 2
    rows_c = a_ref.shape[0] // 2
    band = b_ref.shape[0]
    cols = b_ref.shape[1]
    steps = band // GROUP
    last = steps - 1
    half = cols // 2
    width = half // SUBS
    fine = half // FINE
    body = last * SUBS
    per = TILE // width
    tiles = half // TILE

    row_far = lax.rem(row + 2, 4)
    row_peer = chip_x * 2 + (1 - core)
    row_far_peer = lax.rem(row_peer + 2, 4)
    dev_x = (depth, col, row_far)
    dev_y = (depth, 1 - col, row)
    dev_z = (1 - depth, col, row)
    dev_p = (depth, col, row_peer)
    near = chip_x * 2 * GROUP
    far = (1 - chip_x) * 2 * GROUP

    def slot_of(step):
        return lax.rem(step, 2)

    def remote(src, dst, send, recv, num, dev):
        return pltpu.make_async_remote_copy(
            src, dst, send.at[num], recv.at[num], device_id=dev, device_id_type=MESH)

    def a_cols(step, side):
        return a_v.at[step, :, pl.ds(side * 2 * GROUP, 2 * GROUP)]

    def a_load(step, part):
        return pltpu.make_async_copy(
            a_ref.at[pl.ds(depth * rows_c, rows_c), pl.ds(part * band + step * GROUP, GROUP)],
            a_v.at[step, :, pl.ds(col * 2 * GROUP + part * GROUP, GROUP)], load_a.at[step])

    def a_load_wait(step):
        pltpu.make_async_copy(a_cols(step, col), a_cols(step, col), load_a.at[step]).wait()

    def a_send(step):
        return remote(a_cols(step, col), a_cols(step, col), send_a, recv_a, step, dev_y)

    def a_recv(step):
        return remote(a_cols(step, 1 - col), a_cols(step, 1 - col), send_a, recv_a, step, dev_y)

    def piece(band_row, num, which):
        return ball.at[pl.ds(band_row * band + (num // SUBS) * GROUP, GROUP),
                       pl.ds(which * half + lax.rem(num, SUBS) * width, width)]

    def source(num, which):
        return b_ref.at[pl.ds((num // SUBS) * GROUP, GROUP),
                        pl.ds(which * half + lax.rem(num, SUBS) * width, width)]

    def x_send(num):
        return remote(source(num, depth), piece(row, num, depth), send_x, recv_x, num, dev_x)

    def x_recv(num):
        here = piece(row_far, num, depth)
        return remote(here, here, send_x, recv_x, num, dev_x)

    def z_send(num):
        here = piece(row_far, num, depth)
        return remote(here, here, send_z, recv_z, num, dev_z)

    def z_recv(num):
        here = piece(row_far, num, 1 - depth)
        return remote(here, here, send_z, recv_z, num, dev_z)

    def px_send(num):
        here = piece(row_far, num, depth)
        return remote(here, here, send_px, recv_px, num, dev_p)

    def px_recv(num):
        here = piece(row_far_peer, num, depth)
        return remote(here, here, send_px, recv_px, num, dev_p)

    def pz_send(num):
        here = piece(row_far, num, 1 - depth)
        return remote(here, here, send_pz, recv_pz, num, dev_p)

    def pz_recv(num):
        here = piece(row_far_peer, num, 1 - depth)
        return remote(here, here, send_pz, recv_pz, num, dev_p)

    def last_piece(core_of, num, which, first=far):
        return b_v.at[2, pl.ds(first + core_of * GROUP, GROUP), pl.ds(which * half + num * fine, fine)]

    def last_x_send(num):
        return remote(b_ref.at[pl.ds(last * GROUP, GROUP), pl.ds(depth * half + num * fine, fine)],
                      last_piece(core, num, depth, near), send_xl, recv_xl, num, dev_x)

    def last_x_extra(num):
        return remote(b_ref.at[pl.ds(last * GROUP, GROUP), pl.ds((1 - depth) * half + num * fine, fine)],
                      last_piece(core, num, 1 - depth, near), send_zl, recv_zl, num, dev_x)

    def last_x_recv(num):
        here = last_piece(core, num, depth)
        return remote(here, here, send_xl, recv_xl, num, dev_x)

    def last_z_send(num):
        here = last_piece(core, num, depth)
        return remote(here, here, send_zl, recv_zl, num, dev_z)

    def last_z_recv(num):
        here = last_piece(core, num, 1 - depth)
        return remote(here, here, send_zl, recv_zl, num, dev_z)

    def last_px_send(num):
        here = last_piece(core, num, depth)
        return remote(here, here, send_pxl, recv_pxl, num, dev_p)

    def last_px_recv(num):
        here = last_piece(1 - core, num, depth)
        return remote(here, here, send_pxl, recv_pxl, num, dev_p)

    def last_pz_send(num):
        here = last_piece(core, num, 1 - depth)
        return remote(here, here, send_pzl, recv_pzl, num, dev_p)

    def last_pz_recv(num):
        here = last_piece(1 - core, num, 1 - depth)
        return remote(here, here, send_pzl, recv_pzl, num, dev_p)

    def own_send(step):
        return remote(
            b_ref.at[pl.ds(step * GROUP, GROUP), :], ball.at[pl.ds(row * band + step * GROUP, GROUP), :],
            send_own, recv_own, step, dev_p)

    def own_recv(step):
        here = ball.at[pl.ds(row_peer * band + step * GROUP, GROUP), :]
        return remote(here, here, send_own, recv_own, step, dev_p)

    def near_loads(step, slot):
        pltpu.make_async_copy(
            b_ref.at[pl.ds(step * GROUP, GROUP), :],
            b_v.at[slot, pl.ds(near + core * GROUP, GROUP), :], load_near.at[lax.rem(step, 2)]).start()
        pltpu.make_async_copy(
            ball.at[pl.ds(row_peer * band + step * GROUP, GROUP), :],
            b_v.at[slot, pl.ds(near + (1 - core) * GROUP, GROUP), :], load_near.at[lax.rem(step, 2)]).start()

    def near_wait(step, slot):
        here = b_v.at[slot, pl.ds(near, 2 * GROUP), :]
        pltpu.make_async_copy(here, here, load_near.at[lax.rem(step, 2)]).wait()

    def tile_cols(num):
        at = lax.rem(num, 2 * tiles)
        which = jnp.where(at < tiles, depth, 1 - depth)
        return pl.ds(pl.multiple_of(which * half + lax.rem(at, tiles) * TILE, TILE), TILE)

    def far_loads(num):
        step = num // SUBS
        slot = slot_of(step)
        at = tile_cols(num)
        for band_row, part in ((row_far, core), (row_far_peer, 1 - core)):
            pltpu.make_async_copy(
                ball.at[pl.ds(band_row * band + step * GROUP, GROUP), at],
                b_v.at[slot, pl.ds(far + part * GROUP, GROUP), at], load_far.at[lax.rem(num, SUBS)]).start()

    def far_wait(num):
        here = b_v.at[slot_of(num // SUBS), pl.ds(far, 2 * GROUP), tile_cols(num)]
        pltpu.make_async_copy(here, here, load_far.at[lax.rem(num, SUBS)]).wait()

    def sent(num):
        x_send(num).wait_send()
        z_send(num).wait_send()
        px_send(num).wait_send()
        pz_send(num).wait_send()

    def start_group(step, slot):
        own_recv(step).wait_recv()
        near_loads(step, slot)

        @pl.when(step + 2 < steps)
        def _():
            own_send(step + 2).start()

        @pl.when(step >= 1)
        def _():
            a_recv(step - 1).wait_recv()
            near_wait(step - 1, slot_of(step - 1))

    def add(step, at):
        acc[:, at] += jnp.dot(a_v[step], b_v[slot_of(step), :, at], preferred_element_type=jnp.float32)

    def load(new):
        at = lax.rem(new, 2 * tiles)
        first = (new // SUBS) * SUBS + lax.rem(at, tiles) * per

        @pl.when(at < tiles)
        def _():
            for k in range(per):
                px_recv(first + k).wait_recv()

        @pl.when(at >= tiles)
        def _():
            for k in range(per):
                pz_recv(first + k).wait_recv()
        far_loads(new)

    barrier = pltpu.get_barrier_semaphore()
    for dev in (dev_x, dev_y, dev_z, dev_p):
        pl.semaphore_signal(barrier, inc=1, device_id=dev, device_id_type=MESH)

    def staged(num):
        return o_v.at[pl.ds(0, GROUP), pl.ds(num * width, width)]

    def stage(num):
        return pltpu.make_async_copy(source(num, depth), staged(num), load_far.at[num])

    a_load(0, 0).start()
    a_load(0, 1).start()
    for num in range(SUBS):
        stage(num).start()
    a_load_wait(0)
    for num in range(SUBS):
        stage(num).wait()
    pl.semaphore_wait(barrier, 4)

    for num in range(SUBS):
        remote(staged(num), piece(row, num, depth), send_x, recv_x, num, dev_x).start()
        if num == 0:
            a_send(0).start()

    @pl.loop(SUBS, AHEAD)
    def _(num):
        x_send(num).start()

    @pl.loop(1, steps)
    def _(step):
        a_load(step, 0).start()
        a_load(step, 1).start()

    own_send(0).start()
    own_send(1).start()

    @pl.loop(1, steps)
    def _(step):
        a_load_wait(step)
        a_send(step).start()

    @pl.loop(0, cols // TILE)
    def _(tile):
        at = pl.ds(pl.multiple_of(tile * TILE, TILE), TILE)
        acc[:, at] = jnp.zeros((rows_c, TILE), jnp.float32)

    @pl.loop(0, body)
    def _(num):
        step = num // SUBS
        x_recv(num).wait_recv()
        z_send(num).start()
        px_send(num).start()

        @pl.when(num + AHEAD < body)
        def _():
            x_send(num + AHEAD).start()

        @pl.when(num + AHEAD >= body)
        def _():
            for k in range(2):
                new = (num + AHEAD - body) * 2 + k

                @pl.when(new < FINE)
                def _():
                    last_x_send(new).start()

                @pl.when((new >= FINE) & (new < FINE + SHIFT))
                def _():
                    last_x_extra(new - SHIFT).start()

        @pl.when(lax.rem(num, SUBS) == 0)
        def _():
            start_group(step, slot_of(step))

        @pl.when(step >= 1)
        def _():
            far_wait(num - SUBS)
            add(step - 1, tile_cols(num))

        @pl.when(num >= LAG)
        def _():
            z_recv(num - LAG).wait_recv()
            pz_send(num - LAG).start()

        @pl.when(num >= LOAD)
        def _():
            load(num - LOAD)

        @pl.when(num >= BACK)
        def _():
            sent(num - BACK)

        @pl.when((lax.rem(num, SUBS) == 0) & (step >= 2))
        def _():
            a_send(step - 2).wait_send()
            own_send(step - 2).wait_send()

    def relay_out(num):
        last_z_recv(num).wait_recv()
        last_pz_send(num).start()

    for num in range(FINE):
        last_x_recv(num).wait_recv()
        if num < FINE - SHIFT:
            last_z_send(num).start()
        last_px_send(num).start()
        if num == 0:
            start_group(last, 2)
        part = num * SUBS // FINE
        if num % (FINE // SUBS) == 0:
            far_wait(body - SUBS + part)
        which = depth if part < tiles else 1 - depth
        add(last - 1, pl.ds(pl.multiple_of(
            which * half + (part % tiles) * TILE + (num % (FINE // SUBS)) * HALF_TILE, HALF_TILE), HALF_TILE))
        if num in (1, 3):
            z_recv(body - LAG + num // 2).wait_recv()
            pz_send(body - LAG + num // 2).start()
        if num >= FINE_LAG:
            relay_out(num - FINE_LAG)
        if num in LOADS:
            load(body - LOAD + LOADS.index(num))

    def finish(which, first, size):
        at = pl.ds(pl.multiple_of(which * half + first, HALF_TILE), size)
        total = acc[:, at] + jnp.dot(a_v[last], b_v[2, :, at], preferred_element_type=jnp.float32)
        o_v[:, at] = total.astype(o_v.dtype)

    for num in range(FINE - FINE_LAG, FINE - 1):
        relay_out(num)
    a_recv(last).wait_recv()
    near_wait(last, 2)
    for part in range(2 * tiles):
        for k in range(FINE // tiles):
            (last_px_recv if part < tiles else last_pz_recv)(part % tiles * FINE // tiles + k).wait_recv()
        finish(depth if part < tiles else 1 - depth, part % tiles * TILE, TILE)
        if part == 0:
            relay_out(FINE - 1)

    @pl.loop(body - BACK, body)
    def _(num):
        sent(num)

    @pl.loop(0, FINE)
    def _(num):
        last_x_send(num).wait_send()
        last_z_send(num).wait_send()
        last_px_send(num).wait_send()
        last_pz_send(num).wait_send()

    @pl.loop(steps - 3, steps)
    def _(step):
        a_send(step).wait_send()
        own_send(step).wait_send()


def solution(mesh):
    def local_mm(a_blk, b_blk):
        band, cols = b_blk.shape
        rows_c = a_blk.shape[0] // 2
        steps = band // GROUP
        count = (steps - 1) * SUBS
        any_spec = pl.BlockSpec(memory_space=pl.ANY)
        dma = pltpu.SemaphoreType.DMA
        c_blk, _ = pl.pallas_call(
            kernel,
            out_shape=(pltpu.VMEM((rows_c, cols), jnp.bfloat16),
                       jax.ShapeDtypeStruct((4 * band, cols), jnp.bfloat16)),
            in_specs=[any_spec] * 2,
            out_specs=(pl.BlockSpec(memory_space=pltpu.VMEM), any_spec),
            scratch_shapes=[
                pltpu.VMEM((steps, rows_c, 4 * GROUP), jnp.bfloat16),
                pltpu.VMEM((rows_c, cols), jnp.float32),
                pltpu.VMEM((3, 4 * GROUP, cols), jnp.bfloat16),
                dma((steps,)), dma((steps,)), dma((steps,)),
                dma((count,)), dma((count,)), dma((count,)), dma((count,)),
                dma((steps,)), dma((steps,)),
                dma((count,)), dma((count,)), dma((count,)), dma((count,)),
                dma((SUBS,)), dma((2,)),
                *[dma((FINE,))] * 8,
            ],
            compiler_params=pltpu.CompilerParams(
                collective_id=0, has_side_effects=True, vmem_limit_bytes=52 * 1024 * 1024),
            cost_estimate=pl.CostEstimate(
                flops=2 * rows_c * cols * 2 * cols, bytes_accessed=200 * 2 ** 20, transcendentals=0),
        )(a_blk, b_blk)
        return c_blk

    return jax.shard_map(
        local_mm, mesh=mesh, in_specs=(P("row", "col"), P("row", "col")),
        out_specs=P(("row", "depth"), "col"), check_vma=False)
```

```python
import jax
import jax.numpy as jnp
from jax import lax
from jax.experimental import pallas as pl
from jax.experimental.pallas import tpu as pltpu
from jax.sharding import PartitionSpec as P

MESH = pl.DeviceIdType.MESH
GROUP = 128
SUBS = 4
AHEAD = 6
LAG = 2
FINE = 8
FINE_LAG = 3
SHIFT = 2
LOAD = 3
TILE = 1024
BACK = 8
HALF_TILE = 512
LOADS = (0, 2, 5)


def kernel(a_ref, b_ref, o_v, ball, a_v, acc, b_v,
           load_a, send_a, recv_a, send_x, recv_x, send_z, recv_z, send_own, recv_own,
           send_px, recv_px, send_pz, recv_pz, load_far, load_near,
           send_xl, recv_xl, send_zl, recv_zl, send_pxl, recv_pxl, send_pzl, recv_pzl):
    depth = lax.axis_index("depth")
    col = lax.axis_index("col")
    row = lax.axis_index("row")
    core = lax.rem(row, 2)
    chip_x = row // 2
    rows_c = a_ref.shape[0] // 2
    band = b_ref.shape[0]
    cols = b_ref.shape[1]
    steps = band // GROUP
    last = steps - 1
    half = cols // 2
    width = half // SUBS
    fine = half // FINE
    body = last * SUBS
    per = TILE // width
    tiles = half // TILE

    row_far = lax.rem(row + 2, 4)
    row_peer = chip_x * 2 + (1 - core)
    row_far_peer = lax.rem(row_peer + 2, 4)
    dev_x = (depth, col, row_far)
    dev_y = (depth, 1 - col, row)
    dev_z = (1 - depth, col, row)
    dev_p = (depth, col, row_peer)
    near = chip_x * 2 * GROUP
    far = (1 - chip_x) * 2 * GROUP

    def slot_of(step):
        return lax.rem(step, 2)

    def remote(src, dst, send, recv, num, dev):
        return pltpu.make_async_remote_copy(
            src, dst, send.at[num], recv.at[num], device_id=dev, device_id_type=MESH)

    def a_cols(step, side):
        return a_v.at[step, :, pl.ds(side * 2 * GROUP, 2 * GROUP)]

    def a_load(step, part):
        return pltpu.make_async_copy(
            a_ref.at[pl.ds(depth * rows_c, rows_c), pl.ds(part * band + step * GROUP, GROUP)],
            a_v.at[step, :, pl.ds(col * 2 * GROUP + part * GROUP, GROUP)], load_a.at[step])

    def a_load_wait(step):
        pltpu.make_async_copy(a_cols(step, col), a_cols(step, col), load_a.at[step]).wait()

    def a_send(step):
        return remote(a_cols(step, col), a_cols(step, col), send_a, recv_a, step, dev_y)

    def a_recv(step):
        return remote(a_cols(step, 1 - col), a_cols(step, 1 - col), send_a, recv_a, step, dev_y)

    def piece(band_row, num, which):
        return ball.at[pl.ds(band_row * band + (num // SUBS) * GROUP, GROUP),
                       pl.ds(which * half + lax.rem(num, SUBS) * width, width)]

    def source(num, which):
        return b_ref.at[pl.ds((num // SUBS) * GROUP, GROUP),
                        pl.ds(which * half + lax.rem(num, SUBS) * width, width)]

    def x_send(num):
        return remote(source(num, depth), piece(row, num, depth), send_x, recv_x, num, dev_x)

    def x_recv(num):
        here = piece(row_far, num, depth)
        return remote(here, here, send_x, recv_x, num, dev_x)

    def z_send(num):
        here = piece(row_far, num, depth)
        return remote(here, here, send_z, recv_z, num, dev_z)

    def z_recv(num):
        here = piece(row_far, num, 1 - depth)
        return remote(here, here, send_z, recv_z, num, dev_z)

    def px_send(num):
        here = piece(row_far, num, depth)
        return remote(here, here, send_px, recv_px, num, dev_p)

    def px_recv(num):
        here = piece(row_far_peer, num, depth)
        return remote(here, here, send_px, recv_px, num, dev_p)

    def pz_send(num):
        here = piece(row_far, num, 1 - depth)
        return remote(here, here, send_pz, recv_pz, num, dev_p)

    def pz_recv(num):
        here = piece(row_far_peer, num, 1 - depth)
        return remote(here, here, send_pz, recv_pz, num, dev_p)

    def last_piece(core_of, num, which, first=far):
        return b_v.at[2, pl.ds(first + core_of * GROUP, GROUP), pl.ds(which * half + num * fine, fine)]

    def last_x_send(num):
        return remote(b_ref.at[pl.ds(last * GROUP, GROUP), pl.ds(depth * half + num * fine, fine)],
                      last_piece(core, num, depth, near), send_xl, recv_xl, num, dev_x)

    def last_x_extra(num):
        return remote(b_ref.at[pl.ds(last * GROUP, GROUP), pl.ds((1 - depth) * half + num * fine, fine)],
                      last_piece(core, num, 1 - depth, near), send_zl, recv_zl, num, dev_x)

    def last_x_recv(num):
        here = last_piece(core, num, depth)
        return remote(here, here, send_xl, recv_xl, num, dev_x)

    def last_z_send(num):
        here = last_piece(core, num, depth)
        return remote(here, here, send_zl, recv_zl, num, dev_z)

    def last_z_recv(num):
        here = last_piece(core, num, 1 - depth)
        return remote(here, here, send_zl, recv_zl, num, dev_z)

    def last_px_send(num):
        here = last_piece(core, num, depth)
        return remote(here, here, send_pxl, recv_pxl, num, dev_p)

    def last_px_recv(num):
        here = last_piece(1 - core, num, depth)
        return remote(here, here, send_pxl, recv_pxl, num, dev_p)

    def last_pz_send(num):
        here = last_piece(core, num, 1 - depth)
        return remote(here, here, send_pzl, recv_pzl, num, dev_p)

    def last_pz_recv(num):
        here = last_piece(1 - core, num, 1 - depth)
        return remote(here, here, send_pzl, recv_pzl, num, dev_p)

    def own_send(step):
        return remote(
            b_ref.at[pl.ds(step * GROUP, GROUP), :], ball.at[pl.ds(row * band + step * GROUP, GROUP), :],
            send_own, recv_own, step, dev_p)

    def own_recv(step):
        here = ball.at[pl.ds(row_peer * band + step * GROUP, GROUP), :]
        return remote(here, here, send_own, recv_own, step, dev_p)

    def near_loads(step, slot):
        pltpu.make_async_copy(
            b_ref.at[pl.ds(step * GROUP, GROUP), :],
            b_v.at[slot, pl.ds(near + core * GROUP, GROUP), :], load_near.at[lax.rem(step, 2)]).start()
        pltpu.make_async_copy(
            ball.at[pl.ds(row_peer * band + step * GROUP, GROUP), :],
            b_v.at[slot, pl.ds(near + (1 - core) * GROUP, GROUP), :], load_near.at[lax.rem(step, 2)]).start()

    def near_wait(step, slot):
        here = b_v.at[slot, pl.ds(near, 2 * GROUP), :]
        pltpu.make_async_copy(here, here, load_near.at[lax.rem(step, 2)]).wait()

    def tile_cols(num):
        at = lax.rem(num, 2 * tiles)
        which = jnp.where(at < tiles, depth, 1 - depth)
        return pl.ds(pl.multiple_of(which * half + lax.rem(at, tiles) * TILE, TILE), TILE)

    def far_loads(num):
        step = num // SUBS
        slot = slot_of(step)
        at = tile_cols(num)
        for band_row, part in ((row_far, core), (row_far_peer, 1 - core)):
            pltpu.make_async_copy(
                ball.at[pl.ds(band_row * band + step * GROUP, GROUP), at],
                b_v.at[slot, pl.ds(far + part * GROUP, GROUP), at], load_far.at[lax.rem(num, SUBS)]).start()

    def far_wait(num):
        here = b_v.at[slot_of(num // SUBS), pl.ds(far, 2 * GROUP), tile_cols(num)]
        pltpu.make_async_copy(here, here, load_far.at[lax.rem(num, SUBS)]).wait()

    def sent(num):
        x_send(num).wait_send()
        z_send(num).wait_send()
        px_send(num).wait_send()
        pz_send(num).wait_send()

    def start_group(step, slot):
        own_recv(step).wait_recv()
        near_loads(step, slot)

        @pl.when(step + 2 < steps)
        def _():
            own_send(step + 2).start()

        @pl.when(step >= 1)
        def _():
            a_recv(step - 1).wait_recv()
            near_wait(step - 1, slot_of(step - 1))

    def add(step, at):
        acc[:, at] += jnp.dot(a_v[step], b_v[slot_of(step), :, at], preferred_element_type=jnp.float32)

    def load(new):
        at = lax.rem(new, 2 * tiles)
        first = (new // SUBS) * SUBS + lax.rem(at, tiles) * per

        @pl.when(at < tiles)
        def _():
            for k in range(per):
                px_recv(first + k).wait_recv()

        @pl.when(at >= tiles)
        def _():
            for k in range(per):
                pz_recv(first + k).wait_recv()
        far_loads(new)

    barrier = pltpu.get_barrier_semaphore()
    for dev in (dev_x, dev_y, dev_z, dev_p):
        pl.semaphore_signal(barrier, inc=1, device_id=dev, device_id_type=MESH)

    def staged(num):
        return o_v.at[pl.ds(0, GROUP), pl.ds(num * width, width)]

    def stage(num):
        return pltpu.make_async_copy(source(num, depth), staged(num), load_far.at[num])

    a_load(0, 0).start()
    a_load(0, 1).start()
    for num in range(SUBS):
        stage(num).start()
    a_load_wait(0)
    for num in range(SUBS):
        stage(num).wait()
    pl.semaphore_wait(barrier, 4)

    for num in range(SUBS):
        remote(staged(num), piece(row, num, depth), send_x, recv_x, num, dev_x).start()
        if num == 0:
            a_send(0).start()

    @pl.loop(SUBS, AHEAD)
    def _(num):
        x_send(num).start()

    @pl.loop(1, steps)
    def _(step):
        a_load(step, 0).start()
        a_load(step, 1).start()

    own_send(0).start()
    own_send(1).start()

    @pl.loop(0, body)
    def _(num):
        step = num // SUBS
        x_recv(num).wait_recv()
        z_send(num).start()
        px_send(num).start()

        @pl.when(num + AHEAD < body)
        def _():
            x_send(num + AHEAD).start()

        @pl.when(num + AHEAD >= body)
        def _():
            for k in range(2):
                new = (num + AHEAD - body) * 2 + k

                @pl.when(new < FINE)
                def _():
                    last_x_send(new).start()

                @pl.when((new >= FINE) & (new < FINE + SHIFT))
                def _():
                    last_x_extra(new - SHIFT).start()

        @pl.when((num == 0) | (num == 1))
        def _():
            a_load_wait(num + 1)
            a_send(num + 1).start()

        @pl.when((lax.rem(num, SUBS) == 0) & (step >= 1) & (step + 2 < steps))
        def _():
            a_load_wait(step + 2)
            a_send(step + 2).start()

        @pl.when(lax.rem(num, SUBS) == 0)
        def _():
            start_group(step, slot_of(step))

        @pl.when(step == 0)
        def _():
            acc[:, tile_cols(num)] = jnp.zeros((rows_c, TILE), jnp.float32)

        @pl.when(step >= 1)
        def _():
            far_wait(num - SUBS)
            add(step - 1, tile_cols(num))

        @pl.when(num >= LAG)
        def _():
            z_recv(num - LAG).wait_recv()
            pz_send(num - LAG).start()

        @pl.when(num >= LOAD)
        def _():
            load(num - LOAD)

        @pl.when(num >= BACK)
        def _():
            sent(num - BACK)

        @pl.when((lax.rem(num, SUBS) == 0) & (step >= 2))
        def _():
            a_send(step - 2).wait_send()
            own_send(step - 2).wait_send()

    def relay_out(num):
        last_z_recv(num).wait_recv()
        last_pz_send(num).start()

    for num in range(FINE):
        last_x_recv(num).wait_recv()
        if num < FINE - SHIFT:
            last_z_send(num).start()
        last_px_send(num).start()
        if num == 0:
            start_group(last, 2)
        part = num * SUBS // FINE
        if num % (FINE // SUBS) == 0:
            far_wait(body - SUBS + part)
        which = depth if part < tiles else 1 - depth
        add(last - 1, pl.ds(pl.multiple_of(
            which * half + (part % tiles) * TILE + (num % (FINE // SUBS)) * HALF_TILE, HALF_TILE), HALF_TILE))
        if num in (1, 3):
            z_recv(body - LAG + num // 2).wait_recv()
            pz_send(body - LAG + num // 2).start()
        if num >= FINE_LAG:
            relay_out(num - FINE_LAG)
        if num in LOADS:
            load(body - LOAD + LOADS.index(num))

    def finish(which, first, size):
        at = pl.ds(pl.multiple_of(which * half + first, HALF_TILE), size)
        total = acc[:, at] + jnp.dot(a_v[last], b_v[2, :, at], preferred_element_type=jnp.float32)
        o_v[:, at] = total.astype(o_v.dtype)

    for num in range(FINE - FINE_LAG, FINE - 1):
        relay_out(num)
    a_recv(last).wait_recv()
    near_wait(last, 2)
    for part in range(2 * tiles):
        for k in range(FINE // tiles):
            (last_px_recv if part < tiles else last_pz_recv)(part % tiles * FINE // tiles + k).wait_recv()
        finish(depth if part < tiles else 1 - depth, part % tiles * TILE, TILE)
        if part == 0:
            relay_out(FINE - 1)

    @pl.loop(body - BACK, body)
    def _(num):
        sent(num)

    @pl.loop(0, FINE)
    def _(num):
        last_x_send(num).wait_send()
        last_z_send(num).wait_send()
        last_px_send(num).wait_send()
        last_pz_send(num).wait_send()

    @pl.loop(steps - 3, steps)
    def _(step):
        a_send(step).wait_send()
        own_send(step).wait_send()


def solution(mesh):
    def local_mm(a_blk, b_blk):
        band, cols = b_blk.shape
        rows_c = a_blk.shape[0] // 2
        steps = band // GROUP
        count = (steps - 1) * SUBS
        any_spec = pl.BlockSpec(memory_space=pl.ANY)
        dma = pltpu.SemaphoreType.DMA
        c_blk, _ = pl.pallas_call(
            kernel,
            out_shape=(pltpu.VMEM((rows_c, cols), jnp.bfloat16),
                       jax.ShapeDtypeStruct((4 * band, cols), jnp.bfloat16)),
            in_specs=[any_spec] * 2,
            out_specs=(pl.BlockSpec(memory_space=pltpu.VMEM), any_spec),
            scratch_shapes=[
                pltpu.VMEM((steps, rows_c, 4 * GROUP), jnp.bfloat16),
                pltpu.VMEM((rows_c, cols), jnp.float32),
                pltpu.VMEM((3, 4 * GROUP, cols), jnp.bfloat16),
                dma((steps,)), dma((steps,)), dma((steps,)),
                dma((count,)), dma((count,)), dma((count,)), dma((count,)),
                dma((steps,)), dma((steps,)),
                dma((count,)), dma((count,)), dma((count,)), dma((count,)),
                dma((SUBS,)), dma((2,)),
                *[dma((FINE,))] * 8,
            ],
            compiler_params=pltpu.CompilerParams(
                collective_id=0, has_side_effects=True, vmem_limit_bytes=52 * 1024 * 1024),
            cost_estimate=pl.CostEstimate(
                flops=2 * rows_c * cols * 2 * cols, bytes_accessed=200 * 2 ** 20, transcendentals=0),
        )(a_blk, b_blk)
        return c_blk

    return jax.shard_map(
        local_mm, mesh=mesh, in_specs=(P("row", "col"), P("row", "col")),
        out_specs=P(("row", "depth"), "col"), check_vma=False)
```

```python
import jax
import jax.numpy as jnp
from jax import lax
from jax.experimental import pallas as pl
from jax.experimental.pallas import tpu as pltpu
from jax.sharding import PartitionSpec as P

MESH = pl.DeviceIdType.MESH
GROUP = 128
SUBS = 4
AHEAD = 6
LAG = 2
FINE = 8
FINE_LAG = 3
SHIFT = 2
LOAD = 3
TILE = 1024
BACK = 8
HALF_TILE = 512
LOADS = (0, 2, 5)


def kernel(a_ref, b_ref, o_v, ball, a_v, acc, b_v,
           load_a, send_a, recv_a, send_x, recv_x, send_z, recv_z, send_own, recv_own,
           send_px, recv_px, send_pz, recv_pz, load_far, load_near,
           send_xl, recv_xl, send_zl, recv_zl, send_pxl, recv_pxl, send_pzl, recv_pzl):
    depth = lax.axis_index("depth")
    col = lax.axis_index("col")
    row = lax.axis_index("row")
    core = lax.rem(row, 2)
    chip_x = row // 2
    rows_c = a_ref.shape[0] // 2
    band = b_ref.shape[0]
    cols = b_ref.shape[1]
    steps = band // GROUP
    last = steps - 1
    half = cols // 2
    width = half // SUBS
    fine = half // FINE
    body = last * SUBS
    per = TILE // width
    tiles = half // TILE

    row_far = lax.rem(row + 2, 4)
    row_peer = chip_x * 2 + (1 - core)
    row_far_peer = lax.rem(row_peer + 2, 4)
    dev_x = (depth, col, row_far)
    dev_y = (depth, 1 - col, row)
    dev_z = (1 - depth, col, row)
    dev_p = (depth, col, row_peer)
    near = chip_x * 2 * GROUP
    far = (1 - chip_x) * 2 * GROUP

    def slot_of(step):
        return lax.rem(step, 2)

    def remote(src, dst, send, recv, num, dev):
        return pltpu.make_async_remote_copy(
            src, dst, send.at[num], recv.at[num], device_id=dev, device_id_type=MESH)

    def a_cols(step, side):
        return a_v.at[step, :, pl.ds(side * 2 * GROUP, 2 * GROUP)]

    def a_load(step, part):
        return pltpu.make_async_copy(
            a_ref.at[pl.ds(depth * rows_c, rows_c), pl.ds(part * band + step * GROUP, GROUP)],
            a_v.at[step, :, pl.ds(col * 2 * GROUP + part * GROUP, GROUP)], load_a.at[step])

    def a_load_wait(step):
        pltpu.make_async_copy(a_cols(step, col), a_cols(step, col), load_a.at[step]).wait()

    def a_send(step):
        return remote(a_cols(step, col), a_cols(step, col), send_a, recv_a, step, dev_y)

    def a_recv(step):
        return remote(a_cols(step, 1 - col), a_cols(step, 1 - col), send_a, recv_a, step, dev_y)

    def piece(band_row, num, which):
        return ball.at[pl.ds(band_row * band + (num // SUBS) * GROUP, GROUP),
                       pl.ds(which * half + lax.rem(num, SUBS) * width, width)]

    def source(num, which):
        return b_ref.at[pl.ds((num // SUBS) * GROUP, GROUP),
                        pl.ds(which * half + lax.rem(num, SUBS) * width, width)]

    def x_send(num):
        return remote(source(num, depth), piece(row, num, depth), send_x, recv_x, num, dev_x)

    def x_recv(num):
        here = piece(row_far, num, depth)
        return remote(here, here, send_x, recv_x, num, dev_x)

    def z_send(num):
        here = piece(row_far, num, depth)
        return remote(here, here, send_z, recv_z, num, dev_z)

    def z_recv(num):
        here = piece(row_far, num, 1 - depth)
        return remote(here, here, send_z, recv_z, num, dev_z)

    def px_send(num):
        here = piece(row_far, num, depth)
        return remote(here, here, send_px, recv_px, num, dev_p)

    def px_recv(num):
        here = piece(row_far_peer, num, depth)
        return remote(here, here, send_px, recv_px, num, dev_p)

    def pz_send(num):
        here = piece(row_far, num, 1 - depth)
        return remote(here, here, send_pz, recv_pz, num, dev_p)

    def pz_recv(num):
        here = piece(row_far_peer, num, 1 - depth)
        return remote(here, here, send_pz, recv_pz, num, dev_p)

    def last_piece(core_of, num, which, first=far):
        return b_v.at[2, pl.ds(first + core_of * GROUP, GROUP), pl.ds(which * half + num * fine, fine)]

    def last_x_send(num):
        return remote(b_ref.at[pl.ds(last * GROUP, GROUP), pl.ds(depth * half + num * fine, fine)],
                      last_piece(core, num, depth, near), send_xl, recv_xl, num, dev_x)

    def last_x_extra(num):
        return remote(b_ref.at[pl.ds(last * GROUP, GROUP), pl.ds((1 - depth) * half + num * fine, fine)],
                      last_piece(core, num, 1 - depth, near), send_zl, recv_zl, num, dev_x)

    def last_x_recv(num):
        here = last_piece(core, num, depth)
        return remote(here, here, send_xl, recv_xl, num, dev_x)

    def last_z_send(num):
        here = last_piece(core, num, depth)
        return remote(here, here, send_zl, recv_zl, num, dev_z)

    def last_z_recv(num):
        here = last_piece(core, num, 1 - depth)
        return remote(here, here, send_zl, recv_zl, num, dev_z)

    def last_px_send(num):
        here = last_piece(core, num, depth)
        return remote(here, here, send_pxl, recv_pxl, num, dev_p)

    def last_px_recv(num):
        here = last_piece(1 - core, num, depth)
        return remote(here, here, send_pxl, recv_pxl, num, dev_p)

    def last_pz_send(num):
        here = last_piece(core, num, 1 - depth)
        return remote(here, here, send_pzl, recv_pzl, num, dev_p)

    def last_pz_recv(num):
        here = last_piece(1 - core, num, 1 - depth)
        return remote(here, here, send_pzl, recv_pzl, num, dev_p)

    def own_send(step):
        return remote(
            b_ref.at[pl.ds(step * GROUP, GROUP), :], ball.at[pl.ds(row * band + step * GROUP, GROUP), :],
            send_own, recv_own, step, dev_p)

    def own_recv(step):
        here = ball.at[pl.ds(row_peer * band + step * GROUP, GROUP), :]
        return remote(here, here, send_own, recv_own, step, dev_p)

    def near_loads(step, slot):
        pltpu.make_async_copy(
            b_ref.at[pl.ds(step * GROUP, GROUP), :],
            b_v.at[slot, pl.ds(near + core * GROUP, GROUP), :], load_near.at[lax.rem(step, 2)]).start()
        pltpu.make_async_copy(
            ball.at[pl.ds(row_peer * band + step * GROUP, GROUP), :],
            b_v.at[slot, pl.ds(near + (1 - core) * GROUP, GROUP), :], load_near.at[lax.rem(step, 2)]).start()

    def near_wait(step, slot):
        here = b_v.at[slot, pl.ds(near, 2 * GROUP), :]
        pltpu.make_async_copy(here, here, load_near.at[lax.rem(step, 2)]).wait()

    def tile_cols(num):
        at = lax.rem(num, 2 * tiles)
        which = jnp.where(at < tiles, depth, 1 - depth)
        return pl.ds(pl.multiple_of(which * half + lax.rem(at, tiles) * TILE, TILE), TILE)

    def far_loads(num):
        step = num // SUBS
        slot = slot_of(step)
        at = tile_cols(num)
        for band_row, part in ((row_far, core), (row_far_peer, 1 - core)):
            pltpu.make_async_copy(
                ball.at[pl.ds(band_row * band + step * GROUP, GROUP), at],
                b_v.at[slot, pl.ds(far + part * GROUP, GROUP), at], load_far.at[lax.rem(num, SUBS)]).start()

    def far_wait(num):
        here = b_v.at[slot_of(num // SUBS), pl.ds(far, 2 * GROUP), tile_cols(num)]
        pltpu.make_async_copy(here, here, load_far.at[lax.rem(num, SUBS)]).wait()

    def sent(num):
        x_send(num).wait_send()
        z_send(num).wait_send()
        px_send(num).wait_send()
        pz_send(num).wait_send()

    def start_group(step, slot):
        own_recv(step).wait_recv()
        near_loads(step, slot)

        @pl.when(step + 2 < steps)
        def _():
            own_send(step + 2).start()

        @pl.when(step >= 1)
        def _():
            a_recv(step - 1).wait_recv()
            near_wait(step - 1, slot_of(step - 1))

    def add(step, at):
        acc[:, at] += jnp.dot(a_v[step], b_v[slot_of(step), :, at], preferred_element_type=jnp.float32)

    def load(new):
        at = lax.rem(new, 2 * tiles)
        first = (new // SUBS) * SUBS + lax.rem(at, tiles) * per

        @pl.when(at < tiles)
        def _():
            for k in range(per):
                px_recv(first + k).wait_recv()

        @pl.when(at >= tiles)
        def _():
            for k in range(per):
                pz_recv(first + k).wait_recv()
        far_loads(new)

    barrier = pltpu.get_barrier_semaphore()
    for dev in (dev_x, dev_y, dev_z, dev_p):
        pl.semaphore_signal(barrier, inc=1, device_id=dev, device_id_type=MESH)

    a_load(0, 0).start()
    a_load(0, 1).start()
    pl.semaphore_wait(barrier, 4)
    x_send(0).start()
    x_send(1).start()
    a_load_wait(0)
    a_send(0).start()

    @pl.loop(2, AHEAD)
    def _(num):
        x_send(num).start()

    @pl.loop(1, steps)
    def _(step):
        a_load(step, 0).start()
        a_load(step, 1).start()

    own_send(0).start()
    own_send(1).start()

    @pl.loop(0, body)
    def _(num):
        step = num // SUBS
        x_recv(num).wait_recv()
        z_send(num).start()
        px_send(num).start()

        @pl.when(num + AHEAD < body)
        def _():
            x_send(num + AHEAD).start()

        @pl.when(num + AHEAD >= body)
        def _():
            for k in range(2):
                new = (num + AHEAD - body) * 2 + k

                @pl.when(new < FINE)
                def _():
                    last_x_send(new).start()

                @pl.when((new >= FINE) & (new < FINE + SHIFT))
                def _():
                    last_x_extra(new - SHIFT).start()

        @pl.when((num == 0) | (num == 1))
        def _():
            a_load_wait(num + 1)
            a_send(num + 1).start()

        @pl.when((lax.rem(num, SUBS) == 0) & (step >= 1) & (step + 2 < steps))
        def _():
            a_load_wait(step + 2)
            a_send(step + 2).start()

        @pl.when(lax.rem(num, SUBS) == 0)
        def _():
            start_group(step, slot_of(step))

        @pl.when(step == 0)
        def _():
            acc[:, tile_cols(num)] = jnp.zeros((rows_c, TILE), jnp.float32)

        @pl.when(step >= 1)
        def _():
            far_wait(num - SUBS)
            add(step - 1, tile_cols(num))

        @pl.when(num >= LAG)
        def _():
            z_recv(num - LAG).wait_recv()
            pz_send(num - LAG).start()

        @pl.when(num >= LOAD)
        def _():
            load(num - LOAD)

        @pl.when(num >= BACK)
        def _():
            sent(num - BACK)

        @pl.when((lax.rem(num, SUBS) == 0) & (step >= 2))
        def _():
            a_send(step - 2).wait_send()
            own_send(step - 2).wait_send()

    def relay_out(num):
        last_z_recv(num).wait_recv()
        last_pz_send(num).start()

    for num in range(FINE):
        last_x_recv(num).wait_recv()
        if num < FINE - SHIFT:
            last_z_send(num).start()
        last_px_send(num).start()
        if num == 0:
            start_group(last, 2)
        part = num * SUBS // FINE
        if num % (FINE // SUBS) == 0:
            far_wait(body - SUBS + part)
        which = depth if part < tiles else 1 - depth
        add(last - 1, pl.ds(pl.multiple_of(
            which * half + (part % tiles) * TILE + (num % (FINE // SUBS)) * HALF_TILE, HALF_TILE), HALF_TILE))
        if num in (1, 3):
            z_recv(body - LAG + num // 2).wait_recv()
            pz_send(body - LAG + num // 2).start()
        if num >= FINE_LAG:
            relay_out(num - FINE_LAG)
        if num in LOADS:
            load(body - LOAD + LOADS.index(num))

    def finish(which, first, size):
        at = pl.ds(pl.multiple_of(which * half + first, HALF_TILE), size)
        total = acc[:, at] + jnp.dot(a_v[last], b_v[2, :, at], preferred_element_type=jnp.float32)
        o_v[:, at] = total.astype(o_v.dtype)

    for num in range(FINE - FINE_LAG, FINE - 1):
        relay_out(num)
    a_recv(last).wait_recv()
    near_wait(last, 2)
    for part in range(2 * tiles):
        for k in range(FINE // tiles):
            (last_px_recv if part < tiles else last_pz_recv)(part % tiles * FINE // tiles + k).wait_recv()
        finish(depth if part < tiles else 1 - depth, part % tiles * TILE, TILE)
        if part == 0:
            relay_out(FINE - 1)

    @pl.loop(body - BACK, body)
    def _(num):
        sent(num)

    @pl.loop(0, FINE)
    def _(num):
        last_x_send(num).wait_send()
        last_z_send(num).wait_send()
        last_px_send(num).wait_send()
        last_pz_send(num).wait_send()

    @pl.loop(steps - 3, steps)
    def _(step):
        a_send(step).wait_send()
        own_send(step).wait_send()


def solution(mesh):
    def local_mm(a_blk, b_blk):
        band, cols = b_blk.shape
        rows_c = a_blk.shape[0] // 2
        steps = band // GROUP
        count = (steps - 1) * SUBS
        any_spec = pl.BlockSpec(memory_space=pl.ANY)
        dma = pltpu.SemaphoreType.DMA
        c_blk, _ = pl.pallas_call(
            kernel,
            out_shape=(pltpu.VMEM((rows_c, cols), jnp.bfloat16),
                       jax.ShapeDtypeStruct((4 * band, cols), jnp.bfloat16)),
            in_specs=[any_spec] * 2,
            out_specs=(pl.BlockSpec(memory_space=pltpu.VMEM), any_spec),
            scratch_shapes=[
                pltpu.VMEM((steps, rows_c, 4 * GROUP), jnp.bfloat16),
                pltpu.VMEM((rows_c, cols), jnp.float32),
                pltpu.VMEM((3, 4 * GROUP, cols), jnp.bfloat16),
                dma((steps,)), dma((steps,)), dma((steps,)),
                dma((count,)), dma((count,)), dma((count,)), dma((count,)),
                dma((steps,)), dma((steps,)),
                dma((count,)), dma((count,)), dma((count,)), dma((count,)),
                dma((SUBS,)), dma((2,)),
                *[dma((FINE,))] * 8,
            ],
            compiler_params=pltpu.CompilerParams(
                collective_id=0, has_side_effects=True, vmem_limit_bytes=52 * 1024 * 1024),
            cost_estimate=pl.CostEstimate(
                flops=2 * rows_c * cols * 2 * cols, bytes_accessed=200 * 2 ** 20, transcendentals=0),
        )(a_blk, b_blk)
        return c_blk

    return jax.shard_map(
        local_mm, mesh=mesh, in_specs=(P("row", "col"), P("row", "col")),
        out_specs=P(("row", "depth"), "col"), check_vma=False)
```

```python
import jax
import jax.numpy as jnp
from jax import lax
from jax.experimental import pallas as pl
from jax.experimental.pallas import tpu as pltpu
from jax.sharding import PartitionSpec as P

MESH = pl.DeviceIdType.MESH
GROUP = 128
SUBS = 4
AHEAD = 6
LAG = 2
FINE = 8
FINE_LAG = 3
SHIFT = 2
LOAD = 3
TILE = 1024
BACK = 8
EARLY = 768
HALF_TILE = 512
LOADS = (0, 2, 5)


def kernel(a_ref, b_ref, o_v, ball, a_v, acc, b_v,
           load_a, send_a, recv_a, send_x, recv_x, send_z, recv_z, send_own, recv_own,
           send_px, recv_px, send_pz, recv_pz, load_far, load_near,
           send_xl, recv_xl, send_zl, recv_zl, send_pxl, recv_pxl, send_pzl, recv_pzl,
           send_al, recv_al):
    depth = lax.axis_index("depth")
    col = lax.axis_index("col")
    row = lax.axis_index("row")
    core = lax.rem(row, 2)
    chip_x = row // 2
    rows_c = a_ref.shape[0] // 2
    band = b_ref.shape[0]
    cols = b_ref.shape[1]
    steps = band // GROUP
    last = steps - 1
    half = cols // 2
    width = half // SUBS
    fine = half // FINE
    body = last * SUBS
    per = TILE // width
    tiles = half // TILE
    row_parts = ((0, EARLY), (EARLY, rows_c - EARLY))

    row_far = lax.rem(row + 2, 4)
    row_peer = chip_x * 2 + (1 - core)
    row_far_peer = lax.rem(row_peer + 2, 4)
    dev_x = (depth, col, row_far)
    dev_y = (depth, 1 - col, row)
    dev_z = (1 - depth, col, row)
    dev_p = (depth, col, row_peer)
    near = chip_x * 2 * GROUP
    far = (1 - chip_x) * 2 * GROUP

    def slot_of(step):
        return lax.rem(step, 2)

    def remote(src, dst, send, recv, num, dev):
        return pltpu.make_async_remote_copy(
            src, dst, send.at[num], recv.at[num], device_id=dev, device_id_type=MESH)

    def a_cols(step, side):
        return a_v.at[step, :, pl.ds(side * 2 * GROUP, 2 * GROUP)]

    def a_load(step, part):
        return pltpu.make_async_copy(
            a_ref.at[pl.ds(depth * rows_c, rows_c), pl.ds(part * band + step * GROUP, GROUP)],
            a_v.at[step, :, pl.ds(col * 2 * GROUP + part * GROUP, GROUP)], load_a.at[step])

    def a_load_wait(step):
        pltpu.make_async_copy(a_cols(step, col), a_cols(step, col), load_a.at[step]).wait()

    def a_send(step):
        return remote(a_cols(step, col), a_cols(step, col), send_a, recv_a, step, dev_y)

    def a_recv(step):
        return remote(a_cols(step, 1 - col), a_cols(step, 1 - col), send_a, recv_a, step, dev_y)

    def last_a(part, side):
        here = a_v.at[last, pl.ds(*row_parts[part]), pl.ds(side * 2 * GROUP, 2 * GROUP)]
        return remote(here, here, send_al, recv_al, part, dev_y)

    def piece(band_row, num, which):
        return ball.at[pl.ds(band_row * band + (num // SUBS) * GROUP, GROUP),
                       pl.ds(which * half + lax.rem(num, SUBS) * width, width)]

    def source(num, which):
        return b_ref.at[pl.ds((num // SUBS) * GROUP, GROUP),
                        pl.ds(which * half + lax.rem(num, SUBS) * width, width)]

    def x_send(num):
        return remote(source(num, depth), piece(row, num, depth), send_x, recv_x, num, dev_x)

    def x_recv(num):
        here = piece(row_far, num, depth)
        return remote(here, here, send_x, recv_x, num, dev_x)

    def z_send(num):
        here = piece(row_far, num, depth)
        return remote(here, here, send_z, recv_z, num, dev_z)

    def z_recv(num):
        here = piece(row_far, num, 1 - depth)
        return remote(here, here, send_z, recv_z, num, dev_z)

    def px_send(num):
        here = piece(row_far, num, depth)
        return remote(here, here, send_px, recv_px, num, dev_p)

    def px_recv(num):
        here = piece(row_far_peer, num, depth)
        return remote(here, here, send_px, recv_px, num, dev_p)

    def pz_send(num):
        here = piece(row_far, num, 1 - depth)
        return remote(here, here, send_pz, recv_pz, num, dev_p)

    def pz_recv(num):
        here = piece(row_far_peer, num, 1 - depth)
        return remote(here, here, send_pz, recv_pz, num, dev_p)

    def last_piece(core_of, num, which, first=far):
        return b_v.at[2, pl.ds(first + core_of * GROUP, GROUP), pl.ds(which * half + num * fine, fine)]

    def last_x_send(num):
        return remote(b_ref.at[pl.ds(last * GROUP, GROUP), pl.ds(depth * half + num * fine, fine)],
                      last_piece(core, num, depth, near), send_xl, recv_xl, num, dev_x)

    def last_x_extra(num):
        return remote(b_ref.at[pl.ds(last * GROUP, GROUP), pl.ds((1 - depth) * half + num * fine, fine)],
                      last_piece(core, num, 1 - depth, near), send_zl, recv_zl, num, dev_x)

    def last_x_recv(num):
        here = last_piece(core, num, depth)
        return remote(here, here, send_xl, recv_xl, num, dev_x)

    def last_z_send(num):
        here = last_piece(core, num, depth)
        return remote(here, here, send_zl, recv_zl, num, dev_z)

    def last_z_recv(num):
        here = last_piece(core, num, 1 - depth)
        return remote(here, here, send_zl, recv_zl, num, dev_z)

    def last_px_send(num):
        here = last_piece(core, num, depth)
        return remote(here, here, send_pxl, recv_pxl, num, dev_p)

    def last_px_recv(num):
        here = last_piece(1 - core, num, depth)
        return remote(here, here, send_pxl, recv_pxl, num, dev_p)

    def last_pz_send(num):
        here = last_piece(core, num, 1 - depth)
        return remote(here, here, send_pzl, recv_pzl, num, dev_p)

    def last_pz_recv(num):
        here = last_piece(1 - core, num, 1 - depth)
        return remote(here, here, send_pzl, recv_pzl, num, dev_p)

    def own_send(step):
        return remote(
            b_ref.at[pl.ds(step * GROUP, GROUP), :], ball.at[pl.ds(row * band + step * GROUP, GROUP), :],
            send_own, recv_own, step, dev_p)

    def own_recv(step):
        here = ball.at[pl.ds(row_peer * band + step * GROUP, GROUP), :]
        return remote(here, here, send_own, recv_own, step, dev_p)

    def near_loads(step, slot):
        pltpu.make_async_copy(
            b_ref.at[pl.ds(step * GROUP, GROUP), :],
            b_v.at[slot, pl.ds(near + core * GROUP, GROUP), :], load_near.at[lax.rem(step, 2)]).start()
        pltpu.make_async_copy(
            ball.at[pl.ds(row_peer * band + step * GROUP, GROUP), :],
            b_v.at[slot, pl.ds(near + (1 - core) * GROUP, GROUP), :], load_near.at[lax.rem(step, 2)]).start()

    def near_wait(step, slot):
        here = b_v.at[slot, pl.ds(near, 2 * GROUP), :]
        pltpu.make_async_copy(here, here, load_near.at[lax.rem(step, 2)]).wait()

    def tile_cols(num):
        at = lax.rem(num, 2 * tiles)
        which = jnp.where(at < tiles, depth, 1 - depth)
        return pl.ds(pl.multiple_of(which * half + lax.rem(at, tiles) * TILE, TILE), TILE)

    def far_loads(num):
        step = num // SUBS
        slot = slot_of(step)
        at = tile_cols(num)
        for band_row, part in ((row_far, core), (row_far_peer, 1 - core)):
            pltpu.make_async_copy(
                ball.at[pl.ds(band_row * band + step * GROUP, GROUP), at],
                b_v.at[slot, pl.ds(far + part * GROUP, GROUP), at], load_far.at[lax.rem(num, SUBS)]).start()

    def far_wait(num):
        here = b_v.at[slot_of(num // SUBS), pl.ds(far, 2 * GROUP), tile_cols(num)]
        pltpu.make_async_copy(here, here, load_far.at[lax.rem(num, SUBS)]).wait()

    def sent(num):
        x_send(num).wait_send()
        z_send(num).wait_send()
        px_send(num).wait_send()
        pz_send(num).wait_send()

    def start_group(step, slot):
        own_recv(step).wait_recv()
        near_loads(step, slot)

        @pl.when(step + 2 < steps)
        def _():
            own_send(step + 2).start()

        @pl.when(step >= 1)
        def _():
            a_recv(step - 1).wait_recv()
            near_wait(step - 1, slot_of(step - 1))

    def add(step, at):
        acc[:, at] += jnp.dot(a_v[step], b_v[slot_of(step), :, at], preferred_element_type=jnp.float32)

    def load(new):
        at = lax.rem(new, 2 * tiles)
        first = (new // SUBS) * SUBS + lax.rem(at, tiles) * per

        @pl.when(at < tiles)
        def _():
            for k in range(per):
                px_recv(first + k).wait_recv()

        @pl.when(at >= tiles)
        def _():
            for k in range(per):
                pz_recv(first + k).wait_recv()
        far_loads(new)

    barrier = pltpu.get_barrier_semaphore()
    for dev in (dev_x, dev_y, dev_z, dev_p):
        pl.semaphore_signal(barrier, inc=1, device_id=dev, device_id_type=MESH)

    a_load(0, 0).start()
    a_load(0, 1).start()
    pl.semaphore_wait(barrier, 4)
    x_send(0).start()
    x_send(1).start()
    a_load_wait(0)
    a_send(0).start()

    @pl.loop(2, AHEAD)
    def _(num):
        x_send(num).start()

    @pl.loop(1, steps)
    def _(step):
        a_load(step, 0).start()
        a_load(step, 1).start()

    own_send(0).start()
    own_send(1).start()

    @pl.loop(0, body)
    def _(num):
        step = num // SUBS
        x_recv(num).wait_recv()
        z_send(num).start()
        px_send(num).start()

        @pl.when(num + AHEAD < body)
        def _():
            x_send(num + AHEAD).start()

        @pl.when(num + AHEAD >= body)
        def _():
            for k in range(2):
                new = (num + AHEAD - body) * 2 + k

                @pl.when(new < FINE)
                def _():
                    last_x_send(new).start()

                @pl.when((new >= FINE) & (new < FINE + SHIFT))
                def _():
                    last_x_extra(new - SHIFT).start()

        @pl.when((num == 0) | (num == 1))
        def _():
            a_load_wait(num + 1)
            a_send(num + 1).start()

        @pl.when((lax.rem(num, SUBS) == 0) & (step >= 1) & (step + 2 < steps))
        def _():
            a_load_wait(step + 2)

            @pl.when(step + 2 < last)
            def _():
                a_send(step + 2).start()

            @pl.when(step + 2 == last)
            def _():
                for part in range(2):
                    last_a(part, col).start()

        @pl.when(lax.rem(num, SUBS) == 0)
        def _():
            start_group(step, slot_of(step))

        @pl.when(step == 0)
        def _():
            acc[:, tile_cols(num)] = jnp.zeros((rows_c, TILE), jnp.float32)

        @pl.when(step >= 1)
        def _():
            far_wait(num - SUBS)
            add(step - 1, tile_cols(num))

        @pl.when(num >= LAG)
        def _():
            z_recv(num - LAG).wait_recv()
            pz_send(num - LAG).start()

        @pl.when(num >= LOAD)
        def _():
            load(num - LOAD)

        @pl.when(num >= BACK)
        def _():
            sent(num - BACK)

        @pl.when((lax.rem(num, SUBS) == 0) & (step >= 2))
        def _():
            a_send(step - 2).wait_send()
            own_send(step - 2).wait_send()

    def relay_out(num):
        last_z_recv(num).wait_recv()
        last_pz_send(num).start()

    for num in range(FINE):
        last_x_recv(num).wait_recv()
        if num < FINE - SHIFT:
            last_z_send(num).start()
        last_px_send(num).start()
        if num == 0:
            start_group(last, 2)
        part = num * SUBS // FINE
        if num % (FINE // SUBS) == 0:
            far_wait(body - SUBS + part)
        which = depth if part < tiles else 1 - depth
        add(last - 1, pl.ds(pl.multiple_of(
            which * half + (part % tiles) * TILE + (num % (FINE // SUBS)) * HALF_TILE, HALF_TILE), HALF_TILE))
        if num in (1, 3):
            z_recv(body - LAG + num // 2).wait_recv()
            pz_send(body - LAG + num // 2).start()
        if num >= FINE_LAG:
            relay_out(num - FINE_LAG)
        if num in LOADS:
            load(body - LOAD + LOADS.index(num))

    def finish(tile, first, size):
        which = depth if tile < tiles else 1 - depth
        at = pl.ds(pl.multiple_of(which * half + tile % tiles * TILE, TILE), TILE)
        rows = pl.ds(first, size)
        total = acc[rows, at] + jnp.dot(a_v[last, rows, :], b_v[2, :, at], preferred_element_type=jnp.float32)
        o_v[rows, at] = total.astype(o_v.dtype)

    def wait_tile(tile):
        for k in range(FINE // tiles):
            (last_px_recv if tile < tiles else last_pz_recv)(tile % tiles * FINE // tiles + k).wait_recv()

    for num in range(FINE - FINE_LAG, FINE - 1):
        relay_out(num)
    last_a(0, 1 - col).wait_recv()
    near_wait(last, 2)
    for tile in range(2 * tiles - 1):
        wait_tile(tile)
        finish(tile, *row_parts[0])
        if tile == 0:
            relay_out(FINE - 1)
    last_a(1, 1 - col).wait_recv()
    for tile in range(2 * tiles - 1):
        finish(tile, *row_parts[1])
    wait_tile(2 * tiles - 1)
    finish(2 * tiles - 1, 0, rows_c)

    @pl.loop(body - BACK, body)
    def _(num):
        sent(num)

    @pl.loop(0, FINE)
    def _(num):
        last_x_send(num).wait_send()
        last_z_send(num).wait_send()
        last_px_send(num).wait_send()
        last_pz_send(num).wait_send()

    for part in range(2):
        last_a(part, col).wait_send()

    @pl.loop(steps - 3, last)
    def _(step):
        a_send(step).wait_send()

    @pl.loop(steps - 3, steps)
    def _(step):
        own_send(step).wait_send()


def solution(mesh):
    def local_mm(a_blk, b_blk):
        band, cols = b_blk.shape
        rows_c = a_blk.shape[0] // 2
        steps = band // GROUP
        count = (steps - 1) * SUBS
        any_spec = pl.BlockSpec(memory_space=pl.ANY)
        dma = pltpu.SemaphoreType.DMA
        c_blk, _ = pl.pallas_call(
            kernel,
            out_shape=(pltpu.VMEM((rows_c, cols), jnp.bfloat16),
                       jax.ShapeDtypeStruct((4 * band, cols), jnp.bfloat16)),
            in_specs=[any_spec] * 2,
            out_specs=(pl.BlockSpec(memory_space=pltpu.VMEM), any_spec),
            scratch_shapes=[
                pltpu.VMEM((steps, rows_c, 4 * GROUP), jnp.bfloat16),
                pltpu.VMEM((rows_c, cols), jnp.float32),
                pltpu.VMEM((3, 4 * GROUP, cols), jnp.bfloat16),
                dma((steps,)), dma((steps,)), dma((steps,)),
                dma((count,)), dma((count,)), dma((count,)), dma((count,)),
                dma((steps,)), dma((steps,)),
                dma((count,)), dma((count,)), dma((count,)), dma((count,)),
                dma((SUBS,)), dma((2,)),
                *[dma((FINE,))] * 8,
                dma((2,)), dma((2,)),
            ],
            compiler_params=pltpu.CompilerParams(
                collective_id=0, has_side_effects=True, vmem_limit_bytes=52 * 1024 * 1024),
            cost_estimate=pl.CostEstimate(
                flops=2 * rows_c * cols * 2 * cols, bytes_accessed=200 * 2 ** 20, transcendentals=0),
        )(a_blk, b_blk)
        return c_blk

    return jax.shard_map(
        local_mm, mesh=mesh, in_specs=(P("row", "col"), P("row", "col")),
        out_specs=P(("row", "depth"), "col"), check_vma=False)
```

```python
import jax
import jax.numpy as jnp
from jax import lax
from jax.experimental import pallas as pl
from jax.experimental.pallas import tpu as pltpu
from jax.sharding import PartitionSpec as P

MESH = pl.DeviceIdType.MESH
GROUP = 128
SUBS = 4
AHEAD = 6
LAG = 2
FINE = 8
FINE_LAG = 6
SHIFT = 2
LOAD = 4
FAR = 6
TILE = 1024
BACK = 8
HALF_TILE = 512
LOADS = (0, 1, 2, 5)
DOTS = (0, 1, 2, 3, 4, 7)


def kernel(a_ref, b_ref, o_v, ball, a_v, acc, b_v,
           load_a, send_a, recv_a, send_x, recv_x, send_z, recv_z, send_own, recv_own,
           send_px, recv_px, send_pz, recv_pz, load_far, load_near,
           send_xl, recv_xl, send_zl, recv_zl, send_pxl, recv_pxl, send_pzl, recv_pzl):
    depth = lax.axis_index("depth")
    col = lax.axis_index("col")
    row = lax.axis_index("row")
    core = lax.rem(row, 2)
    chip_x = row // 2
    rows_c = a_ref.shape[0] // 2
    band = b_ref.shape[0]
    cols = b_ref.shape[1]
    steps = band // GROUP
    last = steps - 1
    half = cols // 2
    width = half // SUBS
    fine = half // FINE
    body = last * SUBS
    per = TILE // width
    tiles = half // TILE

    row_far = lax.rem(row + 2, 4)
    row_peer = chip_x * 2 + (1 - core)
    row_far_peer = lax.rem(row_peer + 2, 4)
    dev_x = (depth, col, row_far)
    dev_y = (depth, 1 - col, row)
    dev_z = (1 - depth, col, row)
    dev_p = (depth, col, row_peer)
    near = chip_x * 2 * GROUP
    far = (1 - chip_x) * 2 * GROUP

    def slot_of(step):
        return lax.rem(step, 2)

    def remote(src, dst, send, recv, num, dev):
        return pltpu.make_async_remote_copy(
            src, dst, send.at[num], recv.at[num], device_id=dev, device_id_type=MESH)

    def a_cols(step, side):
        return a_v.at[step, :, pl.ds(side * 2 * GROUP, 2 * GROUP)]

    def a_load(step, part):
        return pltpu.make_async_copy(
            a_ref.at[pl.ds(depth * rows_c, rows_c), pl.ds(part * band + step * GROUP, GROUP)],
            a_v.at[step, :, pl.ds(col * 2 * GROUP + part * GROUP, GROUP)], load_a.at[step])

    def a_load_wait(step):
        pltpu.make_async_copy(a_cols(step, col), a_cols(step, col), load_a.at[step]).wait()

    def a_send(step):
        return remote(a_cols(step, col), a_cols(step, col), send_a, recv_a, step, dev_y)

    def a_recv(step):
        return remote(a_cols(step, 1 - col), a_cols(step, 1 - col), send_a, recv_a, step, dev_y)

    def piece(band_row, num, which):
        return ball.at[pl.ds(band_row * band + (num // SUBS) * GROUP, GROUP),
                       pl.ds(which * half + lax.rem(num, SUBS) * width, width)]

    def source(num, which):
        return b_ref.at[pl.ds((num // SUBS) * GROUP, GROUP),
                        pl.ds(which * half + lax.rem(num, SUBS) * width, width)]

    def x_send(num):
        return remote(source(num, depth), piece(row, num, depth), send_x, recv_x, num, dev_x)

    def x_recv(num):
        here = piece(row_far, num, depth)
        return remote(here, here, send_x, recv_x, num, dev_x)

    def z_send(num):
        here = piece(row_far, num, depth)
        return remote(here, here, send_z, recv_z, num, dev_z)

    def z_recv(num):
        here = piece(row_far, num, 1 - depth)
        return remote(here, here, send_z, recv_z, num, dev_z)

    def px_send(num):
        here = piece(row_far, num, depth)
        return remote(here, here, send_px, recv_px, num, dev_p)

    def px_recv(num):
        here = piece(row_far_peer, num, depth)
        return remote(here, here, send_px, recv_px, num, dev_p)

    def pz_send(num):
        here = piece(row_far, num, 1 - depth)
        return remote(here, here, send_pz, recv_pz, num, dev_p)

    def pz_recv(num):
        here = piece(row_far_peer, num, 1 - depth)
        return remote(here, here, send_pz, recv_pz, num, dev_p)

    def last_piece(core_of, num, which, first=far):
        return b_v.at[2, pl.ds(first + core_of * GROUP, GROUP), pl.ds(which * half + num * fine, fine)]

    def last_x_send(num):
        return remote(b_ref.at[pl.ds(last * GROUP, GROUP), pl.ds(depth * half + num * fine, fine)],
                      last_piece(core, num, depth, near), send_xl, recv_xl, num, dev_x)

    def last_x_extra(num):
        return remote(b_ref.at[pl.ds(last * GROUP, GROUP), pl.ds((1 - depth) * half + num * fine, fine)],
                      last_piece(core, num, 1 - depth, near), send_zl, recv_zl, num, dev_x)

    def last_x_recv(num):
        here = last_piece(core, num, depth)
        return remote(here, here, send_xl, recv_xl, num, dev_x)

    def last_z_send(num):
        here = last_piece(core, num, depth)
        return remote(here, here, send_zl, recv_zl, num, dev_z)

    def last_z_recv(num):
        here = last_piece(core, num, 1 - depth)
        return remote(here, here, send_zl, recv_zl, num, dev_z)

    def last_px_send(num):
        here = last_piece(core, num, depth)
        return remote(here, here, send_pxl, recv_pxl, num, dev_p)

    def last_px_recv(num):
        here = last_piece(1 - core, num, depth)
        return remote(here, here, send_pxl, recv_pxl, num, dev_p)

    def last_pz_send(num):
        here = last_piece(core, num, 1 - depth)
        return remote(here, here, send_pzl, recv_pzl, num, dev_p)

    def last_pz_recv(num):
        here = last_piece(1 - core, num, 1 - depth)
        return remote(here, here, send_pzl, recv_pzl, num, dev_p)

    def own_send(step):
        return remote(
            b_ref.at[pl.ds(step * GROUP, GROUP), :], ball.at[pl.ds(row * band + step * GROUP, GROUP), :],
            send_own, recv_own, step, dev_p)

    def own_recv(step):
        here = ball.at[pl.ds(row_peer * band + step * GROUP, GROUP), :]
        return remote(here, here, send_own, recv_own, step, dev_p)

    def near_loads(step, slot):
        pltpu.make_async_copy(
            b_ref.at[pl.ds(step * GROUP, GROUP), :],
            b_v.at[slot, pl.ds(near + core * GROUP, GROUP), :], load_near.at[lax.rem(step, 2)]).start()
        pltpu.make_async_copy(
            ball.at[pl.ds(row_peer * band + step * GROUP, GROUP), :],
            b_v.at[slot, pl.ds(near + (1 - core) * GROUP, GROUP), :], load_near.at[lax.rem(step, 2)]).start()

    def near_wait(step, slot):
        here = b_v.at[slot, pl.ds(near, 2 * GROUP), :]
        pltpu.make_async_copy(here, here, load_near.at[lax.rem(step, 2)]).wait()

    def tile_cols(num):
        at = lax.rem(num, 2 * tiles)
        which = jnp.where(at < tiles, depth, 1 - depth)
        return pl.ds(pl.multiple_of(which * half + lax.rem(at, tiles) * TILE, TILE), TILE)

    def far_loads(num):
        step = num // SUBS
        slot = slot_of(step)
        at = tile_cols(num)
        for band_row, part in ((row_far, core), (row_far_peer, 1 - core)):
            pltpu.make_async_copy(
                ball.at[pl.ds(band_row * band + step * GROUP, GROUP), at],
                b_v.at[slot, pl.ds(far + part * GROUP, GROUP), at], load_far.at[lax.rem(num, SUBS)]).start()

    def far_wait(num):
        here = b_v.at[slot_of(num // SUBS), pl.ds(far, 2 * GROUP), tile_cols(num)]
        pltpu.make_async_copy(here, here, load_far.at[lax.rem(num, SUBS)]).wait()

    def sent(num):
        x_send(num).wait_send()
        z_send(num).wait_send()
        px_send(num).wait_send()
        pz_send(num).wait_send()

    def start_group(step, slot):
        own_recv(step).wait_recv()
        near_loads(step, slot)

        @pl.when(step + 2 < steps)
        def _():
            own_send(step + 2).start()

    def meet(step):
        a_recv(step).wait_recv()
        near_wait(step, slot_of(step))

    def add(step, at):
        acc[:, at] += jnp.dot(a_v[step], b_v[slot_of(step), :, at], preferred_element_type=jnp.float32)

    def load(new):
        at = lax.rem(new, 2 * tiles)
        first = (new // SUBS) * SUBS + lax.rem(at, tiles) * per

        @pl.when(at < tiles)
        def _():
            for k in range(per):
                px_recv(first + k).wait_recv()

        @pl.when(at >= tiles)
        def _():
            for k in range(per):
                pz_recv(first + k).wait_recv()
        far_loads(new)

    barrier = pltpu.get_barrier_semaphore()
    for dev in (dev_x, dev_y, dev_z, dev_p):
        pl.semaphore_signal(barrier, inc=1, device_id=dev, device_id_type=MESH)

    a_load(0, 0).start()
    a_load(0, 1).start()
    pl.semaphore_wait(barrier, 4)
    x_send(0).start()
    x_send(1).start()
    a_load_wait(0)
    a_send(0).start()

    @pl.loop(2, AHEAD)
    def _(num):
        x_send(num).start()

    @pl.loop(1, steps)
    def _(step):
        a_load(step, 0).start()
        a_load(step, 1).start()

    own_send(0).start()
    own_send(1).start()

    @pl.loop(0, body)
    def _(num):
        step = num // SUBS
        x_recv(num).wait_recv()
        z_send(num).start()
        px_send(num).start()

        @pl.when(num + AHEAD < body)
        def _():
            x_send(num + AHEAD).start()

        @pl.when(num + AHEAD >= body)
        def _():
            for k in range(2):
                new = (num + AHEAD - body) * 2 + k

                @pl.when(new < FINE)
                def _():
                    last_x_send(new).start()

                @pl.when((new >= FINE) & (new < FINE + SHIFT))
                def _():
                    last_x_extra(new - SHIFT).start()

        @pl.when((num == 0) | (num == 1))
        def _():
            a_load_wait(num + 1)
            a_send(num + 1).start()

        @pl.when((lax.rem(num, SUBS) == 0) & (step >= 1) & (step + 2 < steps))
        def _():
            a_load_wait(step + 2)
            a_send(step + 2).start()

        @pl.when(step == 0)
        def _():
            acc[:, tile_cols(num)] = jnp.zeros((rows_c, TILE), jnp.float32)

        @pl.when(num >= FAR)
        def _():
            new = num - FAR

            @pl.when(lax.rem(new, SUBS) == 0)
            def _():
                meet(new // SUBS)
            far_wait(new)
            add(new // SUBS, tile_cols(new))

        @pl.when(lax.rem(num, SUBS) == FAR - SUBS)
        def _():
            start_group(step, slot_of(step))

        @pl.when(num >= LAG)
        def _():
            z_recv(num - LAG).wait_recv()
            pz_send(num - LAG).start()

        @pl.when(num >= LOAD)
        def _():
            load(num - LOAD)

        @pl.when(num >= BACK)
        def _():
            sent(num - BACK)

        @pl.when((lax.rem(num, SUBS) == 0) & (step >= 2))
        def _():
            a_send(step - 2).wait_send()
            own_send(step - 2).wait_send()

    def relay_out(num):
        last_z_recv(num).wait_recv()
        last_pz_send(num).start()

    for num in range(FINE):
        last_x_recv(num).wait_recv()
        if num < FINE - SHIFT:
            last_z_send(num).start()
        last_px_send(num).start()
        if num in DOTS:
            new = body - FAR + DOTS.index(num)
            if new % SUBS == 0:
                meet(last - 1)
            far_wait(new)
            add(new // SUBS, tile_cols(new))
        if num == 1:
            start_group(last, 2)
        if num in (1, 3):
            z_recv(body - LAG + num // 2).wait_recv()
            pz_send(body - LAG + num // 2).start()
        if num >= FINE_LAG:
            relay_out(num - FINE_LAG)
        if num in LOADS:
            load(body - LOAD + LOADS.index(num))

    def finish(which, first, size):
        at = pl.ds(pl.multiple_of(which * half + first, HALF_TILE), size)
        total = acc[:, at] + jnp.dot(a_v[last], b_v[2, :, at], preferred_element_type=jnp.float32)
        o_v[:, at] = total.astype(o_v.dtype)

    def direct(part):
        for k in range(FINE // tiles):
            last_px_recv(part * FINE // tiles + k).wait_recv()
        finish(depth, part * TILE, TILE)

    def relayed(first, size):
        for k in range(size // fine):
            last_pz_recv(first // fine + k).wait_recv()
        finish(1 - depth, first, size)

    relay_out(2)
    relay_out(3)
    relay_out(6)
    a_recv(last).wait_recv()
    near_wait(last, 2)
    direct(0)
    relay_out(7)
    relay_out(4)
    direct(1)
    relay_out(5)
    relayed(0, TILE)
    relayed(TILE + HALF_TILE, HALF_TILE)
    relayed(TILE, HALF_TILE)

    @pl.loop(body - BACK, body)
    def _(num):
        sent(num)

    @pl.loop(0, FINE)
    def _(num):
        last_x_send(num).wait_send()
        last_z_send(num).wait_send()
        last_px_send(num).wait_send()
        last_pz_send(num).wait_send()

    @pl.loop(steps - 3, steps)
    def _(step):
        a_send(step).wait_send()
        own_send(step).wait_send()


def solution(mesh):
    def local_mm(a_blk, b_blk):
        band, cols = b_blk.shape
        rows_c = a_blk.shape[0] // 2
        steps = band // GROUP
        count = (steps - 1) * SUBS
        any_spec = pl.BlockSpec(memory_space=pl.ANY)
        dma = pltpu.SemaphoreType.DMA
        c_blk, _ = pl.pallas_call(
            kernel,
            out_shape=(pltpu.VMEM((rows_c, cols), jnp.bfloat16),
                       jax.ShapeDtypeStruct((4 * band, cols), jnp.bfloat16)),
            in_specs=[any_spec] * 2,
            out_specs=(pl.BlockSpec(memory_space=pltpu.VMEM), any_spec),
            scratch_shapes=[
                pltpu.VMEM((steps, rows_c, 4 * GROUP), jnp.bfloat16),
                pltpu.VMEM((rows_c, cols), jnp.float32),
                pltpu.VMEM((3, 4 * GROUP, cols), jnp.bfloat16),
                dma((steps,)), dma((steps,)), dma((steps,)),
                dma((count,)), dma((count,)), dma((count,)), dma((count,)),
                dma((steps,)), dma((steps,)),
                dma((count,)), dma((count,)), dma((count,)), dma((count,)),
                dma((SUBS,)), dma((2,)),
                *[dma((FINE,))] * 8,
            ],
            compiler_params=pltpu.CompilerParams(
                collective_id=0, has_side_effects=True, vmem_limit_bytes=52 * 1024 * 1024),
            cost_estimate=pl.CostEstimate(
                flops=2 * rows_c * cols * 2 * cols, bytes_accessed=200 * 2 ** 20, transcendentals=0),
        )(a_blk, b_blk)
        return c_blk

    return jax.shard_map(
        local_mm, mesh=mesh, in_specs=(P("row", "col"), P("row", "col")),
        out_specs=P(("row", "depth"), "col"), check_vma=False)
```

```python
import jax
import jax.numpy as jnp
from jax import lax
from jax.experimental import pallas as pl
from jax.experimental.pallas import tpu as pltpu
from jax.sharding import PartitionSpec as P

MESH = pl.DeviceIdType.MESH
GROUP = 128
SUBS = 4
AHEAD = 6
LAG = 2
SHIFT = 1
LOAD = 3
TILE = 1024
BACK = 8
WIDE = 1024


def kernel(a_ref, b_ref, o_v, ball, a_v, acc, b_v,
           load_a, send_a, recv_a, send_x, recv_x, send_z, recv_z, send_own, recv_own,
           send_px, recv_px, send_pz, recv_pz, load_far, load_near):
    depth = lax.axis_index("depth")
    col = lax.axis_index("col")
    row = lax.axis_index("row")
    core = lax.rem(row, 2)
    chip_x = row // 2
    rows_c = a_ref.shape[0] // 2
    band = b_ref.shape[0]
    cols = b_ref.shape[1]
    steps = band // GROUP
    last = steps - 1
    half = cols // 2
    width = half // SUBS
    count = steps * SUBS
    body = count - SUBS
    per = TILE // width
    tiles = half // TILE

    row_far = lax.rem(row + 2, 4)
    row_peer = chip_x * 2 + (1 - core)
    row_far_peer = lax.rem(row_peer + 2, 4)
    dev_x = (depth, col, row_far)
    dev_y = (depth, 1 - col, row)
    dev_z = (1 - depth, col, row)
    dev_p = (depth, col, row_peer)
    near = chip_x * 2 * GROUP
    far = (1 - chip_x) * 2 * GROUP

    def slot_of(step):
        return lax.rem(step, 2)

    def remote(src, dst, send, recv, num, dev):
        return pltpu.make_async_remote_copy(
            src, dst, send.at[num], recv.at[num], device_id=dev, device_id_type=MESH)

    def a_cols(step, side):
        return a_v.at[step, :, pl.ds(side * 2 * GROUP, 2 * GROUP)]

    def a_load(step, part):
        return pltpu.make_async_copy(
            a_ref.at[pl.ds(depth * rows_c, rows_c), pl.ds(part * band + step * GROUP, GROUP)],
            a_v.at[step, :, pl.ds(col * 2 * GROUP + part * GROUP, GROUP)], load_a.at[step])

    def a_load_wait(step):
        pltpu.make_async_copy(a_cols(step, col), a_cols(step, col), load_a.at[step]).wait()

    def a_send(step):
        return remote(a_cols(step, col), a_cols(step, col), send_a, recv_a, step, dev_y)

    def a_recv(step):
        return remote(a_cols(step, 1 - col), a_cols(step, 1 - col), send_a, recv_a, step, dev_y)

    def piece(band_row, num, which):
        return ball.at[pl.ds(band_row * band + (num // SUBS) * GROUP, GROUP),
                       pl.ds(which * half + lax.rem(num, SUBS) * width, width)]

    def last_piece(core_of, num, which, first=far):
        return b_v.at[2, pl.ds(first + core_of * GROUP, GROUP),
                      pl.ds(which * half + lax.rem(num, SUBS) * width, width)]

    def source(num, which):
        return b_ref.at[pl.ds((num // SUBS) * GROUP, GROUP),
                        pl.ds(which * half + lax.rem(num, SUBS) * width, width)]

    def mine(num, which, is_last):
        return last_piece(core, num, which) if is_last else piece(row_far, num, which)

    def peers(num, which, is_last):
        return last_piece(1 - core, num, which) if is_last else piece(row_far_peer, num, which)

    def x_send(num, is_last):
        dst = last_piece(core, num, depth, near) if is_last else piece(row, num, depth)
        return remote(source(num, depth), dst, send_x, recv_x, num, dev_x)

    def x_send_extra(num):
        return remote(source(num, 1 - depth), last_piece(core, num, 1 - depth, near), send_z, recv_z, num, dev_x)

    def x_recv(num, is_last):
        here = mine(num, depth, is_last)
        return remote(here, here, send_x, recv_x, num, dev_x)

    def z_send(num, is_last):
        here = mine(num, depth, is_last)
        return remote(here, here, send_z, recv_z, num, dev_z)

    def z_recv(num, is_last):
        here = mine(num, 1 - depth, is_last)
        return remote(here, here, send_z, recv_z, num, dev_z)

    def px_send(num, is_last):
        here = mine(num, depth, is_last)
        return remote(here, here, send_px, recv_px, num, dev_p)

    def px_recv(num, is_last):
        here = peers(num, depth, is_last)
        return remote(here, here, send_px, recv_px, num, dev_p)

    def pz_send(num, is_last):
        here = mine(num, 1 - depth, is_last)
        return remote(here, here, send_pz, recv_pz, num, dev_p)

    def pz_recv(num, is_last):
        here = peers(num, 1 - depth, is_last)
        return remote(here, here, send_pz, recv_pz, num, dev_p)

    def own_send(step):
        return remote(
            b_ref.at[pl.ds(step * GROUP, GROUP), :], ball.at[pl.ds(row * band + step * GROUP, GROUP), :],
            send_own, recv_own, step, dev_p)

    def own_recv(step):
        here = ball.at[pl.ds(row_peer * band + step * GROUP, GROUP), :]
        return remote(here, here, send_own, recv_own, step, dev_p)

    def near_loads(step, slot):
        pltpu.make_async_copy(
            b_ref.at[pl.ds(step * GROUP, GROUP), :],
            b_v.at[slot, pl.ds(near + core * GROUP, GROUP), :], load_near.at[lax.rem(step, 2)]).start()
        pltpu.make_async_copy(
            ball.at[pl.ds(row_peer * band + step * GROUP, GROUP), :],
            b_v.at[slot, pl.ds(near + (1 - core) * GROUP, GROUP), :], load_near.at[lax.rem(step, 2)]).start()

    def near_wait(step, slot):
        here = b_v.at[slot, pl.ds(near, 2 * GROUP), :]
        pltpu.make_async_copy(here, here, load_near.at[lax.rem(step, 2)]).wait()

    def tile_cols(num):
        at = lax.rem(num, 2 * tiles)
        which = jnp.where(at < tiles, depth, 1 - depth)
        return pl.ds(pl.multiple_of(which * half + lax.rem(at, tiles) * TILE, TILE), TILE)

    def far_loads(num):
        step = num // SUBS
        slot = slot_of(step)
        at = tile_cols(num)
        for band_row, part in ((row_far, core), (row_far_peer, 1 - core)):
            pltpu.make_async_copy(
                ball.at[pl.ds(band_row * band + step * GROUP, GROUP), at],
                b_v.at[slot, pl.ds(far + part * GROUP, GROUP), at], load_far.at[lax.rem(num, SUBS)]).start()

    def far_wait(num):
        here = b_v.at[slot_of(num // SUBS), pl.ds(far, 2 * GROUP), tile_cols(num)]
        pltpu.make_async_copy(here, here, load_far.at[lax.rem(num, SUBS)]).wait()

    def sent(num, is_last):
        x_send(num, is_last).wait_send()
        z_send(num, is_last).wait_send()
        px_send(num, is_last).wait_send()
        pz_send(num, is_last).wait_send()

    def multiply(num, slot):
        step = num // SUBS

        @pl.when(lax.rem(num, SUBS) == 0)
        def _():
            own_recv(step).wait_recv()
            near_loads(step, slot)

            @pl.when(step + 2 < steps)
            def _():
                own_send(step + 2).start()

            @pl.when(step >= 1)
            def _():
                a_recv(step - 1).wait_recv()
                near_wait(step - 1, slot_of(step - 1))

        @pl.when(step >= 1)
        def _():
            far_wait(num - SUBS)
            at = tile_cols(num)
            acc[:, at] += jnp.dot(a_v[step - 1], b_v[slot_of(step - 1), :, at], preferred_element_type=jnp.float32)

    def load(num):
        step = num // SUBS

        @pl.when((num >= LOAD) & (num < body + LOAD))
        def _():
            new = num - LOAD
            at = lax.rem(new, 2 * tiles)
            first = (new // SUBS) * SUBS + lax.rem(at, tiles) * per

            @pl.when(at < tiles)
            def _():
                for k in range(per):
                    px_recv(first + k, False).wait_recv()

            @pl.when(at >= tiles)
            def _():
                for k in range(per):
                    pz_recv(first + k, False).wait_recv()
            far_loads(new)

        @pl.when(num >= BACK)
        def _():
            sent(num - BACK, False)

        @pl.when((lax.rem(num, SUBS) == 0) & (step >= 2))
        def _():
            a_send(step - 2).wait_send()
            own_send(step - 2).wait_send()

    barrier = pltpu.get_barrier_semaphore()
    for dev in (dev_x, dev_y, dev_z, dev_p):
        pl.semaphore_signal(barrier, inc=1, device_id=dev, device_id_type=MESH)

    @pl.loop(0, steps)
    def _(step):
        a_load(step, 0).start()
        a_load(step, 1).start()

    pl.semaphore_wait(barrier, 4)

    x_send(0, False).start()
    a_load_wait(0)
    a_send(0).start()

    @pl.loop(1, AHEAD)
    def _(num):
        x_send(num, False).start()

    own_send(0).start()
    own_send(1).start()

    @pl.loop(1, steps)
    def _(step):
        a_load_wait(step)
        a_send(step).start()

    @pl.loop(0, cols // TILE)
    def _(tile):
        at = pl.ds(pl.multiple_of(tile * TILE, TILE), TILE)
        acc[:, at] = jnp.zeros((rows_c, TILE), jnp.float32)

    @pl.loop(0, body)
    def _(num):
        x_recv(num, False).wait_recv()
        z_send(num, False).start()
        px_send(num, False).start()

        @pl.when(num + AHEAD < body)
        def _():
            x_send(num + AHEAD, False).start()

        @pl.when((num + AHEAD >= body) & (num + AHEAD < count))
        def _():
            x_send(num + AHEAD, True).start()

        @pl.when((num + AHEAD >= count) & (num + AHEAD < count + SHIFT))
        def _():
            x_send_extra(num + AHEAD - SHIFT).start()

        multiply(num, slot_of(num // SUBS))

        @pl.when(num >= LAG)
        def _():
            z_recv(num - LAG, False).wait_recv()
            pz_send(num - LAG, False).start()

        load(num)

    @pl.loop(body, count)
    def _(num):
        x_recv(num, True).wait_recv()

        @pl.when(num < count - SHIFT)
        def _():
            z_send(num, True).start()
        px_send(num, True).start()
        multiply(num, 2)

        @pl.when(num < body + LAG)
        def _():
            z_recv(num - LAG, False).wait_recv()
            pz_send(num - LAG, False).start()

        @pl.when(num >= body + LAG)
        def _():
            z_recv(num - LAG, True).wait_recv()
            pz_send(num - LAG, True).start()

        load(num)

    def relay_out(num):
        z_recv(num, True).wait_recv()
        pz_send(num, True).start()

    a_recv(last).wait_recv()
    near_wait(last, 2)
    wide = half // WIDE
    for part in range(2 * wide):
        which = depth if part < wide else 1 - depth
        first = (part % wide) * (WIDE // width)
        for k in range(WIDE // width):
            if part < wide:
                px_recv(body + first + k, True).wait_recv()
            else:
                pz_recv(body + first + k, True).wait_recv()
        at = pl.ds(pl.multiple_of(which * half + (part % wide) * WIDE, WIDE), WIDE)
        total = acc[:, at] + jnp.dot(a_v[last], b_v[2, :, at], preferred_element_type=jnp.float32)
        o_v[:, at] = total.astype(o_v.dtype)
        if part < LAG:
            relay_out(count - LAG + part)

    @pl.loop(count - BACK, body)
    def _(num):
        sent(num, False)

    @pl.loop(body, count)
    def _(num):
        sent(num, True)

    @pl.loop(steps - 2, steps)
    def _(step):
        a_send(step).wait_send()
        own_send(step).wait_send()


CHUNKS = 8


def write_out(done, c_ref, sems):
    rows = done.shape[0] // CHUNKS
    copies = [pltpu.make_async_copy(done.at[pl.ds(k * rows, rows)], c_ref.at[pl.ds(k * rows, rows)], sems.at[k])
              for k in range(CHUNKS)]
    for copy in copies:
        copy.start()
    for copy in copies:
        copy.wait()


def solution(mesh):
    def local_mm(a_blk, b_blk):
        band, cols = b_blk.shape
        rows_c = a_blk.shape[0] // 2
        steps = band // GROUP
        count = steps * SUBS
        any_spec = pl.BlockSpec(memory_space=pl.ANY)
        dma = pltpu.SemaphoreType.DMA
        c_blk, _ = pl.pallas_call(
            kernel,
            out_shape=(pltpu.VMEM((rows_c, cols), jnp.bfloat16),
                       jax.ShapeDtypeStruct((4 * band, cols), jnp.bfloat16)),
            in_specs=[any_spec] * 2,
            out_specs=(pl.BlockSpec(memory_space=pltpu.VMEM), any_spec),
            scratch_shapes=[
                pltpu.VMEM((steps, rows_c, 4 * GROUP), jnp.bfloat16),
                pltpu.VMEM((rows_c, cols), jnp.float32),
                pltpu.VMEM((3, 4 * GROUP, cols), jnp.bfloat16),
                dma((steps,)), dma((steps,)), dma((steps,)),
                dma((count,)), dma((count,)), dma((count,)), dma((count,)),
                dma((steps,)), dma((steps,)),
                dma((count,)), dma((count,)), dma((count,)), dma((count,)),
                dma((SUBS,)), dma((2,)),
            ],
            compiler_params=pltpu.CompilerParams(
                collective_id=0, has_side_effects=True, vmem_limit_bytes=52 * 1024 * 1024),
            cost_estimate=pl.CostEstimate(
                flops=2 * rows_c * cols * 2 * cols, bytes_accessed=200 * 2 ** 20, transcendentals=0),
        )(a_blk, b_blk)
        return pl.pallas_call(
            write_out,
            out_shape=jax.ShapeDtypeStruct((rows_c, cols), jnp.bfloat16),
            in_specs=[pl.BlockSpec(memory_space=pltpu.VMEM)],
            out_specs=any_spec,
            scratch_shapes=[dma((CHUNKS,))],
            compiler_params=pltpu.CompilerParams(vmem_limit_bytes=1024 * 1024),
        )(pltpu.with_memory_space_constraint(c_blk, pltpu.VMEM))

    return jax.shard_map(
        local_mm, mesh=mesh, in_specs=(P("row", "col"), P("row", "col")),
        out_specs=P(("row", "depth"), "col"), check_vma=False)
```

```python
import jax
import jax.numpy as jnp
from jax import lax
from jax.experimental import pallas as pl
from jax.experimental.pallas import tpu as pltpu
from jax.sharding import PartitionSpec as P

MESH = pl.DeviceIdType.MESH
GROUP = 128
SUBS = 4
AHEAD = 6
LAG = 2
SHIFT = 1
LOAD = 3
TILE = 1024
BACK = 8
WIDE = 1024


def kernel(a_ref, b_ref, o_v, ball, a_v, acc, b_v,
           load_a, send_a, recv_a, send_x, recv_x, send_z, recv_z, send_own, recv_own,
           send_px, recv_px, send_pz, recv_pz, load_far, load_near):
    depth = lax.axis_index("depth")
    col = lax.axis_index("col")
    row = lax.axis_index("row")
    core = lax.rem(row, 2)
    chip_x = row // 2
    rows_c = a_ref.shape[0] // 2
    band = b_ref.shape[0]
    cols = b_ref.shape[1]
    steps = band // GROUP
    last = steps - 1
    half = cols // 2
    width = half // SUBS
    count = steps * SUBS
    body = count - SUBS
    per = TILE // width
    tiles = half // TILE

    row_far = lax.rem(row + 2, 4)
    row_peer = chip_x * 2 + (1 - core)
    row_far_peer = lax.rem(row_peer + 2, 4)
    dev_x = (depth, col, row_far)
    dev_y = (depth, 1 - col, row)
    dev_z = (1 - depth, col, row)
    dev_p = (depth, col, row_peer)
    near = chip_x * 2 * GROUP
    far = (1 - chip_x) * 2 * GROUP

    def slot_of(step):
        return lax.rem(step, 2)

    def remote(src, dst, send, recv, num, dev):
        return pltpu.make_async_remote_copy(
            src, dst, send.at[num], recv.at[num], device_id=dev, device_id_type=MESH)

    def a_cols(step, side):
        return a_v.at[step, :, pl.ds(side * 2 * GROUP, 2 * GROUP)]

    def a_load(step, part):
        return pltpu.make_async_copy(
            a_ref.at[pl.ds(depth * rows_c, rows_c), pl.ds(part * band + step * GROUP, GROUP)],
            a_v.at[step, :, pl.ds(col * 2 * GROUP + part * GROUP, GROUP)], load_a.at[step])

    def a_load_wait(step):
        pltpu.make_async_copy(a_cols(step, col), a_cols(step, col), load_a.at[step]).wait()

    def a_send(step):
        return remote(a_cols(step, col), a_cols(step, col), send_a, recv_a, step, dev_y)

    def a_recv(step):
        return remote(a_cols(step, 1 - col), a_cols(step, 1 - col), send_a, recv_a, step, dev_y)

    def piece(band_row, num, which):
        return ball.at[pl.ds(band_row * band + (num // SUBS) * GROUP, GROUP),
                       pl.ds(which * half + lax.rem(num, SUBS) * width, width)]

    def last_piece(core_of, num, which, first=far):
        return b_v.at[2, pl.ds(first + core_of * GROUP, GROUP),
                      pl.ds(which * half + lax.rem(num, SUBS) * width, width)]

    def source(num, which):
        return b_ref.at[pl.ds((num // SUBS) * GROUP, GROUP),
                        pl.ds(which * half + lax.rem(num, SUBS) * width, width)]

    def mine(num, which, is_last):
        return last_piece(core, num, which) if is_last else piece(row_far, num, which)

    def peers(num, which, is_last):
        return last_piece(1 - core, num, which) if is_last else piece(row_far_peer, num, which)

    def x_send(num, is_last):
        dst = last_piece(core, num, depth, near) if is_last else piece(row, num, depth)
        return remote(source(num, depth), dst, send_x, recv_x, num, dev_x)

    def x_send_extra(num):
        return remote(source(num, 1 - depth), last_piece(core, num, 1 - depth, near), send_z, recv_z, num, dev_x)

    def x_recv(num, is_last):
        here = mine(num, depth, is_last)
        return remote(here, here, send_x, recv_x, num, dev_x)

    def z_send(num, is_last):
        here = mine(num, depth, is_last)
        return remote(here, here, send_z, recv_z, num, dev_z)

    def z_recv(num, is_last):
        here = mine(num, 1 - depth, is_last)
        return remote(here, here, send_z, recv_z, num, dev_z)

    def px_send(num, is_last):
        here = mine(num, depth, is_last)
        return remote(here, here, send_px, recv_px, num, dev_p)

    def px_recv(num, is_last):
        here = peers(num, depth, is_last)
        return remote(here, here, send_px, recv_px, num, dev_p)

    def pz_send(num, is_last):
        here = mine(num, 1 - depth, is_last)
        return remote(here, here, send_pz, recv_pz, num, dev_p)

    def pz_recv(num, is_last):
        here = peers(num, 1 - depth, is_last)
        return remote(here, here, send_pz, recv_pz, num, dev_p)

    def own_send(step):
        return remote(
            b_ref.at[pl.ds(step * GROUP, GROUP), :], ball.at[pl.ds(row * band + step * GROUP, GROUP), :],
            send_own, recv_own, step, dev_p)

    def own_recv(step):
        here = ball.at[pl.ds(row_peer * band + step * GROUP, GROUP), :]
        return remote(here, here, send_own, recv_own, step, dev_p)

    def near_loads(step, slot):
        pltpu.make_async_copy(
            b_ref.at[pl.ds(step * GROUP, GROUP), :],
            b_v.at[slot, pl.ds(near + core * GROUP, GROUP), :], load_near.at[lax.rem(step, 2)]).start()
        pltpu.make_async_copy(
            ball.at[pl.ds(row_peer * band + step * GROUP, GROUP), :],
            b_v.at[slot, pl.ds(near + (1 - core) * GROUP, GROUP), :], load_near.at[lax.rem(step, 2)]).start()

    def near_wait(step, slot):
        here = b_v.at[slot, pl.ds(near, 2 * GROUP), :]
        pltpu.make_async_copy(here, here, load_near.at[lax.rem(step, 2)]).wait()

    def tile_cols(num):
        at = lax.rem(num, 2 * tiles)
        which = jnp.where(at < tiles, depth, 1 - depth)
        return pl.ds(pl.multiple_of(which * half + lax.rem(at, tiles) * TILE, TILE), TILE)

    def far_loads(num):
        step = num // SUBS
        slot = slot_of(step)
        at = tile_cols(num)
        for band_row, part in ((row_far, core), (row_far_peer, 1 - core)):
            pltpu.make_async_copy(
                ball.at[pl.ds(band_row * band + step * GROUP, GROUP), at],
                b_v.at[slot, pl.ds(far + part * GROUP, GROUP), at], load_far.at[lax.rem(num, SUBS)]).start()

    def far_wait(num):
        here = b_v.at[slot_of(num // SUBS), pl.ds(far, 2 * GROUP), tile_cols(num)]
        pltpu.make_async_copy(here, here, load_far.at[lax.rem(num, SUBS)]).wait()

    def sent(num, is_last):
        x_send(num, is_last).wait_send()
        z_send(num, is_last).wait_send()
        px_send(num, is_last).wait_send()
        pz_send(num, is_last).wait_send()

    def multiply(num, slot):
        step = num // SUBS

        @pl.when(lax.rem(num, SUBS) == 0)
        def _():
            own_recv(step).wait_recv()
            near_loads(step, slot)

            @pl.when(step + 2 < steps)
            def _():
                own_send(step + 2).start()

            @pl.when(step >= 1)
            def _():
                a_recv(step - 1).wait_recv()
                near_wait(step - 1, slot_of(step - 1))

        @pl.when(step >= 1)
        def _():
            far_wait(num - SUBS)
            at = tile_cols(num)
            acc[:, at] += jnp.dot(a_v[step - 1], b_v[slot_of(step - 1), :, at], preferred_element_type=jnp.float32)

    def load(num):
        step = num // SUBS

        @pl.when((num >= LOAD) & (num < body + LOAD))
        def _():
            new = num - LOAD
            at = lax.rem(new, 2 * tiles)
            first = (new // SUBS) * SUBS + lax.rem(at, tiles) * per

            @pl.when(at < tiles)
            def _():
                for k in range(per):
                    px_recv(first + k, False).wait_recv()

            @pl.when(at >= tiles)
            def _():
                for k in range(per):
                    pz_recv(first + k, False).wait_recv()
            far_loads(new)

        @pl.when(num >= BACK)
        def _():
            sent(num - BACK, False)

        @pl.when((lax.rem(num, SUBS) == 0) & (step >= 2))
        def _():
            a_send(step - 2).wait_send()
            own_send(step - 2).wait_send()

    barrier = pltpu.get_barrier_semaphore()
    for dev in (dev_x, dev_y, dev_z, dev_p):
        pl.semaphore_signal(barrier, inc=1, device_id=dev, device_id_type=MESH)

    @pl.loop(0, steps)
    def _(step):
        a_load(step, 0).start()
        a_load(step, 1).start()

    pl.semaphore_wait(barrier, 4)

    x_send(0, False).start()
    a_load_wait(0)
    a_send(0).start()

    @pl.loop(1, AHEAD)
    def _(num):
        x_send(num, False).start()

    own_send(0).start()
    own_send(1).start()

    @pl.loop(1, steps)
    def _(step):
        a_load_wait(step)
        a_send(step).start()

    @pl.loop(0, cols // TILE)
    def _(tile):
        at = pl.ds(pl.multiple_of(tile * TILE, TILE), TILE)
        acc[:, at] = jnp.zeros((rows_c, TILE), jnp.float32)

    @pl.loop(0, body)
    def _(num):
        x_recv(num, False).wait_recv()
        z_send(num, False).start()
        px_send(num, False).start()

        @pl.when(num + AHEAD < body)
        def _():
            x_send(num + AHEAD, False).start()

        @pl.when((num + AHEAD >= body) & (num + AHEAD < count))
        def _():
            x_send(num + AHEAD, True).start()

        @pl.when((num + AHEAD >= count) & (num + AHEAD < count + SHIFT))
        def _():
            x_send_extra(num + AHEAD - SHIFT).start()

        multiply(num, slot_of(num // SUBS))

        @pl.when(num >= LAG)
        def _():
            z_recv(num - LAG, False).wait_recv()
            pz_send(num - LAG, False).start()

        load(num)

    @pl.loop(body, count)
    def _(num):
        x_recv(num, True).wait_recv()

        @pl.when(num < count - SHIFT)
        def _():
            z_send(num, True).start()
        px_send(num, True).start()
        multiply(num, 2)

        @pl.when(num < body + LAG)
        def _():
            z_recv(num - LAG, False).wait_recv()
            pz_send(num - LAG, False).start()

        @pl.when(num >= body + LAG)
        def _():
            z_recv(num - LAG, True).wait_recv()
            pz_send(num - LAG, True).start()

        load(num)

    def relay_out(num):
        z_recv(num, True).wait_recv()
        pz_send(num, True).start()

    def finish(part, first, size):
        which = depth if part < wide else 1 - depth
        at = pl.ds(pl.multiple_of(which * half + part % wide * WIDE + first, size), size)
        total = acc[:, at] + jnp.dot(a_v[last], b_v[2, :, at], preferred_element_type=jnp.float32)
        o_v[:, at] = total.astype(o_v.dtype)

    a_recv(last).wait_recv()
    near_wait(last, 2)
    wide = half // WIDE
    for part in range(wide):
        for k in range(WIDE // width):
            px_recv(body + part * (WIDE // width) + k, True).wait_recv()
        finish(part, 0, WIDE)
        relay_out(count - 1 - part)
    for k in range(2):
        pz_recv(body + k, True).wait_recv()
    finish(wide, 0, WIDE)
    for k in (1, 0):
        pz_recv(body + 2 + k, True).wait_recv()
        finish(wide + 1, k * width, width)

    @pl.loop(count - BACK, body)
    def _(num):
        sent(num, False)

    @pl.loop(body, count)
    def _(num):
        sent(num, True)

    @pl.loop(steps - 2, steps)
    def _(step):
        a_send(step).wait_send()
        own_send(step).wait_send()


CHUNKS = 8


def write_out(done, c_ref, sems):
    rows = done.shape[0] // CHUNKS
    copies = [pltpu.make_async_copy(done.at[pl.ds(k * rows, rows)], c_ref.at[pl.ds(k * rows, rows)], sems.at[k])
              for k in range(CHUNKS)]
    for copy in copies:
        copy.start()
    for copy in copies:
        copy.wait()


def solution(mesh):
    def local_mm(a_blk, b_blk):
        band, cols = b_blk.shape
        rows_c = a_blk.shape[0] // 2
        steps = band // GROUP
        count = steps * SUBS
        any_spec = pl.BlockSpec(memory_space=pl.ANY)
        dma = pltpu.SemaphoreType.DMA
        c_blk, _ = pl.pallas_call(
            kernel,
            out_shape=(pltpu.VMEM((rows_c, cols), jnp.bfloat16),
                       jax.ShapeDtypeStruct((4 * band, cols), jnp.bfloat16)),
            in_specs=[any_spec] * 2,
            out_specs=(pl.BlockSpec(memory_space=pltpu.VMEM), any_spec),
            scratch_shapes=[
                pltpu.VMEM((steps, rows_c, 4 * GROUP), jnp.bfloat16),
                pltpu.VMEM((rows_c, cols), jnp.float32),
                pltpu.VMEM((3, 4 * GROUP, cols), jnp.bfloat16),
                dma((steps,)), dma((steps,)), dma((steps,)),
                dma((count,)), dma((count,)), dma((count,)), dma((count,)),
                dma((steps,)), dma((steps,)),
                dma((count,)), dma((count,)), dma((count,)), dma((count,)),
                dma((SUBS,)), dma((2,)),
            ],
            compiler_params=pltpu.CompilerParams(
                collective_id=0, has_side_effects=True, vmem_limit_bytes=52 * 1024 * 1024),
            cost_estimate=pl.CostEstimate(
                flops=2 * rows_c * cols * 2 * cols, bytes_accessed=200 * 2 ** 20, transcendentals=0),
        )(a_blk, b_blk)
        return pl.pallas_call(
            write_out,
            out_shape=jax.ShapeDtypeStruct((rows_c, cols), jnp.bfloat16),
            in_specs=[pl.BlockSpec(memory_space=pltpu.VMEM)],
            out_specs=any_spec,
            scratch_shapes=[dma((CHUNKS,))],
            compiler_params=pltpu.CompilerParams(vmem_limit_bytes=1024 * 1024),
        )(pltpu.with_memory_space_constraint(c_blk, pltpu.VMEM))

    return jax.shard_map(
        local_mm, mesh=mesh, in_specs=(P("row", "col"), P("row", "col")),
        out_specs=P(("row", "depth"), "col"), check_vma=False)
```
